128 devices in a mesh: gz: 128 (over x, y, z, core).
Axes of the slice: x: 4, y: 4, z: 4, core: 2. Of those that a mesh axis runs over, the one named last changes fastest.
Arguments:
- density: float32 [2, 128, 256, 256], P(None, 'gz'), may hold values from 0.02 to 0.8
- kernel_hat: float32 [256, 512, 512], P(None, 'gz'), may hold values from 0.37 to 7, as said below
Outputs:
- potential: float32 [2, 128, 256, 256], P(None, 'gz')
- energies: float32 [2], replicated
The draws below stay inside these ranges and needn't reach their ends.
Inputs may be any that keep to these rules, and one draw needn't show every extreme that they name: kernel_hat at (a, b, c) equals kernel_hat at ((-a) mod 256, (-b) mod 512, (-c) mod 512).
All inputs are finite; a program needn't handle non-finite values.
Results may differ from the reference program's by a relative error of at most 0.00015.
Values sent between devices are 32-bit elements; how exact they have to be, the bound alone decides.
No kernel may reach another device: no remote copies, remote signals or barrier semaphores. Data moves between devices by JAX's collectives and lax.ppermute only.
A program may use at most 64 MiB of HBM per device.

```python
import math
import jax
import jax.numpy as jnp
from jax import lax

NX = 256
NY = 256
NZ = 128
MX = 512
MY = 512
MZ = 256


SCREEN = 0.01


STRENGTH = 0.02


CONTACT = 1.5


def draw_density(key, part):
    height = jnp.arange(NZ, dtype=jnp.float32)[None, :, None, None] / max(NZ - 1, 1)
    uniform_draw = jax.random.uniform(key, (2, NZ, NY, NX), jnp.float32)
    ramp_values = 0.1 * jnp.exp(math.log(4.5) * height)
    return ramp_values * 0.3 * jnp.exp(math.log(5.0) * uniform_draw)


def symbol(length_cells):
    indices = jnp.arange(length_cells, dtype=jnp.int32)
    folded = jnp.minimum(indices, length_cells - indices).astype(jnp.float32)
    return (2.0 * jnp.sin(math.pi * folded / length_cells)) ** 2


def draw_kernel_hat(key, part):
    laplace = symbol(MZ)[:, None, None] + symbol(MY)[None, :, None] + symbol(MX)[None, None, :]
    uniform_draw = jax.random.uniform(key, (MZ, MY, MX), jnp.float32)
    roughness = jnp.exp(math.log(0.5) + math.log(4.0) * uniform_draw)
    mirrored = roughness
    for direction in range(3):
        mirrored = jnp.roll(jnp.flip(mirrored, direction), 1, direction)
    return (STRENGTH / (laplace + SCREEN) + CONTACT) * (0.5 * (roughness + mirrored))


def setup_inputs(seed: int = 0) -> dict:
    key_list = jax.random.split(jax.random.key(seed), 3)
    density = draw_density(jax.random.fold_in(key_list[2], 71), 0)
    kernel_hat = draw_kernel_hat(jax.random.fold_in(key_list[2], 71), 0)
    return {"density": density, "kernel_hat": kernel_hat}


HGRID = 0.35
STENCIL = (0.8, -0.2, 4.0 / 105.0, -1.0 / 280.0)
KAPPA = 0.804
MU_X = 0.2195149727645171
BETA_C = 0.06672455060314922
GAMMA_C = 0.031090690869654894
FZ_CURV = 1.709921
PARAMS_UNPOL = (0.031091, 0.2137, 7.5957, 3.5876, 1.6382, 0.49294)
PARAMS_POL = (0.015545, 0.20548, 14.1189, 6.1977, 3.3662, 0.62517)
PARAMS_STIFF = (0.016887, 0.11125, 10.357, 3.6231, 0.88026, 0.49671)

def inner_slope(extended, direction):
    stencil_reach = len(STENCIL)
    length_out = extended.shape[direction] - 2 * stencil_reach
    result = 0.0
    for offset, weight in enumerate(STENCIL):
        upper_part = lax.slice_in_dim(extended, stencil_reach + offset + 1, stencil_reach + offset + 1 + length_out, axis=direction)
        lower_part = lax.slice_in_dim(extended, stencil_reach - offset - 1, stencil_reach - offset - 1 + length_out, axis=direction)
        result = result + weight * (upper_part - lower_part)
    return result / HGRID

def plane_slope(field, direction):
    stencil_reach = len(STENCIL)
    widths = [(0, 0)] * field.ndim
    widths[direction] = (stencil_reach, stencil_reach)
    return inner_slope(jnp.pad(field, widths), direction)

def pw_piece(radius, params):
    half_root = jnp.sqrt(radius)
    series = params[2] * half_root + params[3] * radius + params[4] * radius * half_root + params[5] * radius * radius
    return -2.0 * params[0] * (1.0 + params[1] * radius) * jnp.log1p(1.0 / (2.0 * params[0] * series))

def exchange_part(doubled, sigma_four):
    cube_root = jnp.cbrt(doubled)
    uniform_part = -0.75 * (3.0 / math.pi) ** (1.0 / 3.0) * cube_root
    reduced = sigma_four / (4.0 * (3.0 * math.pi ** 2) ** (2.0 / 3.0) * doubled ** 2 * cube_root ** 2)
    enhance = 1.0 + KAPPA - KAPPA / (1.0 + MU_X * reduced / KAPPA)
    return doubled * uniform_part * enhance

def energy_density(dens_up, dens_down, sigma_uu, sigma_ud, sigma_dd):
    exchange_term = 0.5 * exchange_part(2.0 * dens_up, 4.0 * sigma_uu) + 0.5 * exchange_part(2.0 * dens_down, 4.0 * sigma_dd)
    density_sum = dens_up + dens_down
    polarization = (dens_up - dens_down) / density_sum
    radius = jnp.cbrt(3.0 / (4.0 * math.pi * density_sum))
    plus_side = 1.0 + polarization
    minus_side = 1.0 - polarization
    plus_cube = jnp.cbrt(plus_side)
    minus_cube = jnp.cbrt(minus_side)
    spin_weight = (plus_side * plus_cube + minus_side * minus_cube - 2.0) / (2.0 ** (4.0 / 3.0) - 2.0)
    unpolar = pw_piece(radius, PARAMS_UNPOL)
    polarized = pw_piece(radius, PARAMS_POL)
    stiffness = pw_piece(radius, PARAMS_STIFF)
    polar_four = polarization ** 4
    local_corr = unpolar - stiffness * spin_weight * (1.0 - polar_four) / FZ_CURV + (polarized - unpolar) * spin_weight * polar_four
    phi_factor = 0.5 * (plus_cube ** 2 + minus_cube ** 2)
    phi_cubed = phi_factor ** 3
    screening_sq = 4.0 * jnp.cbrt(3.0 * math.pi ** 2 * density_sum) / math.pi
    sigma_total = sigma_uu + 2.0 * sigma_ud + sigma_dd
    scaled_sq = sigma_total / (4.0 * phi_factor ** 2 * screening_sq * density_sum ** 2)
    weight_a = BETA_C / GAMMA_C / jnp.expm1(-local_corr / (GAMMA_C * phi_cubed))
    gradient_term = GAMMA_C * phi_cubed * jnp.log1p(BETA_C / GAMMA_C * scaled_sq * (1.0 + weight_a * scaled_sq) / (1.0 + weight_a * scaled_sq + weight_a ** 2 * scaled_sq ** 2))
    return exchange_term + density_sum * (local_corr + gradient_term)

def flux_pair(deriv_uu, deriv_ud, deriv_dd, gradient):
    return jnp.stack([2.0 * deriv_uu * gradient[0] + deriv_ud * gradient[1], 2.0 * deriv_dd * gradient[1] + deriv_ud * gradient[0]])

def xc_fields(dens, grad_z, grad_y, grad_x):
    sigma_uu = grad_z[0] * grad_z[0] + grad_y[0] * grad_y[0] + grad_x[0] * grad_x[0]
    sigma_ud = grad_z[0] * grad_z[1] + grad_y[0] * grad_y[1] + grad_x[0] * grad_x[1]
    sigma_dd = grad_z[1] * grad_z[1] + grad_y[1] * grad_y[1] + grad_x[1] * grad_x[1]
    energy, pullback = jax.vjp(energy_density, dens[0], dens[1], sigma_uu, sigma_ud, sigma_dd)
    d_up, d_down, d_uu, d_ud, d_dd = pullback(jnp.ones_like(energy))
    return (energy, jnp.stack([d_up, d_down]), flux_pair(d_uu, d_ud, d_dd, grad_z), flux_pair(d_uu, d_ud, d_dd, grad_y), flux_pair(d_uu, d_ud, d_dd, grad_x))

def plane_terms(slices):
    density_plane, grad_z, grad_y, grad_x = slices
    return xc_fields(density_plane, grad_z, grad_y, grad_x)

def reference(density, kernel_hat):
    grad_z = plane_slope(density, 1)
    grad_y = plane_slope(density, 2)
    grad_x = plane_slope(density, 3)
    moved = tuple((jnp.moveaxis(array_item, 1, 0) for array_item in (density, grad_z, grad_y, grad_x)))
    energy, d_dens, flux_z, flux_y, flux_x = lax.map(plane_terms, moved)
    d_dens = jnp.moveaxis(d_dens, 0, 1)
    flux_z = jnp.moveaxis(flux_z, 0, 1)
    flux_y = jnp.moveaxis(flux_y, 0, 1)
    flux_x = jnp.moveaxis(flux_x, 0, 1)
    v_xc = d_dens - (plane_slope(flux_z, 1) + plane_slope(flux_y, 2) + plane_slope(flux_x, 3))
    density_sum = density[0] + density[1]
    padded = jnp.pad(density_sum, ((0, NZ), (0, NY), (0, NX)))
    spectrum = jnp.fft.rfftn(padded)
    filtered = jnp.fft.irfftn(spectrum * kernel_hat[:, :, :NX + 1], s=padded.shape)
    hartree = filtered[:NZ, :NY, :NX]
    potential = v_xc + hartree[None]
    energies = jnp.stack([jnp.mean(energy), 0.5 * jnp.mean(density_sum * hartree)])
    return (potential, energies)
```

```python
import math

import jax
import jax.numpy as jnp
import numpy as np
from jax import lax
from jax.experimental import pallas as pl
from jax.experimental.pallas import tpu as pltpu
from jax.sharding import Mesh
from jax.sharding import PartitionSpec as P

GZ = ("gz_0", "gz_1", "gz_2", "gz_3")
HGRID = 0.35
STENCIL = (0.8, -0.2, 4.0 / 105.0, -1.0 / 280.0)
KAPPA = 0.804
MU_X = 0.2195149727645171
BETA_C = 0.06672455060314922
GAMMA_C = 0.031090690869654894
FZ_CURV = 1.709921
PARAMS_UNPOL = (0.031091, 0.2137, 7.5957, 3.5876, 1.6382, 0.49294)
PARAMS_POL = (0.015545, 0.20548, 14.1189, 6.1977, 3.3662, 0.62517)
PARAMS_STIFF = (0.016887, 0.11125, 10.357, 3.6231, 0.88026, 0.49671)

F32 = jnp.float32
BF16 = jnp.bfloat16
NZ, NY, NX = 128, 256, 256
MZ, MY, MX = 256, 512, 512
ND = 128
A_ROWS = 16
B_ROWS = 10
D_ROWS = 12
CELLS = NZ * NY * NX
VMEM = pl.BlockSpec(memory_space=pltpu.VMEM)
SMEM = pl.BlockSpec(memory_space=pltpu.SMEM)


def slope_matrix(n):
    m = np.zeros((n, n))
    for k, c in enumerate(STENCIL, 1):
        m += np.diag(np.full(n - k, c / HGRID), k) - np.diag(np.full(n - k, c / HGRID), -k)
    return m.astype(np.float32)


def halves(m):
    m = np.asarray(m, np.float32)
    hi = m.astype(BF16)
    lo = (m - hi.astype(np.float32)).astype(BF16)
    return np.stack([hi, lo])


def owned_frequencies():
    q = np.arange(ND)
    first = np.where(q < ND // 2, 4 * q + 1, 4 * q)
    return first, first + 1


def y_forward():
    y = np.arange(NY)
    rows = []
    for ky in owned_frequencies():
        angle = 2.0 * np.pi * (np.outer(ky, y) % MY) / MY
        rows += [np.cos(angle), -np.sin(angle)]
    return halves(np.concatenate(rows, 0))


def y_backward():
    y = np.arange(NY)
    cols = []
    for ky in owned_frequencies():
        angle = 2.0 * np.pi * (np.outer(y, ky) % MY) / MY
        weight = np.where(ky == MY // 2, 1.0, 2.0) / (MX * MY * MZ)
        cols += [np.cos(angle) * weight, -np.sin(angle) * weight]
    return halves(np.concatenate(cols, 1))


def parity_matrix():
    m = np.zeros((NX, NX), np.float32)
    x = np.arange(NX)
    m[x, (x % 2) * (NX // 2) + x // 2] = 1.0
    return m


def rotation(angle):
    c, s = np.cos(angle), np.sin(angle)
    return np.block([[c, s], [-s, c]])


def x_forward():
    out = []
    k = np.arange(MX // 2)
    for parity in (0, 1):
        x = 2 * np.arange(NX // 2) + parity
        out.append(rotation(2.0 * np.pi * (np.outer(k, x) % MX) / MX).T)
    return np.stack([halves(m) for m in out])


def x_backward():
    out = []
    k = np.arange(MX // 2)
    for parity in (0, 1):
        x = 2 * np.arange(NX // 2) + parity
        out.append(rotation(2.0 * np.pi * (np.outer(k, x) % MX) / MX))
    return np.stack([halves(m) for m in out])


Z_CHUNK = 32


def z_forward():
    z = np.arange(NZ)
    rows = []
    for c in range(0, NZ, Z_CHUNK):
        low = np.arange(c, c + Z_CHUNK)
        kz = np.concatenate([low, low + NZ])
        rows.append(rotation(2.0 * np.pi * (np.outer(kz, z) % MZ) / MZ))
    return halves(np.concatenate(rows, 0))


def z_backward():
    out = []
    k = np.arange(NZ)
    for parity in (0, 1):
        z = 2 * np.arange(NZ // 2) + parity
        out.append(rotation(2.0 * np.pi * (np.outer(k, z) % MZ) / MZ).T)
    return np.stack([halves(m) for m in out])


def split(value):
    hi = value.astype(BF16)
    lo = (value - hi.astype(F32)).astype(BF16)
    return hi, lo


def dot1(a, b):
    return jnp.dot(a, b, preferred_element_type=F32)


def dot3(a_hi, a_lo, b_hi, b_lo):
    return dot1(a_hi, b_hi) + (dot1(a_lo, b_hi) + dot1(a_hi, b_lo))


def dot_exact(a, b):
    return jnp.dot(a, b, precision=lax.Precision.HIGHEST, preferred_element_type=F32)


def put_rows(ref, row, rows, value, count=ND, scale=1):
    for half in range(value.shape[1] // 128):
        ref[pl.ds(row + half, count, stride=rows * scale), :] = value[
            :, half * 128 : half * 128 + 128
        ]


def get_rows(ref, row, rows):
    return jnp.concatenate(
        [ref[pl.ds(row + half, ND, stride=rows), :] for half in range(2)], axis=1
    )


def gradient_kernel(dens_ref, slope_ref, out_ref):
    for spin in range(2):
        field = dens_ref[spin * NY : (spin + 1) * NY, :]
        grad = dot_exact(slope_ref[...], field)
        for part in range(2):
            rows = slice(part * 128, part * 128 + 128)
            put_rows(out_ref, spin * 4 + part * 2, A_ROWS, field[rows])
            put_rows(out_ref, 8 + spin * 4 + part * 2, A_ROWS, grad[rows])


def y_forward_kernel(dens_ref, parity_ref, table_ref, out_ref):
    hi, lo = split(dens_ref[0:NY, :] + dens_ref[NY : 2 * NY, :])
    parity = parity_ref[...]
    hi, lo = dot1(hi, parity), dot1(lo, parity)
    mean_row = jnp.sum(hi + lo, axis=0, keepdims=True)
    put_rows(out_ref, 8, B_ROWS, jnp.broadcast_to(mean_row, (ND, NX)))
    hi, lo = hi.astype(BF16), lo.astype(BF16)
    for s in range(4):
        rows = slice(s * ND, (s + 1) * ND)
        value = dot3(table_ref[0, rows, :], table_ref[1, rows, :], hi, lo)
        put_rows(out_ref, s * 2, B_ROWS, value)


def pw_piece(root, params):
    radius = root * root
    scale = 2.0 * params[0]
    series = root * (
        scale * params[2]
        + root * (scale * params[3] + root * (scale * params[4] + root * (scale * params[5])))
    )
    slope = root * (
        0.5 * scale * params[2]
        + root
        * (
            scale * params[3]
            + root * (1.5 * scale * params[4] + root * (2.0 * scale * params[5]))
        )
    )
    inv = 1.0 / (series * (series + 1.0))
    logarithm = jnp.log(1.0 + inv * (series + 1.0))
    front = -scale - (scale * params[1]) * radius
    value = front * logarithm
    deriv = (-scale * params[1]) * radius * logarithm - front * slope * inv
    return value, deriv


def exchange_piece(dens, inv_root, sigma):
    root = 2.0 * dens * inv_root * inv_root
    inv2 = inv_root * inv_root
    inv4 = inv2 * inv2
    reduced = sigma * (inv4 * inv4) * (1.0 / (3.0 * math.pi**2) ** (2.0 / 3.0))
    damp = 1.0 / (1.0 + (MU_X / KAPPA) * reduced)
    enhance = (1.0 + KAPPA) - KAPPA * damp
    front = -0.75 * (3.0 / math.pi) ** (1.0 / 3.0)
    damp_sq = MU_X * damp * damp
    energy = front * dens * root * enhance
    d_dens = (4.0 / 3.0 * front) * root * (enhance - 2.0 * reduced * damp_sq)
    d_sigma = (0.5 * front / (3.0 * math.pi**2) ** (2.0 / 3.0)) * damp_sq * inv4
    return energy, d_dens, d_sigma, root


def xc_point(up, down, sigma_uu, sigma_ud, sigma_dd):
    inv_up = jnp.exp(jnp.log(2.0 * up) * (-1.0 / 3.0))
    inv_down = jnp.exp(jnp.log(2.0 * down) * (-1.0 / 3.0))
    e_up, d_up, d_uu, root_up = exchange_piece(up, inv_up, sigma_uu)
    e_down, d_down, d_dd, root_down = exchange_piece(down, inv_down, sigma_dd)
    dens = up + down
    sixth = jnp.exp(jnp.log(dens) * (-1.0 / 6.0))
    inv_third = sixth * sixth
    third = dens * inv_third * inv_third
    inv_dens = inv_third * inv_third * inv_third
    zeta = (up - down) * inv_dens
    plus = 2.0 * up * inv_dens
    minus = 2.0 * down * inv_dens
    plus_cube = root_up * inv_third
    minus_cube = root_down * inv_third
    f_scale = 1.0 / (2.0 ** (4.0 / 3.0) - 2.0)
    f = (plus * plus_cube + minus * minus_cube - 2.0) * f_scale
    f_slope = (plus_cube - minus_cube) * (4.0 / 3.0 * f_scale)
    root = (3.0 / (4.0 * math.pi)) ** (1.0 / 6.0) * sixth
    e0, e0_d = pw_piece(root, PARAMS_UNPOL)
    e1, e1_d = pw_piece(root, PARAMS_POL)
    ac, ac_d = pw_piece(root, PARAMS_STIFF)
    z2 = zeta * zeta
    z3_4 = 4.0 * z2 * zeta
    z4 = z2 * z2
    one_z4 = (1.0 - z4) * (-1.0 / FZ_CURV)
    f_z4 = f * z4
    f_one = f * one_z4
    diff = e1 - e0
    local = e0 + ac * f_one + diff * f_z4
    local_r = e0_d + ac_d * f_one + (e1_d - e0_d) * f_z4
    fz3 = z3_4 * f
    local_z = ac * (f_slope * one_z4 + (1.0 / FZ_CURV) * fz3) + diff * (f_slope * z4 + fz3)
    phi = 0.5 * (plus_cube * plus_cube + minus_cube * minus_cube)
    inv_phi = 1.0 / phi
    phi_log_slope = (third * (1.0 / 3.0)) * (inv_up - inv_down) * inv_phi
    g3 = GAMMA_C * phi * phi * phi
    inv_g3 = (1.0 / GAMMA_C) * inv_phi * inv_phi * inv_phi
    grow = jnp.exp(-local * inv_g3)
    weight_a = (BETA_C / GAMMA_C) / (grow - 1.0)
    sigma = sigma_uu + 2.0 * sigma_ud + sigma_dd
    ct = math.pi / (16.0 * (3.0 * math.pi**2) ** (1.0 / 3.0))
    kt = ct * inv_third * inv_dens * inv_dens * inv_phi * inv_phi
    t2 = sigma * kt
    w = weight_a * t2
    num = 1.0 + w
    den = num + w * w
    add = (BETA_C / GAMMA_C) * t2 * num
    both = den + add
    inv_both = 1.0 / (den * both)
    h = g3 * jnp.log(1.0 + add * (inv_both * both))
    h_t = (BETA_C / GAMMA_C) * g3 * (1.0 + 2.0 * w) * inv_both
    h_a = -(w * w * w) * (2.0 + w) * grow * inv_both
    total = local + h
    ht_t2 = h_t * t2
    one_ha = 1.0 + h_a
    d_n = total - (1.0 / 3.0) * one_ha * local_r - (7.0 / 3.0) * ht_t2
    d_z = one_ha * local_z + phi_log_slope * (3.0 * (h - h_a * local) - 2.0 * ht_t2)
    d_sigma = dens * h_t * kt
    energy = e_up + e_down + dens * total
    return (
        energy,
        d_up + d_n + minus * d_z,
        d_down + d_n - plus * d_z,
        d_uu + d_sigma,
        2.0 * d_sigma,
        d_dd + d_sigma,
    )


def xc_kernel(in_ref, slope_z_ref, slope_x_ref, out_ref, energy_ref, dens, gz, gy, gx):
    for spin in range(2):
        for part in range(2):
            rows = slice(part * 128, part * 128 + 128)
            field = get_rows(in_ref, spin * 4 + part * 2, A_ROWS)
            dens[spin, rows, :] = field
            gy[spin, rows, :] = get_rows(in_ref, 8 + spin * 4 + part * 2, A_ROWS)
            gz[spin, rows, :] = dot_exact(slope_z_ref[...], field)
        gx[spin] = dot_exact(dens[spin], slope_x_ref[...])

    def chunk(i, total):
        rows = pl.ds(pl.multiple_of(i * 8, 8), 8)
        zu, zd = gz[0, rows, :], gz[1, rows, :]
        yu, yd = gy[0, rows, :], gy[1, rows, :]
        xu, xd = gx[0, rows, :], gx[1, rows, :]
        energy, d_up, d_down, d_uu, d_ud, d_dd = xc_point(
            dens[0, rows, :],
            dens[1, rows, :],
            zu * zu + yu * yu + xu * xu,
            zu * zd + yu * yd + xu * xd,
            zd * zd + yd * yd + xd * xd,
        )
        dens[0, rows, :] = d_up
        dens[1, rows, :] = d_down
        for ref, gu, gd in ((gz, zu, zd), (gy, yu, yd), (gx, xu, xd)):
            ref[0, rows, :] = 2.0 * d_uu * gu + d_ud * gd
            ref[1, rows, :] = 2.0 * d_dd * gd + d_ud * gu
        return total + energy

    total = lax.fori_loop(0, 32, chunk, jnp.zeros((8, NX), F32))
    energy_ref[0, 0] = jnp.sum(total)
    for spin in range(2):
        div_x = dot_exact(gx[spin], slope_x_ref[...])
        for part in range(2):
            rows = slice(part * 128, part * 128 + 128)
            div_z = dot_exact(slope_z_ref[...], gz[spin, rows, :])
            put_rows(
                out_ref, spin * 4 + part * 2, A_ROWS, dens[spin, rows, :] - (div_z + div_x[rows])
            )
            put_rows(out_ref, 8 + spin * 4 + part * 2, A_ROWS, gy[spin, rows, :])


def hartree_kernel(
    in_ref, filt_ref, weight_ref, exc_ref, wx_ref, wz_ref, wzi_ref, wxi_ref, out_ref,
    xp, sums, back,
):
    even = [in_ref[pl.ds(r, ND, stride=B_ROWS), :] for r in range(0, B_ROWS, 2)]
    odd = [in_ref[pl.ds(r, ND, stride=B_ROWS), :] for r in range(1, B_ROWS, 2)]
    zero = jnp.zeros((ND, 128), F32)
    even.append(zero)
    odd.append(zero)
    for slot in range(3):
        parts = []
        for parity, source in ((0, even), (1, odd)):
            hi, lo = split(jnp.concatenate(source[2 * slot : 2 * slot + 2], axis=1))
            parts.append(dot3(hi, lo, wx_ref[parity, 0], wx_ref[parity, 1]))
        for half, value in ((0, parts[0] + parts[1]), (1, parts[0] - parts[1])):
            cols = slice(half * 256, half * 256 + 256)
            hi, lo = split(value)
            xp[slot, 0, 0:128, cols] = hi[:, 0:256]
            xp[slot, 0, 128:256, cols] = hi[:, 256:512]
            xp[slot, 1, 0:128, cols] = lo[:, 0:256]
            xp[slot, 1, 128:256, cols] = lo[:, 256:512]
    energy = jnp.zeros((8, MX), F32)
    for slot in range(3):
        weight = weight_ref[slot]

        def chunk(c, acc, slot=slot):
            rows = pl.ds(pl.multiple_of(c * 128, 128), 128)
            spec = dot3(wz_ref[0, rows, :], wz_ref[1, rows, :], xp[slot, 0], xp[slot, 1])
            low = pl.ds(pl.multiple_of(c * Z_CHUNK, Z_CHUNK), Z_CHUNK)
            high = pl.ds(pl.multiple_of(NZ + c * Z_CHUNK, Z_CHUNK), Z_CHUNK)
            f_low, f_high = filt_ref[slot, low, :], filt_ref[slot, high, :]
            for kind in range(2):
                a = spec[kind * 64 : kind * 64 + 32]
                b = spec[kind * 64 + 32 : kind * 64 + 64]
                fa, fb = a * f_low, b * f_high
                power = a * fa + b * fb
                acc = acc + (power[0:8] + power[8:16] + power[16:24] + power[24:32])
                dest = pl.ds(pl.multiple_of(kind * NZ + c * Z_CHUNK, Z_CHUNK), Z_CHUNK)
                for parity, value in ((0, fa + fb), (1, fa - fb)):
                    hi, lo = split(value)
                    sums[parity, 0, dest, :] = hi
                    sums[parity, 1, dest, :] = lo
            return acc

        acc = lax.fori_loop(0, NZ // Z_CHUNK, chunk, jnp.zeros((8, MX), F32))
        energy = energy + weight * acc
        for parity in range(2):
            grid = dot3(
                wzi_ref[parity, 0], wzi_ref[parity, 1], sums[parity, 0], sums[parity, 1]
            )
            for sign in range(2):
                a, b = grid[:, 0:256], grid[:, 256:512]
                hi, lo = split(a + b if sign == 0 else a - b)
                for part, value in ((0, hi), (1, lo)):
                    rows = slice(parity * 64, parity * 64 + 64)
                    back[sign, part, rows, 0:256] = value[0:64]
                    back[sign, part, rows, 256:512] = value[64:128]
        for sign in range(2):
            value = dot3(back[sign, 0], back[sign, 1], wxi_ref[sign, 0], wxi_ref[sign, 1])
            for parity in range(2):
                for kind in range(2 if slot < 2 else 1):
                    put_rows(
                        out_ref,
                        parity * D_ROWS + slot * 4 + kind * 2 + sign,
                        D_ROWS,
                        value[parity * 64 : parity * 64 + 64, kind * 128 : kind * 128 + 128],
                        count=64,
                        scale=2,
                    )
    put_rows(out_ref, 10, D_ROWS, jnp.full((ND, 128), exc_ref[0, 0], F32))
    put_rows(out_ref, 11, D_ROWS, jnp.full((ND, 128), jnp.sum(energy), F32))


def divergence_kernel(in_ref, slope_ref, out_ref):
    for spin in range(2):
        flux = jnp.concatenate(
            [get_rows(in_ref, 8 + spin * 4 + part * 2, A_ROWS) for part in range(2)], axis=0
        )
        rest = jnp.concatenate(
            [get_rows(in_ref, spin * 4 + part * 2, A_ROWS) for part in range(2)], axis=0
        )
        out_ref[spin * NY : (spin + 1) * NY, :] = rest - dot_exact(slope_ref[...], flux)


def potential_kernel(in_ref, v_ref, table_ref, parity_ref, out_ref, energy_ref):
    field = jnp.concatenate([get_rows(in_ref, 2 * s, D_ROWS) for s in range(4)], axis=0)
    hi, lo = split(field)
    grid = dot3(table_ref[0], table_ref[1], hi, lo)
    mean_row = jnp.concatenate([in_ref[8:9, :], in_ref[9:10, :]], axis=1)
    grid = grid + mean_row * (1.0 / (MX * MY * MZ))
    hi, lo = split(grid)
    hartree = dot1(hi, parity_ref[...]) + dot1(lo, parity_ref[...])
    for spin in range(2):
        rows = slice(spin * NY, (spin + 1) * NY)
        out_ref[rows, :] = v_ref[rows, :] + hartree
    exc = jnp.sum(in_ref[pl.ds(10, ND, stride=D_ROWS), :], axis=0, keepdims=True)
    power = jnp.sum(in_ref[pl.ds(11, ND, stride=D_ROWS), :], axis=0, keepdims=True)
    energy_ref[0] = jnp.sum(exc) * (1.0 / (128.0 * CELLS))
    energy_ref[1] = jnp.sum(power) * (0.5 / (128.0 * CELLS * MX * MY * MZ))


def call(kernel, outs, n_in, flops, scratch=(), smem_in=(), smem_out=(), limit=48):
    single = not isinstance(outs, (list, tuple))
    shapes = [outs] if single else list(outs)
    specs = [SMEM if i in smem_out else VMEM for i in range(len(shapes))]
    return pl.pallas_call(
        kernel,
        out_shape=shapes[0] if single else shapes,
        in_specs=[SMEM if i in smem_in else VMEM for i in range(n_in)],
        out_specs=specs[0] if single else specs,
        scratch_shapes=list(scratch),
        cost_estimate=pl.CostEstimate(flops=flops, bytes_accessed=4 << 20, transcendentals=0),
        compiler_params=pltpu.CompilerParams(vmem_limit_bytes=limit << 20),
        name=kernel.__name__,
    )


def arr(*shape):
    return jax.ShapeDtypeStruct(shape, F32)


def exchange(value, rows, group):
    shaped = value.reshape(ND * rows // group, group, 128)
    out = lax.all_to_all(shaped, GZ, split_axis=0, concat_axis=0, tiled=True)
    return out.reshape(ND * rows, 128)


def per_device(density, kernel_hat):
    q = lax.axis_index(GZ)
    dens = density.reshape(2 * NY, NX)
    slope_y = jnp.asarray(slope_matrix(NY))
    slope_z = jnp.asarray(slope_matrix(NZ))
    slope_x = jnp.asarray(slope_matrix(NX).T.copy())
    parity = parity_matrix()

    a_out = call(gradient_kernel, arr(ND * A_ROWS, 128), 2, 400_000_000)(dens, slope_y)
    a_in = exchange(a_out, A_ROWS, 8)
    b_out = call(y_forward_kernel, arr(ND * B_ROWS, 128), 3, 300_000_000)(
        dens, jnp.asarray(parity.astype(BF16)), jnp.asarray(y_forward())
    )
    b_in = exchange(b_out, B_ROWS, 2)
    start = jnp.where(q < ND // 2, 1, 0)
    picked = lax.dynamic_slice_in_dim(kernel_hat, start, 2, axis=1)
    filt = jnp.stack([picked[:, 0], picked[:, 1], kernel_hat[:, 0]])
    weights = jnp.stack(
        [
            jnp.where(q == ND // 2, 1.0, 2.0),
            jnp.full((), 2.0),
            jnp.where(q == 0, 1.0, 0.0),
        ]
    ).astype(F32)
    field = pltpu.VMEM((2, NY, NX), F32)
    c_out, exc = call(
        xc_kernel,
        [arr(ND * A_ROWS, 128), arr(1, 1)],
        3,
        4_000_000_000,
        scratch=[field] * 4,
        smem_out=(1,),
    )(a_in, slope_z, slope_x)
    c_in = exchange(c_out, A_ROWS, 8)
    d_out = call(
        hartree_kernel,
        arr(ND * D_ROWS, 128),
        8,
        4_000_000_000,
        scratch=[
            pltpu.VMEM((3, 2, 256, 512), BF16),
            pltpu.VMEM((2, 2, 256, 512), BF16),
            pltpu.VMEM((2, 2, 128, 512), BF16),
        ],
        smem_in=(2, 3),
    )(
        b_in,
        filt,
        weights,
        exc,
        jnp.asarray(x_forward()),
        jnp.asarray(z_forward()),
        jnp.asarray(z_backward()),
        jnp.asarray(x_backward()),
    )
    d_in = exchange(d_out, D_ROWS, 4)
    v = call(divergence_kernel, arr(2 * NY, NX), 2, 500_000_000)(c_in, slope_y)
    potential, energies = call(
        potential_kernel, [arr(2 * NY, NX), arr(2)], 4, 500_000_000, smem_out=(1,)
    )(d_in, v, jnp.asarray(y_backward()), jnp.asarray(parity.T.astype(BF16)))
    return potential.reshape(2, 1, NY, NX), energies


def solution(mesh):
    torus = Mesh(mesh.devices.reshape(4, 4, 4, 2), GZ)
    placed = (P(None, GZ, None, None), P(None, GZ, None))
    return jax.shard_map(
        per_device,
        mesh=torus,
        in_specs=placed,
        out_specs=(P(None, GZ, None, None), P()),
        check_vma=False,
    )
```

```python
import math

import jax
import jax.numpy as jnp
import numpy as np
from jax import lax
from jax.experimental import pallas as pl
from jax.experimental.pallas import tpu as pltpu
from jax.sharding import Mesh
from jax.sharding import PartitionSpec as P

GZ = ("gz_0", "gz_1", "gz_2", "gz_3")
HGRID = 0.35
STENCIL = (0.8, -0.2, 4.0 / 105.0, -1.0 / 280.0)
KAPPA = 0.804
MU_X = 0.2195149727645171
BETA_C = 0.06672455060314922
GAMMA_C = 0.031090690869654894
FZ_CURV = 1.709921
PARAMS_UNPOL = (0.031091, 0.2137, 7.5957, 3.5876, 1.6382, 0.49294)
PARAMS_POL = (0.015545, 0.20548, 14.1189, 6.1977, 3.3662, 0.62517)
PARAMS_STIFF = (0.016887, 0.11125, 10.357, 3.6231, 0.88026, 0.49671)

F32 = jnp.float32
BF16 = jnp.bfloat16
NZ, NY, NX = 128, 256, 256
MZ, MY, MX = 256, 512, 512
ND = 128
HART = 16
OUT_ROWS = 26
BACK_ROWS = 27
CELLS = NZ * NY * NX
Z_CHUNK = 32
XC_ROWS = 8
NORM = 1.0 / (MX * MY * MZ)
VMEM = pl.BlockSpec(memory_space=pltpu.VMEM)
SMEM = pl.BlockSpec(memory_space=pltpu.SMEM)
HBM = pl.BlockSpec(memory_space=pltpu.HBM)


def halves(m):
    m = np.asarray(m, np.float32)
    hi = m.astype(BF16)
    lo = (m - hi.astype(np.float32)).astype(BF16)
    return np.stack([hi, lo])


def y_forward():
    y, q = np.arange(NY), np.arange(ND)
    first = np.where(q < ND // 2, 4 * q + 1, 4 * q)
    rows = []
    for ky in (first, first + 1):
        angle = 2.0 * np.pi * (np.outer(ky, y) % MY) / MY
        rows += [np.cos(angle), -np.sin(angle)]
    return halves(np.concatenate(rows, 0))


def split(value):
    hi = value.astype(BF16)
    lo = (value - hi.astype(F32)).astype(BF16)
    return hi, lo


def dot1(a, b):
    return jnp.dot(a, b, preferred_element_type=F32)


def dot3(a_hi, a_lo, b_hi, b_lo):
    return dot1(a_hi, b_hi) + (dot1(a_lo, b_hi) + dot1(a_hi, b_lo))


def put_rows(ref, row, rows, value, count=ND, scale=1):
    for half in range(value.shape[1] // 128):
        ref[pl.ds(row + half, count, stride=rows * scale), :] = value[
            :, half * 128 : half * 128 + 128
        ]


def get_rows(ref, row, rows):
    return jnp.concatenate(
        [ref[pl.ds(row + half, ND, stride=rows), :] for half in range(2)], axis=1
    )


def iota(shape, dim):
    return lax.broadcasted_iota(jnp.int32, shape, dim)


def slope_parts(n):
    offset = iota((n, n), 1) - iota((n, n), 0)
    parts = []
    coefs = halves([c / HGRID for c in STENCIL]).astype(np.float32)
    for part in range(2):
        value = jnp.zeros((n, n), F32)
        for k in range(1, 5):
            c = float(coefs[part, k - 1])
            value = jnp.where(offset == k, c, jnp.where(offset == -k, -c, value))
        parts.append(value.astype(BF16))
    return parts


def parity_matrix(transposed):
    x, place = iota((NX, NX), int(transposed)), iota((NX, NX), 1 - int(transposed))
    return jnp.where(place == (x & 1) * (NX // 2) + (x >> 1), 1.0, 0.0).astype(BF16)


def cos_sin(product):
    turn = product.astype(jnp.int32) & 511
    quarter = (turn + 64) >> 7
    angle = (turn - 128 * quarter).astype(F32) * (2.0 * math.pi / 512.0)
    sq = angle * angle
    s = angle * (
        1.0 + sq * (-1.0 / 6.0 + sq * (1.0 / 120.0 + sq * (-1.0 / 5040.0 + sq * (1.0 / 362880.0))))
    )
    c = 1.0 + sq * (-0.5 + sq * (1.0 / 24.0 + sq * (-1.0 / 720.0 + sq * (1.0 / 40320.0))))
    odd = (quarter & 1) == 1
    c, s = jnp.where(odd, s, c), jnp.where(odd, c, s)
    return (
        jnp.where(((quarter + 1) & 2) == 2, -c, c),
        jnp.where((quarter & 2) == 2, -s, s),
    )


def put_parts(ref, index, rows, cols, value):
    hi, lo = split(value)
    ref[(*index, 0, rows, cols)] = hi
    ref[(*index, 1, rows, cols)] = lo


def put_rotation(ref, index, row, c, s, transposed):
    n, m = c.shape
    top, low = slice(row, row + n), slice(row + n, row + 2 * n)
    put_parts(ref, index, top, slice(0, m), c)
    put_parts(ref, index, low, slice(m, 2 * m), c)
    put_parts(ref, index, top, slice(m, 2 * m), -s if transposed else s)
    put_parts(ref, index, low, slice(0, m), s if transposed else -s)


def float_iota(shape, dim):
    return iota(shape, dim).astype(F32)


def tables_kernel(wx_ref, wz_ref, wzi_ref, wxi_ref, yb_ref, slope_ref, slope_z_ref):
    for parity in range(2):
        shape = (NX // 2, MX // 2)
        x = 2.0 * float_iota(shape, 0) + parity
        put_rotation(wx_ref, (parity,), 0, *cos_sin(x * float_iota(shape, 1)), True)
        shape = (MX // 2, NX // 2)
        x = 2.0 * float_iota(shape, 1) + parity
        put_rotation(wxi_ref, (parity,), 0, *cos_sin(x * float_iota(shape, 0)), False)
        shape = (NZ // 2, NZ)
        z = 4.0 * float_iota(shape, 0) + 2.0 * parity
        put_rotation(wzi_ref, (parity,), 0, *cos_sin(z * float_iota(shape, 1)), True)
    for chunk in range(NZ // Z_CHUNK):
        shape = (2 * Z_CHUNK, NZ)
        row = iota(shape, 0)
        kz = chunk * Z_CHUNK + jnp.where(row < Z_CHUNK, row, row + NZ - Z_CHUNK)
        angle = 2.0 * kz.astype(F32) * float_iota(shape, 1)
        put_rotation(wz_ref, (), chunk * 4 * Z_CHUNK, *cos_sin(angle), False)
    for slot in range(2):
        shape = (NY, ND)
        q = iota(shape, 1)
        ky = 4 * q + slot + jnp.where(q < ND // 2, 1, 0)
        c, s = cos_sin(ky.astype(F32) * float_iota(shape, 0))
        weight = jnp.where(ky == MY // 2, NORM, 2.0 * NORM)
        put_parts(yb_ref, (), slice(0, NY), slice(256 * slot, 256 * slot + 128), c * weight)
        put_parts(yb_ref, (), slice(0, NY), slice(256 * slot + 128, 256 * slot + 256), -s * weight)
    for part, value in enumerate(slope_parts(NY)):
        slope_ref[part] = value
    for part, value in enumerate(slope_parts(NZ)):
        slope_z_ref[part, :, 0:NZ] = value
        slope_z_ref[part, :, NZ : 2 * NZ] = value


def outward_kernel(dens_hbm, table_hbm, out_ref, dens_ref, table_ref, sems):
    dens_copy = pltpu.make_async_copy(dens_hbm, dens_ref, sems.at[0])
    table_copy = pltpu.make_async_copy(table_hbm, table_ref, sems.at[1])
    dens_copy.start()
    table_copy.start()
    slope = slope_parts(NY)
    parity = parity_matrix(False)
    dens_copy.wait()
    for spin in range(2):
        field = dens_ref[spin * NY : (spin + 1) * NY, :]
        grad = dot3(*slope, *split(field))
        for part in range(2):
            rows = slice(part * 128, part * 128 + 128)
            put_rows(out_ref, spin * 4 + part * 2, OUT_ROWS, field[rows])
            put_rows(out_ref, 8 + spin * 4 + part * 2, OUT_ROWS, grad[rows])
    hi, lo = split(dens_ref[0:NY, :] + dens_ref[NY : 2 * NY, :])
    hi, lo = dot1(hi, parity), dot1(lo, parity)
    mean_row = jnp.sum(hi + lo, axis=0, keepdims=True)
    put_rows(out_ref, HART + 8, OUT_ROWS, jnp.broadcast_to(mean_row, (ND, NX)))
    hi, lo = hi.astype(BF16), lo.astype(BF16)
    table_copy.wait()
    for s in range(4):
        rows = slice(s * ND, (s + 1) * ND)
        value = dot3(table_ref[0, rows, :], table_ref[1, rows, :], hi, lo)
        put_rows(out_ref, HART + s * 2, OUT_ROWS, value)


def pw_piece(root, params):
    radius = root * root
    scale = 2.0 * params[0]
    series = root * (
        scale * params[2]
        + root * (scale * params[3] + root * (scale * params[4] + root * (scale * params[5])))
    )
    slope = root * (
        0.5 * scale * params[2]
        + root
        * (
            scale * params[3]
            + root * (1.5 * scale * params[4] + root * (2.0 * scale * params[5]))
        )
    )
    inv = 1.0 / (series * (series + 1.0))
    logarithm = jnp.log(1.0 + inv * (series + 1.0))
    front = -scale - (scale * params[1]) * radius
    value = front * logarithm
    deriv = (-scale * params[1]) * radius * logarithm - front * slope * inv
    return value, deriv


def exchange_piece(dens, inv_root, sigma):
    root = 2.0 * dens * inv_root * inv_root
    inv2 = inv_root * inv_root
    inv4 = inv2 * inv2
    reduced = sigma * (inv4 * inv4) * (1.0 / (3.0 * math.pi**2) ** (2.0 / 3.0))
    damp = 1.0 / (1.0 + (MU_X / KAPPA) * reduced)
    enhance = (1.0 + KAPPA) - KAPPA * damp
    front = -0.75 * (3.0 / math.pi) ** (1.0 / 3.0)
    damp_sq = MU_X * damp * damp
    energy = front * dens * root * enhance
    d_dens = (4.0 / 3.0 * front) * root * (enhance - 2.0 * reduced * damp_sq)
    d_sigma = (0.5 * front / (3.0 * math.pi**2) ** (2.0 / 3.0)) * damp_sq * inv4
    return energy, d_dens, d_sigma, root


def xc_point(up, down, sigma_uu, sigma_ud, sigma_dd):
    inv_up = jnp.exp(jnp.log(2.0 * up) * (-1.0 / 3.0))
    inv_down = jnp.exp(jnp.log(2.0 * down) * (-1.0 / 3.0))
    e_up, d_up, d_uu, root_up = exchange_piece(up, inv_up, sigma_uu)
    e_down, d_down, d_dd, root_down = exchange_piece(down, inv_down, sigma_dd)
    dens = up + down
    sixth = jnp.exp(jnp.log(dens) * (-1.0 / 6.0))
    inv_third = sixth * sixth
    third = dens * inv_third * inv_third
    inv_dens = inv_third * inv_third * inv_third
    zeta = (up - down) * inv_dens
    plus = 2.0 * up * inv_dens
    minus = 2.0 * down * inv_dens
    plus_cube = root_up * inv_third
    minus_cube = root_down * inv_third
    f_scale = 1.0 / (2.0 ** (4.0 / 3.0) - 2.0)
    f = (plus * plus_cube + minus * minus_cube - 2.0) * f_scale
    f_slope = (plus_cube - minus_cube) * (4.0 / 3.0 * f_scale)
    root = (3.0 / (4.0 * math.pi)) ** (1.0 / 6.0) * sixth
    e0, e0_d = pw_piece(root, PARAMS_UNPOL)
    e1, e1_d = pw_piece(root, PARAMS_POL)
    ac, ac_d = pw_piece(root, PARAMS_STIFF)
    z2 = zeta * zeta
    z3_4 = 4.0 * z2 * zeta
    z4 = z2 * z2
    one_z4 = (1.0 - z4) * (-1.0 / FZ_CURV)
    f_z4 = f * z4
    f_one = f * one_z4
    diff = e1 - e0
    local = e0 + ac * f_one + diff * f_z4
    local_r = e0_d + ac_d * f_one + (e1_d - e0_d) * f_z4
    fz3 = z3_4 * f
    local_z = ac * (f_slope * one_z4 + (1.0 / FZ_CURV) * fz3) + diff * (f_slope * z4 + fz3)
    phi = 0.5 * (plus_cube * plus_cube + minus_cube * minus_cube)
    inv_phi = 1.0 / phi
    phi_log_slope = (third * (1.0 / 3.0)) * (inv_up - inv_down) * inv_phi
    g3 = GAMMA_C * phi * phi * phi
    inv_g3 = (1.0 / GAMMA_C) * inv_phi * inv_phi * inv_phi
    grow = jnp.exp(-local * inv_g3)
    weight_a = (BETA_C / GAMMA_C) / (grow - 1.0)
    sigma = sigma_uu + 2.0 * sigma_ud + sigma_dd
    ct = math.pi / (16.0 * (3.0 * math.pi**2) ** (1.0 / 3.0))
    kt = ct * inv_third * inv_dens * inv_dens * inv_phi * inv_phi
    t2 = sigma * kt
    w = weight_a * t2
    num = 1.0 + w
    den = num + w * w
    add = (BETA_C / GAMMA_C) * t2 * num
    both = den + add
    inv_both = 1.0 / (den * both)
    h = g3 * jnp.log(1.0 + add * (inv_both * both))
    h_t = (BETA_C / GAMMA_C) * g3 * (1.0 + 2.0 * w) * inv_both
    h_a = -(w * w * w) * (2.0 + w) * grow * inv_both
    total = local + h
    ht_t2 = h_t * t2
    one_ha = 1.0 + h_a
    d_n = total - (1.0 / 3.0) * one_ha * local_r - (7.0 / 3.0) * ht_t2
    d_z = one_ha * local_z + phi_log_slope * (3.0 * (h - h_a * local) - 2.0 * ht_t2)
    d_sigma = dens * h_t * kt
    energy = e_up + e_down + dens * total
    return (
        energy,
        d_up + d_n + minus * d_z,
        d_down + d_n - plus * d_z,
        d_uu + d_sigma,
        2.0 * d_sigma,
        d_dd + d_sigma,
    )


def slope_along_z(slope_z_ref, hi, lo):
    both = jnp.concatenate([hi, lo], axis=0)
    return dot1(slope_z_ref[0], both) + dot1(slope_z_ref[1], both)


def slope_along_x(slope_ref, hi, lo):
    return -dot3(hi, lo, slope_ref[0], slope_ref[1])


def xc_part(in_ref, slope_ref, slope_z_ref, out_ref, dens, gz, gy, gx):
    for spin in range(2):
        for part in range(2):
            rows = slice(part * 128, part * 128 + 128)
            field = get_rows(in_ref, spin * 4 + part * 2, OUT_ROWS)
            dens[spin, rows, :] = field
            gy[spin, rows, :] = get_rows(in_ref, 8 + spin * 4 + part * 2, OUT_ROWS)
            hi, lo = split(field)
            gz[spin, rows, :] = slope_along_z(slope_z_ref, hi, lo)
            gx[spin, rows, :] = slope_along_x(slope_ref, hi, lo)

    def chunk(i, total):
        rows = pl.ds(pl.multiple_of(i * XC_ROWS, XC_ROWS), XC_ROWS)
        zu, zd = gz[0, rows, :], gz[1, rows, :]
        yu, yd = gy[0, rows, :], gy[1, rows, :]
        xu, xd = gx[0, rows, :], gx[1, rows, :]
        energy, d_up, d_down, d_uu, d_ud, d_dd = xc_point(
            dens[0, rows, :],
            dens[1, rows, :],
            zu * zu + yu * yu + xu * xu,
            zu * zd + yu * yd + xu * xd,
            zd * zd + yd * yd + xd * xd,
        )
        dens[0, rows, :] = d_up
        dens[1, rows, :] = d_down
        for ref, gu, gd in ((gz, zu, zd), (gy, yu, yd), (gx, xu, xd)):
            ref[0, rows, :] = 2.0 * d_uu * gu + d_ud * gd
            ref[1, rows, :] = 2.0 * d_dd * gd + d_ud * gu
        return total + energy

    total = lax.fori_loop(0, 256 // XC_ROWS, chunk, jnp.zeros((XC_ROWS, NX), F32))
    for spin in range(2):
        for part in range(2):
            rows = slice(part * 128, part * 128 + 128)
            div = slope_along_z(slope_z_ref, *split(gz[spin, rows, :]))
            div = div + slope_along_x(slope_ref, *split(gx[spin, rows, :]))
            put_rows(out_ref, spin * 4 + part * 2, BACK_ROWS, dens[spin, rows, :] - div)
            put_rows(out_ref, 8 + spin * 4 + part * 2, BACK_ROWS, gy[spin, rows, :])
    return jnp.sum(total)


def hartree_part(
    in_ref, filt_ref, weight_ref, wx_ref, wz_ref, wzi_ref, wxi_ref, out_ref, xp, sums, back
):
    even = [in_ref[pl.ds(r, ND, stride=OUT_ROWS), :] for r in range(HART, OUT_ROWS, 2)]
    odd = [in_ref[pl.ds(r, ND, stride=OUT_ROWS), :] for r in range(HART + 1, OUT_ROWS, 2)]
    zero = jnp.zeros((ND, 128), F32)
    even.append(zero)
    odd.append(zero)
    for slot in range(3):
        parts = []
        for parity, source in ((0, even), (1, odd)):
            hi, lo = split(jnp.concatenate(source[2 * slot : 2 * slot + 2], axis=1))
            parts.append(dot3(hi, lo, wx_ref[parity, 0], wx_ref[parity, 1]))
        for half, value in ((0, parts[0] + parts[1]), (1, parts[0] - parts[1])):
            cols = slice(half * 256, half * 256 + 256)
            hi, lo = split(value)
            xp[slot, 0, 0:128, cols] = hi[:, 0:256]
            xp[slot, 0, 128:256, cols] = hi[:, 256:512]
            xp[slot, 1, 0:128, cols] = lo[:, 0:256]
            xp[slot, 1, 128:256, cols] = lo[:, 256:512]
    energy = jnp.zeros((8, MX), F32)
    for slot in range(3):
        weight = weight_ref[slot]

        def chunk(c, acc, slot=slot):
            rows = pl.ds(pl.multiple_of(c * 128, 128), 128)
            spec = dot3(wz_ref[0, rows, :], wz_ref[1, rows, :], xp[slot, 0], xp[slot, 1])
            low = pl.ds(pl.multiple_of(c * Z_CHUNK, Z_CHUNK), Z_CHUNK)
            high = pl.ds(pl.multiple_of(NZ + c * Z_CHUNK, Z_CHUNK), Z_CHUNK)
            f_low, f_high = filt_ref[slot, low, :], filt_ref[slot, high, :]
            for kind in range(2):
                a = spec[kind * 64 : kind * 64 + 32]
                b = spec[kind * 64 + 32 : kind * 64 + 64]
                fa, fb = a * f_low, b * f_high
                power = a * fa + b * fb
                acc = acc + (power[0:8] + power[8:16] + power[16:24] + power[24:32])
                dest = pl.ds(pl.multiple_of(kind * NZ + c * Z_CHUNK, Z_CHUNK), Z_CHUNK)
                for parity, value in ((0, fa + fb), (1, fa - fb)):
                    hi, lo = split(value)
                    sums[parity, 0, dest, :] = hi
                    sums[parity, 1, dest, :] = lo
            return acc

        acc = lax.fori_loop(0, NZ // Z_CHUNK, chunk, jnp.zeros((8, MX), F32))
        energy = energy + weight * acc
        for parity in range(2):
            grid = dot3(
                wzi_ref[parity, 0], wzi_ref[parity, 1], sums[parity, 0], sums[parity, 1]
            )
            for sign in range(2):
                a, b = grid[:, 0:256], grid[:, 256:512]
                hi, lo = split(a + b if sign == 0 else a - b)
                for part, value in ((0, hi), (1, lo)):
                    rows = slice(parity * 64, parity * 64 + 64)
                    back[sign, part, rows, 0:256] = value[0:64]
                    back[sign, part, rows, 256:512] = value[64:128]
        for sign in range(2):
            value = dot3(back[sign, 0], back[sign, 1], wxi_ref[sign, 0], wxi_ref[sign, 1])
            for parity in range(2):
                for kind in range(2 if slot < 2 else 1):
                    put_rows(
                        out_ref,
                        parity * BACK_ROWS + HART + slot * 4 + kind * 2 + sign,
                        BACK_ROWS,
                        value[parity * 64 : parity * 64 + 64, kind * 128 : kind * 128 + 128],
                        count=64,
                        scale=2,
                    )
    return jnp.sum(energy)


def middle_kernel(
    first_ref, weight_ref, in_ref, slope_ref, slope_z_ref, filt_hbm, wx_hbm, wz_hbm, wzi_hbm, wxi_hbm,
    out_ref, filt_ref, wx_ref, wz_ref, wzi_ref, wxi_ref, dens, gz, gy, gx, xp, sums, back, sems,
):
    first = first_ref[0]
    moves = [
        (filt_hbm.at[:, place, :], filt_ref.at[slot])
        for slot, place in enumerate((first, first + 1, 0))
    ]
    moves += [(wx_hbm, wx_ref), (wz_hbm, wz_ref), (wzi_hbm, wzi_ref), (wxi_hbm, wxi_ref)]
    copies = [
        pltpu.make_async_copy(source, target, sems.at[i]) for i, (source, target) in enumerate(moves)
    ]
    for copy in copies:
        copy.start()
    exc = xc_part(in_ref, slope_ref, slope_z_ref, out_ref, dens, gz, gy, gx)
    for copy in copies:
        copy.wait()
    power = hartree_part(
        in_ref, filt_ref, weight_ref, wx_ref, wz_ref, wzi_ref, wxi_ref, out_ref, xp, sums, back
    )
    energies = jnp.where(iota((ND, 128), 1) < 64, exc, power)
    put_rows(out_ref, BACK_ROWS - 1, BACK_ROWS, energies)


def homeward_kernel(in_ref, yb_ref, slope_ref, out_ref, energy_ref):
    field = jnp.concatenate(
        [get_rows(in_ref, HART + 2 * s, BACK_ROWS) for s in range(4)], axis=0
    )
    grid = dot3(yb_ref[0], yb_ref[1], *split(field))
    mean_row = jnp.concatenate(
        [in_ref[HART + 8 : HART + 9, :], in_ref[HART + 9 : HART + 10, :]], axis=1
    )
    grid = grid + mean_row * NORM
    hi, lo = split(grid)
    parity = parity_matrix(True)
    hartree = dot1(hi, parity) + dot1(lo, parity)
    for spin in range(2):
        flux, rest = (
            jnp.concatenate(
                [get_rows(in_ref, base + spin * 4 + part * 2, BACK_ROWS) for part in range(2)],
                axis=0,
            )
            for base in (8, 0)
        )
        rows = slice(spin * NY, (spin + 1) * NY)
        out_ref[rows, :] = rest + hartree - dot3(slope_ref[0], slope_ref[1], *split(flux))
    row = jnp.sum(in_ref[pl.ds(BACK_ROWS - 1, ND, stride=BACK_ROWS), :], axis=0, keepdims=True)
    first = iota((1, 128), 1) < 64
    energy_ref[0] = jnp.sum(jnp.where(first, row, 0.0)) * (1.0 / (64.0 * CELLS))
    energy_ref[1] = jnp.sum(jnp.where(first, 0.0, row)) * (0.5 * NORM / (64.0 * CELLS))


def call(kernel, outs, in_specs, flops, scratch=(), smem_out=(), limit=40):
    specs = [SMEM if i in smem_out else VMEM for i in range(len(outs))]
    return pl.pallas_call(
        kernel,
        out_shape=list(outs),
        in_specs=in_specs,
        out_specs=specs,
        scratch_shapes=list(scratch),
        cost_estimate=pl.CostEstimate(flops=flops, bytes_accessed=4 << 20, transcendentals=0),
        compiler_params=pltpu.CompilerParams(vmem_limit_bytes=limit << 20),
        name=kernel.__name__,
    )


def in_hbm(value):
    return pltpu.with_memory_space_constraint(value, pltpu.HBM)


def arr(*shape, dtype=F32):
    return jax.ShapeDtypeStruct(shape, dtype)


def exchange(value, rows, group):
    shaped = value.reshape(ND * rows // group, group, 128)
    out = lax.all_to_all(shaped, GZ, split_axis=0, concat_axis=0, tiled=True)
    return out.reshape(ND * rows, 128)


def per_device(density, kernel_hat):
    q = lax.axis_index(GZ)
    (outward,) = call(
        outward_kernel,
        [arr(ND * OUT_ROWS, 128)],
        [HBM, HBM],
        400_000_000,
        scratch=[
            pltpu.VMEM((2 * NY, NX), F32),
            pltpu.VMEM((2, 4 * ND, NY), BF16),
            pltpu.SemaphoreType.DMA((2,)),
        ],
    )(in_hbm(density.reshape(2 * NY, NX)), in_hbm(jnp.asarray(y_forward())))
    arrived = exchange(outward, OUT_ROWS, 2)
    shapes = [(2, 2, NX, MX), (2, 2 * MZ, 2 * NZ), (2, 2, NZ, 2 * NZ), (2, 2, MX, NX)]
    wx, wz, wzi, wxi, yb, slope, slope_z = call(
        tables_kernel,
        [arr(*shape, dtype=BF16) for shape in shapes]
        + [
            arr(2, NY, 4 * ND, dtype=BF16),
            arr(2, NY, NY, dtype=BF16),
            arr(2, NZ, 2 * NZ, dtype=BF16),
        ],
        [],
        2_000_000_000,
    )()
    start = jnp.where(q < ND // 2, 1, 0).astype(jnp.int32).reshape(1)
    weights = jnp.stack(
        [
            jnp.where(q == ND // 2, 1.0, 2.0),
            jnp.full((), 2.0),
            jnp.where(q == 0, 1.0, 0.0),
        ]
    ).astype(F32)
    field = pltpu.VMEM((2, 256, NX), F32)
    (back,) = call(
        middle_kernel,
        [arr(ND * BACK_ROWS, 128)],
        [SMEM, SMEM] + [VMEM] * 3 + [HBM] * 5,
        8_000_000_000,
        scratch=[pltpu.VMEM((3, MZ, MX), F32)]
        + [pltpu.VMEM(shape, BF16) for shape in shapes]
        + [field] * 4
        + [
            pltpu.VMEM((3, 2, 256, 512), BF16),
            pltpu.VMEM((2, 2, 256, 512), BF16),
            pltpu.VMEM((2, 2, 128, 512), BF16),
            pltpu.SemaphoreType.DMA((7,)),
        ],
    )(start, weights, arrived, slope, slope_z, *map(in_hbm, (kernel_hat, wx, wz, wzi, wxi)))
    returned = exchange(back, BACK_ROWS, 1)
    potential, energies = call(
        homeward_kernel,
        [arr(2 * NY, NX), arr(2)],
        [VMEM] * 3,
        1_000_000_000,
        smem_out=(1,),
    )(returned, yb, slope)
    return potential.reshape(2, 1, NY, NX), energies


def solution(mesh):
    torus = Mesh(mesh.devices.reshape(4, 4, 4, 2), GZ)
    placed = (P(None, GZ, None, None), P(None, GZ, None))
    return jax.shard_map(
        per_device,
        mesh=torus,
        in_specs=placed,
        out_specs=(P(None, GZ, None, None), P()),
        check_vma=False,
    )
```

```python
import math

import jax
import jax.numpy as jnp
import numpy as np
from jax import lax
from jax.experimental import pallas as pl
from jax.experimental.pallas import tpu as pltpu
from jax.sharding import Mesh
from jax.sharding import PartitionSpec as P

GZ = ("gz_0", "gz_1", "gz_2", "gz_3")
HGRID = 0.35
STENCIL = (0.8, -0.2, 4.0 / 105.0, -1.0 / 280.0)
KAPPA = 0.804
MU_X = 0.2195149727645171
BETA_C = 0.06672455060314922
GAMMA_C = 0.031090690869654894
FZ_CURV = 1.709921
PARAMS_UNPOL = (0.031091, 0.2137, 7.5957, 3.5876, 1.6382, 0.49294)
PARAMS_POL = (0.015545, 0.20548, 14.1189, 6.1977, 3.3662, 0.62517)
PARAMS_STIFF = (0.016887, 0.11125, 10.357, 3.6231, 0.88026, 0.49671)

F32 = jnp.float32
BF16 = jnp.bfloat16
NZ, NY, NX = 128, 256, 256
MZ, MY, MX = 256, 512, 512
ND = 128
HART = 16
OUT_ROWS = 26
BACK_ROWS = 27
CELLS = NZ * NY * NX
Z_CHUNK = 32
XC_ROWS = 8
XC_AHEAD = 6
XC_SPREAD = 27
NORM = 1.0 / (MX * MY * MZ)
VMEM = pl.BlockSpec(memory_space=pltpu.VMEM)
SMEM = pl.BlockSpec(memory_space=pltpu.SMEM)
HBM = pl.BlockSpec(memory_space=pltpu.HBM)


def halves(m):
    m = np.asarray(m, np.float32)
    hi = m.astype(BF16)
    lo = (m - hi.astype(np.float32)).astype(BF16)
    return np.stack([hi, lo])


def y_forward():
    y, q = np.arange(NY), np.arange(ND)
    first = np.where(q < ND // 2, 4 * q + 1, 4 * q)
    rows = []
    for ky in (first, first + 1):
        angle = 2.0 * np.pi * (np.outer(ky, y) % MY) / MY
        rows += [np.cos(angle), -np.sin(angle)]
    return halves(np.concatenate(rows, 0))


def split(value):
    hi = value.astype(BF16)
    lo = (value - hi.astype(F32)).astype(BF16)
    return hi, lo


def dot1(a, b):
    return jnp.dot(a, b, preferred_element_type=F32)


def dot3(a_hi, a_lo, b_hi, b_lo):
    return dot1(a_hi, b_hi) + (dot1(a_lo, b_hi) + dot1(a_hi, b_lo))


def put_rows(ref, row, rows, value, count=ND, scale=1):
    for half in range(value.shape[1] // 128):
        ref[pl.ds(row + half, count, stride=rows * scale), :] = value[
            :, half * 128 : half * 128 + 128
        ]


def get_rows(ref, row, rows):
    return jnp.concatenate(
        [ref[pl.ds(row + half, ND, stride=rows), :] for half in range(2)], axis=1
    )


def iota(shape, dim):
    return lax.broadcasted_iota(jnp.int32, shape, dim)


def slope_parts(n):
    offset = iota((n, n), 1) - iota((n, n), 0)
    parts = []
    coefs = halves([c / HGRID for c in STENCIL]).astype(np.float32)
    for part in range(2):
        value = jnp.zeros((n, n), F32)
        for k in range(1, 5):
            c = float(coefs[part, k - 1])
            value = jnp.where(offset == k, c, jnp.where(offset == -k, -c, value))
        parts.append(value.astype(BF16))
    return parts


def parity_matrix(transposed):
    x, place = iota((NX, NX), int(transposed)), iota((NX, NX), 1 - int(transposed))
    return jnp.where(place == (x & 1) * (NX // 2) + (x >> 1), 1.0, 0.0).astype(BF16)


def cos_sin(product):
    turn = product.astype(jnp.int32) & 511
    quarter = (turn + 64) >> 7
    angle = (turn - 128 * quarter).astype(F32) * (2.0 * math.pi / 512.0)
    sq = angle * angle
    s = angle * (
        1.0 + sq * (-1.0 / 6.0 + sq * (1.0 / 120.0 + sq * (-1.0 / 5040.0 + sq * (1.0 / 362880.0))))
    )
    c = 1.0 + sq * (-0.5 + sq * (1.0 / 24.0 + sq * (-1.0 / 720.0 + sq * (1.0 / 40320.0))))
    odd = (quarter & 1) == 1
    c, s = jnp.where(odd, s, c), jnp.where(odd, c, s)
    return (
        jnp.where(((quarter + 1) & 2) == 2, -c, c),
        jnp.where((quarter & 2) == 2, -s, s),
    )


def put_parts(ref, index, rows, cols, value):
    hi, lo = split(value)
    ref[(*index, 0, rows, cols)] = hi
    ref[(*index, 1, rows, cols)] = lo


def put_rotation(ref, index, row, c, s, transposed):
    n, m = c.shape
    top, low = slice(row, row + n), slice(row + n, row + 2 * n)
    put_parts(ref, index, top, slice(0, m), c)
    put_parts(ref, index, low, slice(m, 2 * m), c)
    put_parts(ref, index, top, slice(m, 2 * m), -s if transposed else s)
    put_parts(ref, index, low, slice(0, m), s if transposed else -s)


def float_iota(shape, dim):
    return iota(shape, dim).astype(F32)


def tables_kernel(wx_ref, wz_ref, wzi_ref, wxi_ref, yb_ref, slope_ref, slope_z_ref):
    for parity in range(2):
        shape = (NX // 2, MX // 2)
        x = 2.0 * float_iota(shape, 0) + parity
        put_rotation(wx_ref, (parity,), 0, *cos_sin(x * float_iota(shape, 1)), True)
        shape = (MX // 2, NX // 2)
        x = 2.0 * float_iota(shape, 1) + parity
        put_rotation(wxi_ref, (parity,), 0, *cos_sin(x * float_iota(shape, 0)), False)
        shape = (NZ // 2, NZ)
        z = 4.0 * float_iota(shape, 0) + 2.0 * parity
        put_rotation(wzi_ref, (parity,), 0, *cos_sin(z * float_iota(shape, 1)), True)
    for chunk in range(NZ // Z_CHUNK):
        shape = (2 * Z_CHUNK, NZ)
        row = iota(shape, 0)
        kz = chunk * Z_CHUNK + jnp.where(row < Z_CHUNK, row, row + NZ - Z_CHUNK)
        angle = 2.0 * kz.astype(F32) * float_iota(shape, 1)
        put_rotation(wz_ref, (), chunk * 4 * Z_CHUNK, *cos_sin(angle), False)
    for slot in range(2):
        shape = (NY, ND)
        q = iota(shape, 1)
        ky = 4 * q + slot + jnp.where(q < ND // 2, 1, 0)
        c, s = cos_sin(ky.astype(F32) * float_iota(shape, 0))
        weight = jnp.where(ky == MY // 2, NORM, 2.0 * NORM)
        put_parts(yb_ref, (), slice(0, NY), slice(256 * slot, 256 * slot + 128), c * weight)
        put_parts(yb_ref, (), slice(0, NY), slice(256 * slot + 128, 256 * slot + 256), -s * weight)
    for part, value in enumerate(slope_parts(NY)):
        slope_ref[part] = value
    for part, value in enumerate(slope_parts(NZ)):
        slope_z_ref[part, :, 0:NZ] = value
        slope_z_ref[part, :, NZ : 2 * NZ] = value


def outward_kernel(dens_hbm, table_hbm, out_ref, dens_ref, table_ref, sems):
    dens_copy = pltpu.make_async_copy(dens_hbm, dens_ref, sems.at[0])
    table_copy = pltpu.make_async_copy(table_hbm, table_ref, sems.at[1])
    dens_copy.start()
    table_copy.start()
    slope = slope_parts(NY)
    parity = parity_matrix(False)
    dens_copy.wait()
    for spin in range(2):
        field = dens_ref[spin * NY : (spin + 1) * NY, :]
        grad = dot3(*slope, *split(field))
        for part in range(2):
            rows = slice(part * 128, part * 128 + 128)
            put_rows(out_ref, spin * 4 + part * 2, OUT_ROWS, field[rows])
            put_rows(out_ref, 8 + spin * 4 + part * 2, OUT_ROWS, grad[rows])
    hi, lo = split(dens_ref[0:NY, :] + dens_ref[NY : 2 * NY, :])
    hi, lo = dot1(hi, parity), dot1(lo, parity)
    mean_row = jnp.sum(hi + lo, axis=0, keepdims=True)
    put_rows(out_ref, HART + 8, OUT_ROWS, jnp.broadcast_to(mean_row, (ND, NX)))
    hi, lo = hi.astype(BF16), lo.astype(BF16)
    table_copy.wait()
    for s in range(4):
        rows = slice(s * ND, (s + 1) * ND)
        value = dot3(table_ref[0, rows, :], table_ref[1, rows, :], hi, lo)
        put_rows(out_ref, HART + s * 2, OUT_ROWS, value)


def pw_piece(root, params):
    radius = root * root
    scale = 2.0 * params[0]
    series = root * (
        scale * params[2]
        + root * (scale * params[3] + root * (scale * params[4] + root * (scale * params[5])))
    )
    slope = root * (
        0.5 * scale * params[2]
        + root
        * (
            scale * params[3]
            + root * (1.5 * scale * params[4] + root * (2.0 * scale * params[5]))
        )
    )
    inv = 1.0 / (series * (series + 1.0))
    logarithm = jnp.log(1.0 + inv * (series + 1.0))
    front = -scale - (scale * params[1]) * radius
    value = front * logarithm
    deriv = (-scale * params[1]) * radius * logarithm - front * slope * inv
    return value, deriv


def exchange_piece(dens, inv_root, sigma):
    root = 2.0 * dens * inv_root * inv_root
    inv2 = inv_root * inv_root
    inv4 = inv2 * inv2
    reduced = sigma * (inv4 * inv4) * (1.0 / (3.0 * math.pi**2) ** (2.0 / 3.0))
    damp = 1.0 / (1.0 + (MU_X / KAPPA) * reduced)
    enhance = (1.0 + KAPPA) - KAPPA * damp
    front = -0.75 * (3.0 / math.pi) ** (1.0 / 3.0)
    damp_sq = MU_X * damp * damp
    energy = front * dens * root * enhance
    d_dens = (4.0 / 3.0 * front) * root * (enhance - 2.0 * reduced * damp_sq)
    d_sigma = (0.5 * front / (3.0 * math.pi**2) ** (2.0 / 3.0)) * damp_sq * inv4
    return energy, d_dens, d_sigma, root


def xc_point(up, down, sigma_uu, sigma_ud, sigma_dd):
    inv_up = jnp.exp(jnp.log(2.0 * up) * (-1.0 / 3.0))
    inv_down = jnp.exp(jnp.log(2.0 * down) * (-1.0 / 3.0))
    e_up, d_up, d_uu, root_up = exchange_piece(up, inv_up, sigma_uu)
    e_down, d_down, d_dd, root_down = exchange_piece(down, inv_down, sigma_dd)
    dens = up + down
    sixth = jnp.exp(jnp.log(dens) * (-1.0 / 6.0))
    inv_third = sixth * sixth
    third = dens * inv_third * inv_third
    inv_dens = inv_third * inv_third * inv_third
    zeta = (up - down) * inv_dens
    plus = 2.0 * up * inv_dens
    minus = 2.0 * down * inv_dens
    plus_cube = root_up * inv_third
    minus_cube = root_down * inv_third
    f_scale = 1.0 / (2.0 ** (4.0 / 3.0) - 2.0)
    f = (plus * plus_cube + minus * minus_cube - 2.0) * f_scale
    f_slope = (plus_cube - minus_cube) * (4.0 / 3.0 * f_scale)
    root = (3.0 / (4.0 * math.pi)) ** (1.0 / 6.0) * sixth
    e0, e0_d = pw_piece(root, PARAMS_UNPOL)
    e1, e1_d = pw_piece(root, PARAMS_POL)
    ac, ac_d = pw_piece(root, PARAMS_STIFF)
    z2 = zeta * zeta
    z3_4 = 4.0 * z2 * zeta
    z4 = z2 * z2
    one_z4 = (1.0 - z4) * (-1.0 / FZ_CURV)
    f_z4 = f * z4
    f_one = f * one_z4
    diff = e1 - e0
    local = e0 + ac * f_one + diff * f_z4
    local_r = e0_d + ac_d * f_one + (e1_d - e0_d) * f_z4
    fz3 = z3_4 * f
    local_z = ac * (f_slope * one_z4 + (1.0 / FZ_CURV) * fz3) + diff * (f_slope * z4 + fz3)
    phi = 0.5 * (plus_cube * plus_cube + minus_cube * minus_cube)
    inv_phi = 1.0 / phi
    phi_log_slope = (third * (1.0 / 3.0)) * (inv_up - inv_down) * inv_phi
    g3 = GAMMA_C * phi * phi * phi
    inv_g3 = (1.0 / GAMMA_C) * inv_phi * inv_phi * inv_phi
    grow = jnp.exp(-local * inv_g3)
    weight_a = (BETA_C / GAMMA_C) / (grow - 1.0)
    sigma = sigma_uu + 2.0 * sigma_ud + sigma_dd
    ct = math.pi / (16.0 * (3.0 * math.pi**2) ** (1.0 / 3.0))
    kt = ct * inv_third * inv_dens * inv_dens * inv_phi * inv_phi
    t2 = sigma * kt
    w = weight_a * t2
    num = 1.0 + w
    den = num + w * w
    add = (BETA_C / GAMMA_C) * t2 * num
    both = den + add
    inv_both = 1.0 / (den * both)
    h = g3 * jnp.log(1.0 + add * (inv_both * both))
    h_t = (BETA_C / GAMMA_C) * g3 * (1.0 + 2.0 * w) * inv_both
    h_a = -(w * w * w) * (2.0 + w) * grow * inv_both
    total = local + h
    ht_t2 = h_t * t2
    one_ha = 1.0 + h_a
    d_n = total - (1.0 / 3.0) * one_ha * local_r - (7.0 / 3.0) * ht_t2
    d_z = one_ha * local_z + phi_log_slope * (3.0 * (h - h_a * local) - 2.0 * ht_t2)
    d_sigma = dens * h_t * kt
    energy = e_up + e_down + dens * total
    return (
        energy,
        d_up + d_n + minus * d_z,
        d_down + d_n - plus * d_z,
        d_uu + d_sigma,
        2.0 * d_sigma,
        d_dd + d_sigma,
    )


def slope_along_z(slope_z_ref, hi, lo):
    both = jnp.concatenate([hi, lo], axis=0)
    return dot1(slope_z_ref[0], both) + dot1(slope_z_ref[1], both)


def slope_along_x(slope_ref, hi, lo):
    return -dot3(hi, lo, slope_ref[0], slope_ref[1])


def xc_steps(in_ref, slope_ref, slope_z_ref, out_ref, total_ref, dens, gz, gy, gx):
    def gradients(part):
        rows = slice(part * 128, part * 128 + 128)
        for spin in range(2):
            field = get_rows(in_ref, spin * 4 + part * 2, OUT_ROWS)
            dens[spin, rows, :] = field
            gy[spin, rows, :] = get_rows(in_ref, 8 + spin * 4 + part * 2, OUT_ROWS)
            hi, lo = split(field)
            gz[spin, rows, :] = slope_along_z(slope_z_ref, hi, lo)
            gx[spin, rows, :] = slope_along_x(slope_ref, hi, lo)

    def points(i):
        rows = slice(i * XC_ROWS, (i + 1) * XC_ROWS)
        zu, zd = gz[0, rows, :], gz[1, rows, :]
        yu, yd = gy[0, rows, :], gy[1, rows, :]
        xu, xd = gx[0, rows, :], gx[1, rows, :]
        energy, d_up, d_down, d_uu, d_ud, d_dd = xc_point(
            dens[0, rows, :],
            dens[1, rows, :],
            zu * zu + yu * yu + xu * xu,
            zu * zd + yu * yd + xu * xd,
            zd * zd + yd * yd + xd * xd,
        )
        dens[0, rows, :] = d_up
        dens[1, rows, :] = d_down
        for ref, gu, gd in ((gz, zu, zd), (gy, yu, yd), (gx, xu, xd)):
            ref[0, rows, :] = 2.0 * d_uu * gu + d_ud * gd
            ref[1, rows, :] = 2.0 * d_dd * gd + d_ud * gu
        folded = sum(energy[r : r + 8] for r in range(0, XC_ROWS, 8))
        total_ref[...] = folded if i == 0 else total_ref[...] + folded

    def divergence(part):
        rows = slice(part * 128, part * 128 + 128)
        for spin in range(2):
            div = slope_along_z(slope_z_ref, *split(gz[spin, rows, :]))
            div = div + slope_along_x(slope_ref, *split(gx[spin, rows, :]))
            put_rows(out_ref, spin * 4 + part * 2, BACK_ROWS, dens[spin, rows, :] - div)
            put_rows(out_ref, 8 + spin * 4 + part * 2, BACK_ROWS, gy[spin, rows, :])

    steps = []
    for part in range(2):
        steps.append(lambda part=part: gradients(part))
        for i in range(part * 128 // XC_ROWS, (part + 1) * 128 // XC_ROWS):
            steps.append(lambda i=i: points(i))
        steps.append(lambda part=part: divergence(part))
    return steps


def hartree_steps(
    in_ref, filt_ref, weight_ref, wx_ref, wz_ref, wzi_ref, wxi_ref, out_ref, power_ref, xp, sums, back
):
    def forward_x(slot):
        parts = []
        for parity in range(2):
            base = HART + 4 * slot + parity
            real = in_ref[pl.ds(base, ND, stride=OUT_ROWS), :]
            if slot < 2:
                imag = in_ref[pl.ds(base + 2, ND, stride=OUT_ROWS), :]
            else:
                imag = jnp.zeros((ND, 128), F32)
            hi, lo = split(jnp.concatenate([real, imag], axis=1))
            parts.append(dot3(hi, lo, wx_ref[parity, 0], wx_ref[parity, 1]))
        for half, value in ((0, parts[0] + parts[1]), (1, parts[0] - parts[1])):
            cols = slice(half * 256, half * 256 + 256)
            hi, lo = split(value)
            xp[slot, 0, 0:128, cols] = hi[:, 0:256]
            xp[slot, 0, 128:256, cols] = hi[:, 256:512]
            xp[slot, 1, 0:128, cols] = lo[:, 0:256]
            xp[slot, 1, 128:256, cols] = lo[:, 256:512]

    def filtered(slot, c):
        rows = slice(c * 128, c * 128 + 128)
        spec = dot3(wz_ref[0, rows, :], wz_ref[1, rows, :], xp[slot, 0], xp[slot, 1])
        low = slice(c * Z_CHUNK, (c + 1) * Z_CHUNK)
        high = slice(NZ + c * Z_CHUNK, NZ + (c + 1) * Z_CHUNK)
        f_low, f_high = filt_ref[slot, low, :], filt_ref[slot, high, :]
        acc = None
        for kind in range(2):
            a = spec[kind * 64 : kind * 64 + 32]
            b = spec[kind * 64 + 32 : kind * 64 + 64]
            fa, fb = a * f_low, b * f_high
            power = a * fa + b * fb
            power = power[0:8] + power[8:16] + (power[16:24] + power[24:32])
            acc = power if acc is None else acc + power
            dest = slice(kind * NZ + c * Z_CHUNK, kind * NZ + (c + 1) * Z_CHUNK)
            for parity, value in ((0, fa + fb), (1, fa - fb)):
                hi, lo = split(value)
                sums[slot % 2, parity, 0, dest, :] = hi
                sums[slot % 2, parity, 1, dest, :] = lo
        acc = weight_ref[slot] * acc
        power_ref[...] = acc if slot == 0 and c == 0 else power_ref[...] + acc

    def back_z(slot, parity):
        src = sums.at[slot % 2, parity]
        grid = dot3(wzi_ref[parity, 0], wzi_ref[parity, 1], src[0], src[1])
        for sign in range(2):
            a, b = grid[:, 0:256], grid[:, 256:512]
            hi, lo = split(a + b if sign == 0 else a - b)
            for part, value in ((0, hi), (1, lo)):
                rows = slice(parity * 64, parity * 64 + 64)
                back[slot % 2, sign, part, rows, 0:256] = value[0:64]
                back[slot % 2, sign, part, rows, 256:512] = value[64:128]

    def back_x(slot, sign):
        src = back.at[slot % 2, sign]
        value = dot3(src[0], src[1], wxi_ref[sign, 0], wxi_ref[sign, 1])
        for parity in range(2):
            for kind in range(2 if slot < 2 else 1):
                put_rows(
                    out_ref,
                    parity * BACK_ROWS + HART + slot * 4 + kind * 2 + sign,
                    BACK_ROWS,
                    value[parity * 64 : parity * 64 + 64, kind * 128 : kind * 128 + 128],
                    count=64,
                    scale=2,
                )

    steps = []
    for slot in range(3):
        steps.append(lambda slot=slot: forward_x(slot))
        for c in range(NZ // Z_CHUNK):
            steps.append(lambda slot=slot, c=c: filtered(slot, c))
        for parity in range(2):
            steps.append(lambda slot=slot, parity=parity: back_z(slot, parity))
        for sign in range(2):
            steps.append(lambda slot=slot, sign=sign: back_x(slot, sign))
    return steps


def middle_kernel(
    first_ref, weight_ref, in_ref, slope_ref, slope_z_ref, filt_hbm, wx_hbm, wz_hbm, wzi_hbm, wxi_hbm,
    out_ref, filt_ref, wx_ref, wz_ref, wzi_ref, wxi_ref, dens, gz, gy, gx, xp, sums, back,
    total_ref, power_ref, sems,
):
    first = first_ref[0]
    moves = [(wx_hbm, wx_ref), (wz_hbm, wz_ref)]
    moves += [
        (filt_hbm.at[:, place, :], filt_ref.at[slot])
        for slot, place in enumerate((first, first + 1, 0))
    ]
    moves += [(wzi_hbm, wzi_ref), (wxi_hbm, wxi_ref)]
    copies = [
        pltpu.make_async_copy(source, target, sems.at[i]) for i, (source, target) in enumerate(moves)
    ]
    for copy in copies:
        copy.start()
    xc = xc_steps(in_ref, slope_ref, slope_z_ref, out_ref, total_ref, dens, gz, gy, gx)
    hartree = hartree_steps(
        in_ref, filt_ref, weight_ref, wx_ref, wz_ref, wzi_ref, wxi_ref, out_ref, power_ref,
        xp, sums, back,
    )
    for step in xc[:XC_AHEAD]:
        step()
    xc = xc[XC_AHEAD:]
    done = 0
    waits = {0: copies[0:1], 1: copies[1:3], 5: copies[5:6], 7: copies[6:7], 8: copies[3:5]}
    for i, step in enumerate(hartree):
        for copy in waits.get(i, ()):
            copy.wait()
        step()
        upto = min(len(xc), -(-(i + 1) * len(xc) // XC_SPREAD))
        for other in xc[done:upto]:
            other()
        done = max(done, upto)
    for other in xc[done:]:
        other()
    energies = jnp.where(
        iota((ND, 128), 1) < 64, jnp.sum(total_ref[...]), jnp.sum(power_ref[...])
    )
    put_rows(out_ref, BACK_ROWS - 1, BACK_ROWS, energies)


def homeward_kernel(in_ref, yb_ref, slope_ref, out_ref, energy_ref):
    field = jnp.concatenate(
        [get_rows(in_ref, HART + 2 * s, BACK_ROWS) for s in range(4)], axis=0
    )
    grid = dot3(yb_ref[0], yb_ref[1], *split(field))
    mean_row = jnp.concatenate(
        [in_ref[HART + 8 : HART + 9, :], in_ref[HART + 9 : HART + 10, :]], axis=1
    )
    grid = grid + mean_row * NORM
    hi, lo = split(grid)
    parity = parity_matrix(True)
    hartree = dot1(hi, parity) + dot1(lo, parity)
    for spin in range(2):
        flux, rest = (
            jnp.concatenate(
                [get_rows(in_ref, base + spin * 4 + part * 2, BACK_ROWS) for part in range(2)],
                axis=0,
            )
            for base in (8, 0)
        )
        rows = slice(spin * NY, (spin + 1) * NY)
        out_ref[rows, :] = rest + hartree - dot3(slope_ref[0], slope_ref[1], *split(flux))
    row = jnp.sum(in_ref[pl.ds(BACK_ROWS - 1, ND, stride=BACK_ROWS), :], axis=0, keepdims=True)
    first = iota((1, 128), 1) < 64
    energy_ref[0] = jnp.sum(jnp.where(first, row, 0.0)) * (1.0 / (64.0 * CELLS))
    energy_ref[1] = jnp.sum(jnp.where(first, 0.0, row)) * (0.5 * NORM / (64.0 * CELLS))


def call(kernel, outs, in_specs, flops, scratch=(), smem_out=(), limit=40, flags=None):
    specs = [SMEM if i in smem_out else VMEM for i in range(len(outs))]
    return pl.pallas_call(
        kernel,
        out_shape=list(outs),
        in_specs=in_specs,
        out_specs=specs,
        scratch_shapes=list(scratch),
        cost_estimate=pl.CostEstimate(flops=flops, bytes_accessed=4 << 20, transcendentals=0),
        compiler_params=pltpu.CompilerParams(vmem_limit_bytes=limit << 20, flags=flags),
        name=kernel.__name__,
    )


def in_hbm(value):
    return pltpu.with_memory_space_constraint(value, pltpu.HBM)


def arr(*shape, dtype=F32):
    return jax.ShapeDtypeStruct(shape, dtype)


def exchange(value, rows, group):
    shaped = value.reshape(ND * rows // group, group, 128)
    out = lax.all_to_all(shaped, GZ, split_axis=0, concat_axis=0, tiled=True)
    return out.reshape(ND * rows, 128)


def per_device(density, kernel_hat):
    q = lax.axis_index(GZ)
    (outward,) = call(
        outward_kernel,
        [arr(ND * OUT_ROWS, 128)],
        [HBM, HBM],
        400_000_000,
        scratch=[
            pltpu.VMEM((2 * NY, NX), F32),
            pltpu.VMEM((2, 4 * ND, NY), BF16),
            pltpu.SemaphoreType.DMA((2,)),
        ],
    )(in_hbm(density.reshape(2 * NY, NX)), in_hbm(jnp.asarray(y_forward())))
    arrived = exchange(outward, OUT_ROWS, 2)
    shapes = [(2, 2, NX, MX), (2, 2 * MZ, 2 * NZ), (2, 2, NZ, 2 * NZ), (2, 2, MX, NX)]
    wx, wz, wzi, wxi, yb, slope, slope_z = call(
        tables_kernel,
        [arr(*shape, dtype=BF16) for shape in shapes]
        + [
            arr(2, NY, 4 * ND, dtype=BF16),
            arr(2, NY, NY, dtype=BF16),
            arr(2, NZ, 2 * NZ, dtype=BF16),
        ],
        [],
        2_000_000_000,
    )()
    start = jnp.where(q < ND // 2, 1, 0).astype(jnp.int32).reshape(1)
    weights = jnp.stack(
        [
            jnp.where(q == ND // 2, 1.0, 2.0),
            jnp.full((), 2.0),
            jnp.where(q == 0, 1.0, 0.0),
        ]
    ).astype(F32)
    field = pltpu.VMEM((2, 256, NX), F32)
    (back,) = call(
        middle_kernel,
        [arr(ND * BACK_ROWS, 128)],
        [SMEM, SMEM] + [VMEM] * 3 + [HBM] * 5,
        8_000_000_000,
        scratch=[pltpu.VMEM((3, MZ, MX), F32)]
        + [pltpu.VMEM(shape, BF16) for shape in shapes]
        + [field] * 4
        + [
            pltpu.VMEM((3, 2, 256, 512), BF16),
            pltpu.VMEM((2, 2, 2, 256, 512), BF16),
            pltpu.VMEM((2, 2, 2, 128, 512), BF16),
            pltpu.VMEM((8, NX), F32),
            pltpu.VMEM((8, MX), F32),
            pltpu.SemaphoreType.DMA((7,)),
        ],
    )(start, weights, arrived, slope, slope_z, *map(in_hbm, (kernel_hat, wx, wz, wzi, wxi)))
    returned = exchange(back, BACK_ROWS, 1)
    potential, energies = call(
        homeward_kernel,
        [arr(2 * NY, NX), arr(2)],
        [VMEM] * 3,
        1_000_000_000,
        smem_out=(1,),
    )(returned, yb, slope)
    return potential.reshape(2, 1, NY, NX), energies


def solution(mesh):
    torus = Mesh(mesh.devices.reshape(4, 4, 4, 2), GZ)
    placed = (P(None, GZ, None, None), P(None, GZ, None))
    return jax.shard_map(
        per_device,
        mesh=torus,
        in_specs=placed,
        out_specs=(P(None, GZ, None, None), P()),
        check_vma=False,
    )
```

```python
import math

import jax
import jax.numpy as jnp
import numpy as np
from jax import lax
from jax.experimental import pallas as pl
from jax.experimental.pallas import tpu as pltpu
from jax.sharding import Mesh
from jax.sharding import PartitionSpec as P

GZ = ("gz_0", "gz_1", "gz_2", "gz_3")
HGRID = 0.35
STENCIL = (0.8, -0.2, 4.0 / 105.0, -1.0 / 280.0)
KAPPA = 0.804
MU_X = 0.2195149727645171
BETA_C = 0.06672455060314922
GAMMA_C = 0.031090690869654894
FZ_CURV = 1.709921
PARAMS_UNPOL = (0.031091, 0.2137, 7.5957, 3.5876, 1.6382, 0.49294)
PARAMS_POL = (0.015545, 0.20548, 14.1189, 6.1977, 3.3662, 0.62517)
PARAMS_STIFF = (0.016887, 0.11125, 10.357, 3.6231, 0.88026, 0.49671)

F32 = jnp.float32
BF16 = jnp.bfloat16
NZ, NY, NX = 128, 256, 256
MZ, MY, MX = 256, 512, 512
ND = 128
HART = 16
OUT_ROWS = 24
BACK_ROWS = 25
PAIR = ND // 2
CELLS = NZ * NY * NX
Z_CHUNK = 32
XC_ROWS = 8
XC_AHEAD = 6
XC_SPREAD = 27
NORM = 1.0 / (MX * MY * MZ)
VMEM = pl.BlockSpec(memory_space=pltpu.VMEM)
SMEM = pl.BlockSpec(memory_space=pltpu.SMEM)
HBM = pl.BlockSpec(memory_space=pltpu.HBM)


def halves(m):
    m = np.asarray(m, np.float32)
    hi = m.astype(BF16)
    lo = (m - hi.astype(np.float32)).astype(BF16)
    return np.stack([hi, lo])


def y_forward():
    y, q = np.arange(NY), np.arange(ND)
    first = np.where(q < ND // 2, 4 * q + 1, 4 * q)
    rows = []
    for ky in (first, first + 1):
        angle = 2.0 * np.pi * (np.outer(ky, y) % MY) / MY
        paired = (ky == MY // 2)[:, None]
        rows += [np.cos(angle), np.where(paired, 1.0, -np.sin(angle))]
    return halves(np.concatenate(rows, 0))


def split(value):
    hi = value.astype(BF16)
    lo = (value - hi.astype(F32)).astype(BF16)
    return hi, lo


def dot1(a, b):
    return jnp.dot(a, b, preferred_element_type=F32)


def dot3(a_hi, a_lo, b_hi, b_lo):
    return dot1(a_hi, b_hi) + (dot1(a_lo, b_hi) + dot1(a_hi, b_lo))


def put_rows(ref, row, rows, value, count=ND, scale=1):
    for half in range(value.shape[1] // 128):
        ref[pl.ds(row + half, count, stride=rows * scale), :] = value[
            :, half * 128 : half * 128 + 128
        ]


def get_rows(ref, row, rows):
    return jnp.concatenate(
        [ref[pl.ds(row + half, ND, stride=rows), :] for half in range(2)], axis=1
    )


def iota(shape, dim):
    return lax.broadcasted_iota(jnp.int32, shape, dim)


def slope_parts(n):
    offset = iota((n, n), 1) - iota((n, n), 0)
    parts = []
    coefs = halves([c / HGRID for c in STENCIL]).astype(np.float32)
    for part in range(2):
        value = jnp.zeros((n, n), F32)
        for k in range(1, 5):
            c = float(coefs[part, k - 1])
            value = jnp.where(offset == k, c, jnp.where(offset == -k, -c, value))
        parts.append(value.astype(BF16))
    return parts


def parity_matrix(transposed):
    x, place = iota((NX, NX), int(transposed)), iota((NX, NX), 1 - int(transposed))
    return jnp.where(place == (x & 1) * (NX // 2) + (x >> 1), 1.0, 0.0).astype(BF16)


def cos_sin(product):
    turn = product.astype(jnp.int32) & 511
    quarter = (turn + 64) >> 7
    angle = (turn - 128 * quarter).astype(F32) * (2.0 * math.pi / 512.0)
    sq = angle * angle
    s = angle * (
        1.0 + sq * (-1.0 / 6.0 + sq * (1.0 / 120.0 + sq * (-1.0 / 5040.0 + sq * (1.0 / 362880.0))))
    )
    c = 1.0 + sq * (-0.5 + sq * (1.0 / 24.0 + sq * (-1.0 / 720.0 + sq * (1.0 / 40320.0))))
    odd = (quarter & 1) == 1
    c, s = jnp.where(odd, s, c), jnp.where(odd, c, s)
    return (
        jnp.where(((quarter + 1) & 2) == 2, -c, c),
        jnp.where((quarter & 2) == 2, -s, s),
    )


def put_parts(ref, index, rows, cols, value):
    hi, lo = split(value)
    ref[(*index, 0, rows, cols)] = hi
    ref[(*index, 1, rows, cols)] = lo


def put_rotation(ref, index, row, c, s, transposed):
    n, m = c.shape
    top, low = slice(row, row + n), slice(row + n, row + 2 * n)
    put_parts(ref, index, top, slice(0, m), c)
    put_parts(ref, index, low, slice(m, 2 * m), c)
    put_parts(ref, index, top, slice(m, 2 * m), -s if transposed else s)
    put_parts(ref, index, low, slice(0, m), s if transposed else -s)


def float_iota(shape, dim):
    return iota(shape, dim).astype(F32)


def tables_kernel(wx_ref, wz_ref, wzi_ref, wxi_ref, yb_ref, slope_ref, slope_z_ref):
    for parity in range(2):
        shape = (NX // 2, MX // 2)
        x = 2.0 * float_iota(shape, 0) + parity
        put_rotation(wx_ref, (parity,), 0, *cos_sin(x * float_iota(shape, 1)), True)
        shape = (MX // 2, NX // 2)
        x = 2.0 * float_iota(shape, 1) + parity
        put_rotation(wxi_ref, (parity,), 0, *cos_sin(x * float_iota(shape, 0)), False)
        shape = (NZ // 2, NZ)
        z = 4.0 * float_iota(shape, 0) + 2.0 * parity
        put_rotation(wzi_ref, (parity,), 0, *cos_sin(z * float_iota(shape, 1)), True)
    for chunk in range(NZ // Z_CHUNK):
        shape = (2 * Z_CHUNK, NZ)
        row = iota(shape, 0)
        kz = chunk * Z_CHUNK + jnp.where(row < Z_CHUNK, row, row + NZ - Z_CHUNK)
        angle = 2.0 * kz.astype(F32) * float_iota(shape, 1)
        put_rotation(wz_ref, (), chunk * 4 * Z_CHUNK, *cos_sin(angle), False)
    for slot in range(2):
        shape = (NY, ND)
        q = iota(shape, 1)
        ky = 4 * q + slot + jnp.where(q < ND // 2, 1, 0)
        c, s = cos_sin(ky.astype(F32) * float_iota(shape, 0))
        weight = jnp.where(ky == MY // 2, NORM, 2.0 * NORM)
        s = jnp.where(ky == MY // 2, -1.0, s)
        put_parts(yb_ref, (), slice(0, NY), slice(256 * slot, 256 * slot + 128), c * weight)
        put_parts(yb_ref, (), slice(0, NY), slice(256 * slot + 128, 256 * slot + 256), -s * weight)
    for part, value in enumerate(slope_parts(NY)):
        slope_ref[part] = value
    for part, value in enumerate(slope_parts(NZ)):
        slope_z_ref[part, :, 0:NZ] = value
        slope_z_ref[part, :, NZ : 2 * NZ] = value


def filter_kernel(first_ref, half_ref, filt_hbm, other_ref, out_ref, planes, sems):
    first = first_ref[0]
    copies = [
        pltpu.make_async_copy(filt_hbm.at[:, first + slot, :], planes.at[slot], sems.at[slot])
        for slot in range(2)
    ]
    for copy in copies:
        copy.start()
    for copy in copies:
        copy.wait()
    half = half_ref[0]
    own = planes[0]
    mirror = (own - other_ref[...]) * half
    out_ref[0] = own - mirror
    out_ref[1] = planes[1]
    out_ref[2] = mirror


def outward_kernel(dens_hbm, table_hbm, out_ref, dens_ref, table_ref, sems):
    dens_copy = pltpu.make_async_copy(dens_hbm, dens_ref, sems.at[0])
    table_copy = pltpu.make_async_copy(table_hbm, table_ref, sems.at[1])
    dens_copy.start()
    table_copy.start()
    slope = slope_parts(NY)
    parity = parity_matrix(False)
    dens_copy.wait()
    for spin in range(2):
        field = dens_ref[spin * NY : (spin + 1) * NY, :]
        grad = dot3(*slope, *split(field))
        for part in range(2):
            rows = slice(part * 128, part * 128 + 128)
            put_rows(out_ref, spin * 4 + part * 2, OUT_ROWS, field[rows])
            put_rows(out_ref, 8 + spin * 4 + part * 2, OUT_ROWS, grad[rows])
    hi, lo = split(dens_ref[0:NY, :] + dens_ref[NY : 2 * NY, :])
    hi, lo = dot1(hi, parity), dot1(lo, parity)
    hi, lo = hi.astype(BF16), lo.astype(BF16)
    table_copy.wait()
    for s in range(4):
        rows = slice(s * ND, (s + 1) * ND)
        value = dot3(table_ref[0, rows, :], table_ref[1, rows, :], hi, lo)
        put_rows(out_ref, HART + s * 2, OUT_ROWS, value)


def pw_piece(root, params):
    radius = root * root
    scale = 2.0 * params[0]
    series = root * (
        scale * params[2]
        + root * (scale * params[3] + root * (scale * params[4] + root * (scale * params[5])))
    )
    slope = root * (
        0.5 * scale * params[2]
        + root
        * (
            scale * params[3]
            + root * (1.5 * scale * params[4] + root * (2.0 * scale * params[5]))
        )
    )
    inv = 1.0 / (series * (series + 1.0))
    logarithm = jnp.log(1.0 + inv * (series + 1.0))
    front = -scale - (scale * params[1]) * radius
    value = front * logarithm
    deriv = (-scale * params[1]) * radius * logarithm - front * slope * inv
    return value, deriv


def exchange_piece(dens, inv_root, sigma):
    root = 2.0 * dens * inv_root * inv_root
    inv2 = inv_root * inv_root
    inv4 = inv2 * inv2
    reduced = sigma * (inv4 * inv4) * (1.0 / (3.0 * math.pi**2) ** (2.0 / 3.0))
    damp = 1.0 / (1.0 + (MU_X / KAPPA) * reduced)
    enhance = (1.0 + KAPPA) - KAPPA * damp
    front = -0.75 * (3.0 / math.pi) ** (1.0 / 3.0)
    damp_sq = MU_X * damp * damp
    energy = front * dens * root * enhance
    d_dens = (4.0 / 3.0 * front) * root * (enhance - 2.0 * reduced * damp_sq)
    d_sigma = (0.5 * front / (3.0 * math.pi**2) ** (2.0 / 3.0)) * damp_sq * inv4
    return energy, d_dens, d_sigma, root


def xc_point(up, down, sigma_uu, sigma_ud, sigma_dd):
    inv_up = jnp.exp(jnp.log(2.0 * up) * (-1.0 / 3.0))
    inv_down = jnp.exp(jnp.log(2.0 * down) * (-1.0 / 3.0))
    e_up, d_up, d_uu, root_up = exchange_piece(up, inv_up, sigma_uu)
    e_down, d_down, d_dd, root_down = exchange_piece(down, inv_down, sigma_dd)
    dens = up + down
    sixth = jnp.exp(jnp.log(dens) * (-1.0 / 6.0))
    inv_third = sixth * sixth
    third = dens * inv_third * inv_third
    inv_dens = inv_third * inv_third * inv_third
    zeta = (up - down) * inv_dens
    plus = 2.0 * up * inv_dens
    minus = 2.0 * down * inv_dens
    plus_cube = root_up * inv_third
    minus_cube = root_down * inv_third
    f_scale = 1.0 / (2.0 ** (4.0 / 3.0) - 2.0)
    f = (plus * plus_cube + minus * minus_cube - 2.0) * f_scale
    f_slope = (plus_cube - minus_cube) * (4.0 / 3.0 * f_scale)
    root = (3.0 / (4.0 * math.pi)) ** (1.0 / 6.0) * sixth
    e0, e0_d = pw_piece(root, PARAMS_UNPOL)
    e1, e1_d = pw_piece(root, PARAMS_POL)
    ac, ac_d = pw_piece(root, PARAMS_STIFF)
    z2 = zeta * zeta
    z3_4 = 4.0 * z2 * zeta
    z4 = z2 * z2
    one_z4 = (1.0 - z4) * (-1.0 / FZ_CURV)
    f_z4 = f * z4
    f_one = f * one_z4
    diff = e1 - e0
    local = e0 + ac * f_one + diff * f_z4
    local_r = e0_d + ac_d * f_one + (e1_d - e0_d) * f_z4
    fz3 = z3_4 * f
    local_z = ac * (f_slope * one_z4 + (1.0 / FZ_CURV) * fz3) + diff * (f_slope * z4 + fz3)
    phi = 0.5 * (plus_cube * plus_cube + minus_cube * minus_cube)
    inv_phi = 1.0 / phi
    phi_log_slope = (third * (1.0 / 3.0)) * (inv_up - inv_down) * inv_phi
    g3 = GAMMA_C * phi * phi * phi
    inv_g3 = (1.0 / GAMMA_C) * inv_phi * inv_phi * inv_phi
    grow = jnp.exp(-local * inv_g3)
    weight_a = (BETA_C / GAMMA_C) / (grow - 1.0)
    sigma = sigma_uu + 2.0 * sigma_ud + sigma_dd
    ct = math.pi / (16.0 * (3.0 * math.pi**2) ** (1.0 / 3.0))
    kt = ct * inv_third * inv_dens * inv_dens * inv_phi * inv_phi
    t2 = sigma * kt
    w = weight_a * t2
    num = 1.0 + w
    den = num + w * w
    add = (BETA_C / GAMMA_C) * t2 * num
    both = den + add
    inv_both = 1.0 / (den * both)
    h = g3 * jnp.log(1.0 + add * (inv_both * both))
    h_t = (BETA_C / GAMMA_C) * g3 * (1.0 + 2.0 * w) * inv_both
    h_a = -(w * w * w) * (2.0 + w) * grow * inv_both
    total = local + h
    ht_t2 = h_t * t2
    one_ha = 1.0 + h_a
    d_n = total - (1.0 / 3.0) * one_ha * local_r - (7.0 / 3.0) * ht_t2
    d_z = one_ha * local_z + phi_log_slope * (3.0 * (h - h_a * local) - 2.0 * ht_t2)
    d_sigma = dens * h_t * kt
    energy = e_up + e_down + dens * total
    return (
        energy,
        d_up + d_n + minus * d_z,
        d_down + d_n - plus * d_z,
        d_uu + d_sigma,
        2.0 * d_sigma,
        d_dd + d_sigma,
    )


def slope_along_z(slope_z_ref, hi, lo):
    both = jnp.concatenate([hi, lo], axis=0)
    return dot1(slope_z_ref[0], both) + dot1(slope_z_ref[1], both)


def slope_along_x(slope_ref, hi, lo):
    return -dot3(hi, lo, slope_ref[0], slope_ref[1])


def xc_steps(in_ref, slope_ref, slope_z_ref, out_ref, total_ref, dens, gz, gy, gx):
    def gradients(part):
        rows = slice(part * 128, part * 128 + 128)
        for spin in range(2):
            field = get_rows(in_ref, spin * 4 + part * 2, OUT_ROWS)
            dens[spin, rows, :] = field
            gy[spin, rows, :] = get_rows(in_ref, 8 + spin * 4 + part * 2, OUT_ROWS)
            hi, lo = split(field)
            gz[spin, rows, :] = slope_along_z(slope_z_ref, hi, lo)
            gx[spin, rows, :] = slope_along_x(slope_ref, hi, lo)

    def points(i):
        rows = slice(i * XC_ROWS, (i + 1) * XC_ROWS)
        zu, zd = gz[0, rows, :], gz[1, rows, :]
        yu, yd = gy[0, rows, :], gy[1, rows, :]
        xu, xd = gx[0, rows, :], gx[1, rows, :]
        energy, d_up, d_down, d_uu, d_ud, d_dd = xc_point(
            dens[0, rows, :],
            dens[1, rows, :],
            zu * zu + yu * yu + xu * xu,
            zu * zd + yu * yd + xu * xd,
            zd * zd + yd * yd + xd * xd,
        )
        dens[0, rows, :] = d_up
        dens[1, rows, :] = d_down
        for ref, gu, gd in ((gz, zu, zd), (gy, yu, yd), (gx, xu, xd)):
            ref[0, rows, :] = 2.0 * d_uu * gu + d_ud * gd
            ref[1, rows, :] = 2.0 * d_dd * gd + d_ud * gu
        folded = sum(energy[r : r + 8] for r in range(0, XC_ROWS, 8))
        total_ref[...] = folded if i == 0 else total_ref[...] + folded

    def divergence(part):
        rows = slice(part * 128, part * 128 + 128)
        for spin in range(2):
            div = slope_along_z(slope_z_ref, *split(gz[spin, rows, :]))
            div = div + slope_along_x(slope_ref, *split(gx[spin, rows, :]))
            put_rows(out_ref, spin * 4 + part * 2, BACK_ROWS, dens[spin, rows, :] - div)
            put_rows(out_ref, 8 + spin * 4 + part * 2, BACK_ROWS, gy[spin, rows, :])

    steps = []
    for part in range(2):
        steps.append(lambda part=part: gradients(part))
        for i in range(part * 128 // XC_ROWS, (part + 1) * 128 // XC_ROWS):
            steps.append(lambda i=i: points(i))
        steps.append(lambda part=part: divergence(part))
    return steps


def hartree_steps(
    in_ref, filt_ref, weight_ref, wx_ref, wz_ref, wzi_ref, wxi_ref, out_ref, power_ref, xp, sums, back
):
    def forward_x(slot, conjugate):
        parts = []
        for parity in range(2):
            base = HART + 4 * slot + parity
            real = in_ref[pl.ds(base, ND, stride=OUT_ROWS), :]
            imag = in_ref[pl.ds(base + 2, ND, stride=OUT_ROWS), :]
            both = jnp.concatenate([real, -imag if conjugate else imag], axis=1)
            parts.append(dot3(*split(both), wx_ref[parity, 0], wx_ref[parity, 1]))
        place = 2 if conjugate else slot
        for half, value in ((0, parts[0] + parts[1]), (1, parts[0] - parts[1])):
            cols = slice(half * 256, half * 256 + 256)
            hi, lo = split(value)
            xp[place, 0, 0:128, cols] = hi[:, 0:256]
            xp[place, 0, 128:256, cols] = hi[:, 256:512]
            xp[place, 1, 0:128, cols] = lo[:, 0:256]
            xp[place, 1, 128:256, cols] = lo[:, 256:512]

    def filtered(slot, c):
        rows = slice(c * 128, c * 128 + 128)
        spec = dot3(wz_ref[0, rows, :], wz_ref[1, rows, :], xp[slot, 0], xp[slot, 1])
        if slot == 0:
            mirror = dot3(wz_ref[0, rows, :], wz_ref[1, rows, :], xp[2, 0], xp[2, 1])
        acc = None
        for kind in range(2):
            pair = []
            for high in range(2):
                place = slice(high * NZ + c * Z_CHUNK, high * NZ + (c + 1) * Z_CHUNK)
                at = slice(kind * 64 + high * 32, kind * 64 + high * 32 + 32)
                value = spec[at] * filt_ref[slot, place, :]
                if slot == 0:
                    value = value + mirror[at] * filt_ref[2, place, :]
                power = spec[at] * value
                power = power[0:8] + power[8:16] + (power[16:24] + power[24:32])
                acc = power if acc is None else acc + power
                pair.append(value)
            dest = slice(kind * NZ + c * Z_CHUNK, kind * NZ + (c + 1) * Z_CHUNK)
            for parity, value in ((0, pair[0] + pair[1]), (1, pair[0] - pair[1])):
                hi, lo = split(value)
                sums[slot, parity, 0, dest, :] = hi
                sums[slot, parity, 1, dest, :] = lo
        acc = weight_ref[slot] * acc
        power_ref[...] = acc if slot == 0 and c == 0 else power_ref[...] + acc

    def back_z(slot, parity):
        src = sums.at[slot, parity]
        grid = dot3(wzi_ref[parity, 0], wzi_ref[parity, 1], src[0], src[1])
        for sign in range(2):
            a, b = grid[:, 0:256], grid[:, 256:512]
            hi, lo = split(a + b if sign == 0 else a - b)
            for part, value in ((0, hi), (1, lo)):
                rows = slice(parity * 64, parity * 64 + 64)
                back[slot, sign, part, rows, 0:256] = value[0:64]
                back[slot, sign, part, rows, 256:512] = value[64:128]

    def back_x(slot, sign):
        src = back.at[slot, sign]
        value = dot3(src[0], src[1], wxi_ref[sign, 0], wxi_ref[sign, 1])
        for parity in range(2):
            for kind in range(2):
                put_rows(
                    out_ref,
                    parity * BACK_ROWS + HART + slot * 4 + kind * 2 + sign,
                    BACK_ROWS,
                    value[parity * 64 : parity * 64 + 64, kind * 128 : kind * 128 + 128],
                    count=64,
                    scale=2,
                )

    steps = []
    for slot in range(2):
        steps.append(lambda slot=slot: forward_x(slot, False))
        if slot == 0:
            steps.append(lambda: forward_x(0, True))
        for c in range(NZ // Z_CHUNK):
            steps.append(lambda slot=slot, c=c: filtered(slot, c))
        for parity in range(2):
            steps.append(lambda slot=slot, parity=parity: back_z(slot, parity))
        for sign in range(2):
            steps.append(lambda slot=slot, sign=sign: back_x(slot, sign))
    return steps


def middle_kernel(
    weight_ref, in_ref, slope_ref, slope_z_ref, filt_hbm, wx_hbm, wz_hbm, wzi_hbm, wxi_hbm,
    out_ref, filt_ref, wx_ref, wz_ref, wzi_ref, wxi_ref, dens, gz, gy, gx, xp, sums, back,
    total_ref, power_ref, sems,
):
    moves = [(wx_hbm, wx_ref), (wz_hbm, wz_ref), (filt_hbm, filt_ref)]
    moves += [(wzi_hbm, wzi_ref), (wxi_hbm, wxi_ref)]
    copies = [
        pltpu.make_async_copy(source, target, sems.at[i]) for i, (source, target) in enumerate(moves)
    ]
    for copy in copies:
        copy.start()
    xc = xc_steps(in_ref, slope_ref, slope_z_ref, out_ref, total_ref, dens, gz, gy, gx)
    hartree = hartree_steps(
        in_ref, filt_ref, weight_ref, wx_ref, wz_ref, wzi_ref, wxi_ref, out_ref, power_ref,
        xp, sums, back,
    )
    for step in xc[:XC_AHEAD]:
        step()
    xc = xc[XC_AHEAD:]
    done = 0
    waits = {0: copies[0:1], 2: copies[1:3], 6: copies[3:4], 8: copies[4:5]}
    for i, step in enumerate(hartree):
        for copy in waits.get(i, ()):
            copy.wait()
        step()
        upto = min(len(xc), -(-(i + 1) * len(xc) // XC_SPREAD))
        for other in xc[done:upto]:
            other()
        done = max(done, upto)
    for other in xc[done:]:
        other()
    energies = jnp.where(
        iota((ND, 128), 1) < 64, jnp.sum(total_ref[...]), jnp.sum(power_ref[...])
    )
    put_rows(out_ref, BACK_ROWS - 1, BACK_ROWS, energies)


def homeward_kernel(in_ref, yb_ref, slope_ref, out_ref, energy_ref):
    field = jnp.concatenate(
        [get_rows(in_ref, HART + 2 * s, BACK_ROWS) for s in range(4)], axis=0
    )
    grid = dot3(yb_ref[0], yb_ref[1], *split(field))
    hi, lo = split(grid)
    parity = parity_matrix(True)
    hartree = dot1(hi, parity) + dot1(lo, parity)
    for spin in range(2):
        flux, rest = (
            jnp.concatenate(
                [get_rows(in_ref, base + spin * 4 + part * 2, BACK_ROWS) for part in range(2)],
                axis=0,
            )
            for base in (8, 0)
        )
        rows = slice(spin * NY, (spin + 1) * NY)
        out_ref[rows, :] = rest + hartree - dot3(slope_ref[0], slope_ref[1], *split(flux))
    row = jnp.sum(in_ref[pl.ds(BACK_ROWS - 1, ND, stride=BACK_ROWS), :], axis=0, keepdims=True)
    first = iota((1, 128), 1) < 64
    energy_ref[0] = jnp.sum(jnp.where(first, row, 0.0)) * (1.0 / (64.0 * CELLS))
    energy_ref[1] = jnp.sum(jnp.where(first, 0.0, row)) * (0.5 * NORM / (64.0 * CELLS))


def call(kernel, outs, in_specs, flops, scratch=(), smem_out=(), limit=40, flags=None):
    specs = [SMEM if i in smem_out else VMEM for i in range(len(outs))]
    return pl.pallas_call(
        kernel,
        out_shape=list(outs),
        in_specs=in_specs,
        out_specs=specs,
        scratch_shapes=list(scratch),
        cost_estimate=pl.CostEstimate(flops=flops, bytes_accessed=4 << 20, transcendentals=0),
        compiler_params=pltpu.CompilerParams(vmem_limit_bytes=limit << 20, flags=flags),
        name=kernel.__name__,
    )


def in_hbm(value):
    return pltpu.with_memory_space_constraint(value, pltpu.HBM)


def arr(*shape, dtype=F32):
    return jax.ShapeDtypeStruct(shape, dtype)


def exchange(value, rows, group):
    shaped = value.reshape(ND * rows // group, group, 128)
    out = lax.all_to_all(shaped, GZ, split_axis=0, concat_axis=0, tiled=True)
    return out.reshape(ND * rows, 128)


def per_device(density, kernel_hat):
    q = lax.axis_index(GZ)
    (outward,) = call(
        outward_kernel,
        [arr(ND * OUT_ROWS, 128)],
        [HBM, HBM],
        400_000_000,
        scratch=[
            pltpu.VMEM((2 * NY, NX), F32),
            pltpu.VMEM((2, 4 * ND, NY), BF16),
            pltpu.SemaphoreType.DMA((2,)),
        ],
    )(in_hbm(density.reshape(2 * NY, NX)), in_hbm(jnp.asarray(y_forward())))
    outward, kernel_hat = lax.optimization_barrier((outward, kernel_hat))
    arrived = exchange(outward, OUT_ROWS, 8)
    shapes = [(2, 2, NX, MX), (2, 2 * MZ, 2 * NZ), (2, 2, NZ, 2 * NZ), (2, 2, MX, NX)]
    wx, wz, wzi, wxi, yb, slope, slope_z = call(
        tables_kernel,
        [arr(*shape, dtype=BF16) for shape in shapes]
        + [
            arr(2, NY, 4 * ND, dtype=BF16),
            arr(2, NY, NY, dtype=BF16),
            arr(2, NZ, 2 * NZ, dtype=BF16),
        ],
        [],
        2_000_000_000,
    )()
    start = jnp.where(q < ND // 2, 1, 0).astype(jnp.int32).reshape(1)
    other = lax.ppermute(kernel_hat[:, 0, :], GZ, [(0, PAIR)])
    (filt,) = call(
        filter_kernel,
        [arr(3, MZ, MX)],
        [SMEM, SMEM, HBM, VMEM],
        100_000_000,
        scratch=[pltpu.VMEM((2, MZ, MX), F32), pltpu.SemaphoreType.DMA((2,))],
    )(start, jnp.where(q == PAIR, 0.5, 0.0).astype(F32).reshape(1), in_hbm(kernel_hat), other)
    weights = jnp.stack([jnp.where(q == PAIR, 1.0, 2.0), jnp.full((), 2.0)]).astype(F32)
    field = pltpu.VMEM((2, 256, NX), F32)
    (back,) = call(
        middle_kernel,
        [arr(ND * BACK_ROWS, 128)],
        [SMEM] + [VMEM] * 3 + [HBM] * 5,
        8_000_000_000,
        scratch=[pltpu.VMEM((3, MZ, MX), F32)]
        + [pltpu.VMEM(shape, BF16) for shape in shapes]
        + [field] * 4
        + [
            pltpu.VMEM((3, 2, 256, 512), BF16),
            pltpu.VMEM((2, 2, 2, 256, 512), BF16),
            pltpu.VMEM((2, 2, 2, 128, 512), BF16),
            pltpu.VMEM((8, NX), F32),
            pltpu.VMEM((8, MX), F32),
            pltpu.SemaphoreType.DMA((5,)),
        ],
    )(weights, arrived, slope, slope_z, *map(in_hbm, (filt, wx, wz, wzi, wxi)))
    returned = exchange(back, BACK_ROWS, 1)
    potential, energies = call(
        homeward_kernel,
        [arr(2 * NY, NX), arr(2)],
        [VMEM] * 3,
        1_000_000_000,
        smem_out=(1,),
    )(returned, yb, slope)
    return potential.reshape(2, 1, NY, NX), energies


def solution(mesh):
    torus = Mesh(mesh.devices.reshape(4, 4, 4, 2), GZ)
    placed = (P(None, GZ, None, None), P(None, GZ, None))
    return jax.shard_map(
        per_device,
        mesh=torus,
        in_specs=placed,
        out_specs=(P(None, GZ, None, None), P()),
        check_vma=False,
    )
```

```python
import math

import jax
import jax.numpy as jnp
import numpy as np
from jax import lax
from jax.experimental import pallas as pl
from jax.experimental.pallas import tpu as pltpu
from jax.sharding import Mesh
from jax.sharding import PartitionSpec as P

GZ = ("gz_0", "gz_1", "gz_2", "gz_3")
HGRID = 0.35
STENCIL = (0.8, -0.2, 4.0 / 105.0, -1.0 / 280.0)
KAPPA = 0.804
MU_X = 0.2195149727645171
BETA_C = 0.06672455060314922
GAMMA_C = 0.031090690869654894
FZ_CURV = 1.709921
PARAMS_UNPOL = (0.031091, 0.2137, 7.5957, 3.5876, 1.6382, 0.49294)
PARAMS_POL = (0.015545, 0.20548, 14.1189, 6.1977, 3.3662, 0.62517)
PARAMS_STIFF = (0.016887, 0.11125, 10.357, 3.6231, 0.88026, 0.49671)

F32 = jnp.float32
BF16 = jnp.bfloat16
NZ, NY, NX = 128, 256, 256
MZ, MY, MX = 256, 512, 512
ND = 128
HART = 16
OUT_ROWS = 24
BACK_ROWS = 25
PAIR = ND // 2
CELLS = NZ * NY * NX
Z_CHUNK = 32
XC_ROWS = 8
XC_AHEAD = 6
XC_SPREAD = 27
NORM = 1.0 / (MX * MY * MZ)
VMEM = pl.BlockSpec(memory_space=pltpu.VMEM)
SMEM = pl.BlockSpec(memory_space=pltpu.SMEM)
HBM = pl.BlockSpec(memory_space=pltpu.HBM)


def halves(m):
    m = np.asarray(m, np.float32)
    hi = m.astype(BF16)
    lo = (m - hi.astype(np.float32)).astype(BF16)
    return np.stack([hi, lo])


def y_forward():
    y, q = np.arange(NY), np.arange(ND)
    first = np.where(q < ND // 2, 4 * q + 1, 4 * q)
    rows = []
    for ky in (first, first + 1):
        angle = 2.0 * np.pi * (np.outer(ky, y) % MY) / MY
        paired = (ky == MY // 2)[:, None]
        rows += [np.cos(angle), np.where(paired, 1.0, -np.sin(angle))]
    return halves(np.concatenate(rows, 0))


def split(value):
    hi = value.astype(BF16)
    lo = (value - hi.astype(F32)).astype(BF16)
    return hi, lo


def dot1(a, b):
    return jnp.dot(a, b, preferred_element_type=F32)


def dot3(a_hi, a_lo, b_hi, b_lo):
    return dot1(a_hi, b_hi) + (dot1(a_lo, b_hi) + dot1(a_hi, b_lo))


def put_rows(ref, row, rows, value, count=ND, scale=1):
    for half in range(value.shape[1] // 128):
        ref[pl.ds(row + half, count, stride=rows * scale), :] = value[
            :, half * 128 : half * 128 + 128
        ]


def get_rows(ref, row, rows):
    return jnp.concatenate(
        [ref[pl.ds(row + half, ND, stride=rows), :] for half in range(2)], axis=1
    )


def iota(shape, dim):
    return lax.broadcasted_iota(jnp.int32, shape, dim)


def slope_parts(n):
    offset = iota((n, n), 1) - iota((n, n), 0)
    parts = []
    coefs = halves([c / HGRID for c in STENCIL]).astype(np.float32)
    for part in range(2):
        value = jnp.zeros((n, n), F32)
        for k in range(1, 5):
            c = float(coefs[part, k - 1])
            value = jnp.where(offset == k, c, jnp.where(offset == -k, -c, value))
        parts.append(value.astype(BF16))
    return parts


def parity_matrix(transposed):
    x, place = iota((NX, NX), int(transposed)), iota((NX, NX), 1 - int(transposed))
    return jnp.where(place == (x & 1) * (NX // 2) + (x >> 1), 1.0, 0.0).astype(BF16)


def cos_sin(product):
    turn = product.astype(jnp.int32) & 511
    quarter = (turn + 64) >> 7
    angle = (turn - 128 * quarter).astype(F32) * (2.0 * math.pi / 512.0)
    sq = angle * angle
    s = angle * (
        1.0 + sq * (-1.0 / 6.0 + sq * (1.0 / 120.0 + sq * (-1.0 / 5040.0 + sq * (1.0 / 362880.0))))
    )
    c = 1.0 + sq * (-0.5 + sq * (1.0 / 24.0 + sq * (-1.0 / 720.0 + sq * (1.0 / 40320.0))))
    odd = (quarter & 1) == 1
    c, s = jnp.where(odd, s, c), jnp.where(odd, c, s)
    return (
        jnp.where(((quarter + 1) & 2) == 2, -c, c),
        jnp.where((quarter & 2) == 2, -s, s),
    )


def put_parts(ref, index, rows, cols, value):
    hi, lo = split(value)
    ref[(*index, 0, rows, cols)] = hi
    ref[(*index, 1, rows, cols)] = lo


def put_rotation(ref, index, row, c, s, transposed):
    n, m = c.shape
    top, low = slice(row, row + n), slice(row + n, row + 2 * n)
    put_parts(ref, index, top, slice(0, m), c)
    put_parts(ref, index, low, slice(m, 2 * m), c)
    put_parts(ref, index, top, slice(m, 2 * m), -s if transposed else s)
    put_parts(ref, index, low, slice(0, m), s if transposed else -s)


def float_iota(shape, dim):
    return iota(shape, dim).astype(F32)


def tables_kernel(wx_ref, wz_ref, wzi_ref, wxi_ref, yb_ref, slope_ref, slope_z_ref):
    for parity in range(2):
        shape = (NX // 2, MX // 2)
        x = 2.0 * float_iota(shape, 0) + parity
        put_rotation(wx_ref, (parity,), 0, *cos_sin(x * float_iota(shape, 1)), True)
        shape = (MX // 2, NX // 2)
        x = 2.0 * float_iota(shape, 1) + parity
        put_rotation(wxi_ref, (parity,), 0, *cos_sin(x * float_iota(shape, 0)), False)
        shape = (NZ // 2, NZ)
        z = 4.0 * float_iota(shape, 0) + 2.0 * parity
        put_rotation(wzi_ref, (parity,), 0, *cos_sin(z * float_iota(shape, 1)), True)
    for chunk in range(NZ // Z_CHUNK):
        shape = (2 * Z_CHUNK, NZ)
        row = iota(shape, 0)
        kz = chunk * Z_CHUNK + jnp.where(row < Z_CHUNK, row, row + NZ - Z_CHUNK)
        angle = 2.0 * kz.astype(F32) * float_iota(shape, 1)
        put_rotation(wz_ref, (), chunk * 4 * Z_CHUNK, *cos_sin(angle), False)
    for slot in range(2):
        shape = (NY, ND)
        q = iota(shape, 1)
        ky = 4 * q + slot + jnp.where(q < ND // 2, 1, 0)
        c, s = cos_sin(ky.astype(F32) * float_iota(shape, 0))
        weight = jnp.where(ky == MY // 2, NORM, 2.0 * NORM)
        s = jnp.where(ky == MY // 2, -1.0, s)
        put_parts(yb_ref, (), slice(0, NY), slice(256 * slot, 256 * slot + 128), c * weight)
        put_parts(yb_ref, (), slice(0, NY), slice(256 * slot + 128, 256 * slot + 256), -s * weight)
    for part, value in enumerate(slope_parts(NY)):
        slope_ref[part] = value
    for part, value in enumerate(slope_parts(NZ)):
        slope_z_ref[part, :, 0:NZ] = value
        slope_z_ref[part, :, NZ : 2 * NZ] = value


def outward_kernel(
    dens_hbm, table_hbm, filt_hbm, out_hbm, plane_ref, dens_ref, table_ref, xc_ref, hart_ref, sems
):
    copies = [
        pltpu.make_async_copy(dens_hbm.at[0:NY, :], dens_ref.at[0:NY, :], sems.at[0]),
        pltpu.make_async_copy(dens_hbm.at[NY : 2 * NY, :], dens_ref.at[NY : 2 * NY, :], sems.at[1]),
        pltpu.make_async_copy(table_hbm, table_ref, sems.at[2]),
        pltpu.make_async_copy(filt_hbm.at[:, 0, :], plane_ref, sems.at[3]),
    ]
    for copy in copies:
        copy.start()
    slope = slope_parts(NY)
    parity = parity_matrix(False)
    for spin in range(2):
        copies[spin].wait()
        field = dens_ref[spin * NY : (spin + 1) * NY, :]
        grad = dot3(*slope, *split(field))
        for part in range(2):
            rows = slice(part * 128, part * 128 + 128)
            put_rows(xc_ref, spin * 4 + part * 2, HART, field[rows])
            put_rows(xc_ref, 8 + spin * 4 + part * 2, HART, grad[rows])
    leave_xc = pltpu.make_async_copy(
        xc_ref.reshape(ND, HART, 128), out_hbm.at[:, 0:HART, :], sems.at[4]
    )
    leave_xc.start()
    hi, lo = split(dens_ref[0:NY, :] + dens_ref[NY : 2 * NY, :])
    hi, lo = dot1(hi, parity), dot1(lo, parity)
    hi, lo = hi.astype(BF16), lo.astype(BF16)
    copies[2].wait()
    for s in range(4):
        rows = slice(s * ND, (s + 1) * ND)
        value = dot3(table_ref[0, rows, :], table_ref[1, rows, :], hi, lo)
        put_rows(hart_ref, s * 2, OUT_ROWS - HART, value)
    leave_hart = pltpu.make_async_copy(
        hart_ref.reshape(ND, OUT_ROWS - HART, 128), out_hbm.at[:, HART:OUT_ROWS, :], sems.at[5]
    )
    leave_hart.start()
    copies[3].wait()
    leave_xc.wait()
    leave_hart.wait()


def pw_piece(root, params):
    radius = root * root
    scale = 2.0 * params[0]
    series = root * (
        scale * params[2]
        + root * (scale * params[3] + root * (scale * params[4] + root * (scale * params[5])))
    )
    slope = root * (
        0.5 * scale * params[2]
        + root
        * (
            scale * params[3]
            + root * (1.5 * scale * params[4] + root * (2.0 * scale * params[5]))
        )
    )
    inv = 1.0 / (series * (series + 1.0))
    logarithm = jnp.log(1.0 + inv * (series + 1.0))
    front = -scale - (scale * params[1]) * radius
    value = front * logarithm
    deriv = (-scale * params[1]) * radius * logarithm - front * slope * inv
    return value, deriv


def exchange_piece(dens, inv_root, sigma):
    root = 2.0 * dens * inv_root * inv_root
    inv2 = inv_root * inv_root
    inv4 = inv2 * inv2
    reduced = sigma * (inv4 * inv4) * (1.0 / (3.0 * math.pi**2) ** (2.0 / 3.0))
    damp = 1.0 / (1.0 + (MU_X / KAPPA) * reduced)
    enhance = (1.0 + KAPPA) - KAPPA * damp
    front = -0.75 * (3.0 / math.pi) ** (1.0 / 3.0)
    damp_sq = MU_X * damp * damp
    energy = front * dens * root * enhance
    d_dens = (4.0 / 3.0 * front) * root * (enhance - 2.0 * reduced * damp_sq)
    d_sigma = (0.5 * front / (3.0 * math.pi**2) ** (2.0 / 3.0)) * damp_sq * inv4
    return energy, d_dens, d_sigma, root


def xc_point(up, down, sigma_uu, sigma_ud, sigma_dd):
    inv_up = jnp.exp(jnp.log(2.0 * up) * (-1.0 / 3.0))
    inv_down = jnp.exp(jnp.log(2.0 * down) * (-1.0 / 3.0))
    e_up, d_up, d_uu, root_up = exchange_piece(up, inv_up, sigma_uu)
    e_down, d_down, d_dd, root_down = exchange_piece(down, inv_down, sigma_dd)
    dens = up + down
    sixth = jnp.exp(jnp.log(dens) * (-1.0 / 6.0))
    inv_third = sixth * sixth
    third = dens * inv_third * inv_third
    inv_dens = inv_third * inv_third * inv_third
    zeta = (up - down) * inv_dens
    plus = 2.0 * up * inv_dens
    minus = 2.0 * down * inv_dens
    plus_cube = root_up * inv_third
    minus_cube = root_down * inv_third
    f_scale = 1.0 / (2.0 ** (4.0 / 3.0) - 2.0)
    f = (plus * plus_cube + minus * minus_cube - 2.0) * f_scale
    f_slope = (plus_cube - minus_cube) * (4.0 / 3.0 * f_scale)
    root = (3.0 / (4.0 * math.pi)) ** (1.0 / 6.0) * sixth
    e0, e0_d = pw_piece(root, PARAMS_UNPOL)
    e1, e1_d = pw_piece(root, PARAMS_POL)
    ac, ac_d = pw_piece(root, PARAMS_STIFF)
    z2 = zeta * zeta
    z3_4 = 4.0 * z2 * zeta
    z4 = z2 * z2
    one_z4 = (1.0 - z4) * (-1.0 / FZ_CURV)
    f_z4 = f * z4
    f_one = f * one_z4
    diff = e1 - e0
    local = e0 + ac * f_one + diff * f_z4
    local_r = e0_d + ac_d * f_one + (e1_d - e0_d) * f_z4
    fz3 = z3_4 * f
    local_z = ac * (f_slope * one_z4 + (1.0 / FZ_CURV) * fz3) + diff * (f_slope * z4 + fz3)
    phi = 0.5 * (plus_cube * plus_cube + minus_cube * minus_cube)
    inv_phi = 1.0 / phi
    phi_log_slope = (third * (1.0 / 3.0)) * (inv_up - inv_down) * inv_phi
    g3 = GAMMA_C * phi * phi * phi
    inv_g3 = (1.0 / GAMMA_C) * inv_phi * inv_phi * inv_phi
    grow = jnp.exp(-local * inv_g3)
    weight_a = (BETA_C / GAMMA_C) / (grow - 1.0)
    sigma = sigma_uu + 2.0 * sigma_ud + sigma_dd
    ct = math.pi / (16.0 * (3.0 * math.pi**2) ** (1.0 / 3.0))
    kt = ct * inv_third * inv_dens * inv_dens * inv_phi * inv_phi
    t2 = sigma * kt
    w = weight_a * t2
    num = 1.0 + w
    den = num + w * w
    add = (BETA_C / GAMMA_C) * t2 * num
    both = den + add
    inv_both = 1.0 / (den * both)
    h = g3 * jnp.log(1.0 + add * (inv_both * both))
    h_t = (BETA_C / GAMMA_C) * g3 * (1.0 + 2.0 * w) * inv_both
    h_a = -(w * w * w) * (2.0 + w) * grow * inv_both
    total = local + h
    ht_t2 = h_t * t2
    one_ha = 1.0 + h_a
    d_n = total - (1.0 / 3.0) * one_ha * local_r - (7.0 / 3.0) * ht_t2
    d_z = one_ha * local_z + phi_log_slope * (3.0 * (h - h_a * local) - 2.0 * ht_t2)
    d_sigma = dens * h_t * kt
    energy = e_up + e_down + dens * total
    return (
        energy,
        d_up + d_n + minus * d_z,
        d_down + d_n - plus * d_z,
        d_uu + d_sigma,
        2.0 * d_sigma,
        d_dd + d_sigma,
    )


def slope_along_z(slope_z_ref, hi, lo):
    both = jnp.concatenate([hi, lo], axis=0)
    return dot1(slope_z_ref[0], both) + dot1(slope_z_ref[1], both)


def slope_along_x(slope_ref, hi, lo):
    return -dot3(hi, lo, slope_ref[0], slope_ref[1])


def xc_steps(in_ref, slope_ref, slope_z_ref, out_ref, total_ref, dens, gz, gy, gx):
    def gradients(part):
        rows = slice(part * 128, part * 128 + 128)
        for spin in range(2):
            field = get_rows(in_ref, spin * 4 + part * 2, OUT_ROWS)
            dens[spin, rows, :] = field
            gy[spin, rows, :] = get_rows(in_ref, 8 + spin * 4 + part * 2, OUT_ROWS)
            hi, lo = split(field)
            gz[spin, rows, :] = slope_along_z(slope_z_ref, hi, lo)
            gx[spin, rows, :] = slope_along_x(slope_ref, hi, lo)

    def points(i):
        rows = slice(i * XC_ROWS, (i + 1) * XC_ROWS)
        zu, zd = gz[0, rows, :], gz[1, rows, :]
        yu, yd = gy[0, rows, :], gy[1, rows, :]
        xu, xd = gx[0, rows, :], gx[1, rows, :]
        energy, d_up, d_down, d_uu, d_ud, d_dd = xc_point(
            dens[0, rows, :],
            dens[1, rows, :],
            zu * zu + yu * yu + xu * xu,
            zu * zd + yu * yd + xu * xd,
            zd * zd + yd * yd + xd * xd,
        )
        dens[0, rows, :] = d_up
        dens[1, rows, :] = d_down
        for ref, gu, gd in ((gz, zu, zd), (gy, yu, yd), (gx, xu, xd)):
            ref[0, rows, :] = 2.0 * d_uu * gu + d_ud * gd
            ref[1, rows, :] = 2.0 * d_dd * gd + d_ud * gu
        folded = sum(energy[r : r + 8] for r in range(0, XC_ROWS, 8))
        total_ref[...] = folded if i == 0 else total_ref[...] + folded

    def divergence(part):
        rows = slice(part * 128, part * 128 + 128)
        for spin in range(2):
            div = slope_along_z(slope_z_ref, *split(gz[spin, rows, :]))
            div = div + slope_along_x(slope_ref, *split(gx[spin, rows, :]))
            put_rows(out_ref, spin * 4 + part * 2, BACK_ROWS, dens[spin, rows, :] - div)
            put_rows(out_ref, 8 + spin * 4 + part * 2, BACK_ROWS, gy[spin, rows, :])

    steps = []
    for part in range(2):
        steps.append(lambda part=part: gradients(part))
        for i in range(part * 128 // XC_ROWS, (part + 1) * 128 // XC_ROWS):
            steps.append(lambda i=i: points(i))
        steps.append(lambda part=part: divergence(part))
    return steps


def hartree_steps(
    in_ref, filt_ref, other_ref, weight_ref, wx_ref, wz_ref, wzi_ref, wxi_ref, out_ref, power_ref,
    xp, sums, back,
):
    def forward_x(slot, conjugate):
        parts = []
        for parity in range(2):
            base = HART + 4 * slot + parity
            real = in_ref[pl.ds(base, ND, stride=OUT_ROWS), :]
            imag = in_ref[pl.ds(base + 2, ND, stride=OUT_ROWS), :]
            both = jnp.concatenate([real, -imag if conjugate else imag], axis=1)
            parts.append(dot3(*split(both), wx_ref[parity, 0], wx_ref[parity, 1]))
        place = 2 if conjugate else slot
        for half, value in ((0, parts[0] + parts[1]), (1, parts[0] - parts[1])):
            cols = slice(half * 256, half * 256 + 256)
            hi, lo = split(value)
            xp[place, 0, 0:128, cols] = hi[:, 0:256]
            xp[place, 0, 128:256, cols] = hi[:, 256:512]
            xp[place, 1, 0:128, cols] = lo[:, 0:256]
            xp[place, 1, 128:256, cols] = lo[:, 256:512]

    def filtered(slot, c):
        rows = slice(c * 128, c * 128 + 128)
        spec = dot3(wz_ref[0, rows, :], wz_ref[1, rows, :], xp[slot, 0], xp[slot, 1])
        if slot == 0:
            mirror = dot3(wz_ref[0, rows, :], wz_ref[1, rows, :], xp[2, 0], xp[2, 1])
        planes = []
        for high in range(2):
            place = slice(high * NZ + c * Z_CHUNK, high * NZ + (c + 1) * Z_CHUNK)
            own = filt_ref[slot, place, :]
            if slot == 0:
                swap = (own - other_ref[place, :]) * weight_ref[2]
                planes.append((own - swap, swap))
            else:
                planes.append((own, None))
        acc = None
        for kind in range(2):
            pair = []
            for high in range(2):
                at = slice(kind * 64 + high * 32, kind * 64 + high * 32 + 32)
                value = spec[at] * planes[high][0]
                if slot == 0:
                    value = value + mirror[at] * planes[high][1]
                power = spec[at] * value
                power = power[0:8] + power[8:16] + (power[16:24] + power[24:32])
                acc = power if acc is None else acc + power
                pair.append(value)
            dest = slice(kind * NZ + c * Z_CHUNK, kind * NZ + (c + 1) * Z_CHUNK)
            for parity, value in ((0, pair[0] + pair[1]), (1, pair[0] - pair[1])):
                hi, lo = split(value)
                sums[slot, parity, 0, dest, :] = hi
                sums[slot, parity, 1, dest, :] = lo
        acc = weight_ref[slot] * acc
        power_ref[...] = acc if slot == 0 and c == 0 else power_ref[...] + acc

    def back_z(slot, parity):
        src = sums.at[slot, parity]
        grid = dot3(wzi_ref[parity, 0], wzi_ref[parity, 1], src[0], src[1])
        for sign in range(2):
            a, b = grid[:, 0:256], grid[:, 256:512]
            hi, lo = split(a + b if sign == 0 else a - b)
            for part, value in ((0, hi), (1, lo)):
                rows = slice(parity * 64, parity * 64 + 64)
                back[slot, sign, part, rows, 0:256] = value[0:64]
                back[slot, sign, part, rows, 256:512] = value[64:128]

    def back_x(slot, sign):
        src = back.at[slot, sign]
        value = dot3(src[0], src[1], wxi_ref[sign, 0], wxi_ref[sign, 1])
        for parity in range(2):
            for kind in range(2):
                put_rows(
                    out_ref,
                    parity * BACK_ROWS + HART + slot * 4 + kind * 2 + sign,
                    BACK_ROWS,
                    value[parity * 64 : parity * 64 + 64, kind * 128 : kind * 128 + 128],
                    count=64,
                    scale=2,
                )

    steps = []
    for slot in range(2):
        steps.append(lambda slot=slot: forward_x(slot, False))
        if slot == 0:
            steps.append(lambda: forward_x(0, True))
        for c in range(NZ // Z_CHUNK):
            steps.append(lambda slot=slot, c=c: filtered(slot, c))
        for parity in range(2):
            steps.append(lambda slot=slot, parity=parity: back_z(slot, parity))
        for sign in range(2):
            steps.append(lambda slot=slot, sign=sign: back_x(slot, sign))
    return steps


def middle_kernel(
    first_ref, weight_ref, in_ref, other_ref, slope_ref, slope_z_ref, filt_hbm, wx_hbm, wz_hbm, wzi_hbm,
    wxi_hbm, out_ref, filt_ref, wx_ref, wz_ref, wzi_ref, wxi_ref, dens, gz, gy, gx, xp, sums, back,
    total_ref, power_ref, sems,
):
    moves = [(wx_hbm, wx_ref), (wz_hbm, wz_ref)]
    moves += [
        (filt_hbm.at[:, first_ref[0] + slot, :], filt_ref.at[slot]) for slot in range(2)
    ]
    moves += [(wzi_hbm, wzi_ref), (wxi_hbm, wxi_ref)]
    copies = [
        pltpu.make_async_copy(source, target, sems.at[i]) for i, (source, target) in enumerate(moves)
    ]
    for copy in copies:
        copy.start()
    xc = xc_steps(in_ref, slope_ref, slope_z_ref, out_ref, total_ref, dens, gz, gy, gx)
    hartree = hartree_steps(
        in_ref, filt_ref, other_ref, weight_ref, wx_ref, wz_ref, wzi_ref, wxi_ref, out_ref,
        power_ref, xp, sums, back,
    )
    for step in xc[:XC_AHEAD]:
        step()
    xc = xc[XC_AHEAD:]
    done = 0
    waits = {0: copies[0:1], 2: copies[1:3], 6: copies[4:5], 8: copies[5:6], 11: copies[3:4]}
    for i, step in enumerate(hartree):
        for copy in waits.get(i, ()):
            copy.wait()
        step()
        upto = min(len(xc), -(-(i + 1) * len(xc) // XC_SPREAD))
        for other in xc[done:upto]:
            other()
        done = max(done, upto)
    for other in xc[done:]:
        other()
    energies = jnp.where(
        iota((ND, 128), 1) < 64, jnp.sum(total_ref[...]), jnp.sum(power_ref[...])
    )
    put_rows(out_ref, BACK_ROWS - 1, BACK_ROWS, energies)


def homeward_kernel(in_ref, yb_ref, slope_ref, out_ref, energy_ref):
    field = jnp.concatenate(
        [get_rows(in_ref, HART + 2 * s, BACK_ROWS) for s in range(4)], axis=0
    )
    grid = dot3(yb_ref[0], yb_ref[1], *split(field))
    hi, lo = split(grid)
    parity = parity_matrix(True)
    hartree = dot1(hi, parity) + dot1(lo, parity)
    for spin in range(2):
        flux, rest = (
            jnp.concatenate(
                [get_rows(in_ref, base + spin * 4 + part * 2, BACK_ROWS) for part in range(2)],
                axis=0,
            )
            for base in (8, 0)
        )
        rows = slice(spin * NY, (spin + 1) * NY)
        out_ref[rows, :] = rest + hartree - dot3(slope_ref[0], slope_ref[1], *split(flux))
    row = jnp.sum(in_ref[pl.ds(BACK_ROWS - 1, ND, stride=BACK_ROWS), :], axis=0, keepdims=True)
    first = iota((1, 128), 1) < 64
    energy_ref[0] = jnp.sum(jnp.where(first, row, 0.0)) * (1.0 / (64.0 * CELLS))
    energy_ref[1] = jnp.sum(jnp.where(first, 0.0, row)) * (0.5 * NORM / (64.0 * CELLS))


def call(kernel, outs, in_specs, flops, scratch=(), smem_out=(), hbm_out=(), limit=40, flags=None):
    specs = [SMEM if i in smem_out else HBM if i in hbm_out else VMEM for i in range(len(outs))]
    return pl.pallas_call(
        kernel,
        out_shape=list(outs),
        in_specs=in_specs,
        out_specs=specs,
        scratch_shapes=list(scratch),
        cost_estimate=pl.CostEstimate(flops=flops, bytes_accessed=4 << 20, transcendentals=0),
        compiler_params=pltpu.CompilerParams(vmem_limit_bytes=limit << 20, flags=flags),
        name=kernel.__name__,
    )


def in_hbm(value):
    return pltpu.with_memory_space_constraint(value, pltpu.HBM)


def arr(*shape, dtype=F32):
    return jax.ShapeDtypeStruct(shape, dtype)


def exchange(value, rows, group):
    shaped = value.reshape(ND * rows // group, group, 128)
    out = lax.all_to_all(shaped, GZ, split_axis=0, concat_axis=0, tiled=True)
    return out.reshape(ND * rows, 128)


def per_device(density, kernel_hat):
    q = lax.axis_index(GZ)
    kernel_hat = in_hbm(kernel_hat)
    outward, plane = call(
        outward_kernel,
        [arr(ND, OUT_ROWS, 128), arr(MZ, MX)],
        [HBM, HBM, HBM],
        400_000_000,
        scratch=[
            pltpu.VMEM((2 * NY, NX), F32),
            pltpu.VMEM((2, 4 * ND, NY), BF16),
            pltpu.VMEM((ND * HART, 128), F32),
            pltpu.VMEM((ND * (OUT_ROWS - HART), 128), F32),
            pltpu.SemaphoreType.DMA((6,)),
        ],
        hbm_out=(0,),
    )(in_hbm(density.reshape(2 * NY, NX)), in_hbm(jnp.asarray(y_forward())), kernel_hat)
    arrived = exchange(outward, OUT_ROWS, 8)
    other = lax.ppermute(plane, GZ, [(0, PAIR)])
    shapes = [(2, 2, NX, MX), (2, 2 * MZ, 2 * NZ), (2, 2, NZ, 2 * NZ), (2, 2, MX, NX)]
    wx, wz, wzi, wxi, yb, slope, slope_z = call(
        tables_kernel,
        [arr(*shape, dtype=BF16) for shape in shapes]
        + [
            arr(2, NY, 4 * ND, dtype=BF16),
            arr(2, NY, NY, dtype=BF16),
            arr(2, NZ, 2 * NZ, dtype=BF16),
        ],
        [],
        2_000_000_000,
    )()
    start = jnp.where(q < ND // 2, 1, 0).astype(jnp.int32).reshape(1)
    weights = jnp.stack(
        [jnp.where(q == PAIR, 1.0, 2.0), jnp.full((), 2.0), jnp.where(q == PAIR, 0.5, 0.0)]
    ).astype(F32)
    field = pltpu.VMEM((2, 256, NX), F32)
    (back,) = call(
        middle_kernel,
        [arr(ND * BACK_ROWS, 128)],
        [SMEM, SMEM] + [VMEM] * 4 + [HBM] * 5,
        8_000_000_000,
        scratch=[pltpu.VMEM((2, MZ, MX), F32)]
        + [pltpu.VMEM(shape, BF16) for shape in shapes]
        + [field] * 4
        + [
            pltpu.VMEM((3, 2, 256, 512), BF16),
            pltpu.VMEM((2, 2, 2, 256, 512), BF16),
            pltpu.VMEM((2, 2, 2, 128, 512), BF16),
            pltpu.VMEM((8, NX), F32),
            pltpu.VMEM((8, MX), F32),
            pltpu.SemaphoreType.DMA((6,)),
        ],
    )(start, weights, arrived, other, slope, slope_z, kernel_hat, *map(in_hbm, (wx, wz, wzi, wxi)))
    returned = exchange(back, BACK_ROWS, 1)
    potential, energies = call(
        homeward_kernel,
        [arr(2 * NY, NX), arr(2)],
        [VMEM] * 3,
        1_000_000_000,
        smem_out=(1,),
    )(returned, yb, slope)
    return potential.reshape(2, 1, NY, NX), energies


def solution(mesh):
    torus = Mesh(mesh.devices.reshape(4, 4, 4, 2), GZ)
    placed = (P(None, GZ, None, None), P(None, GZ, None))
    return jax.shard_map(
        per_device,
        mesh=torus,
        in_specs=placed,
        out_specs=(P(None, GZ, None, None), P()),
        check_vma=False,
    )
```

```python
import math

import jax
import jax.numpy as jnp
import numpy as np
from jax import lax
from jax.experimental import pallas as pl
from jax.experimental.pallas import tpu as pltpu
from jax.sharding import Mesh
from jax.sharding import PartitionSpec as P


GZ = ("gz_0", "gz_1", "gz_2", "gz_3")
HGRID = 0.35
STENCIL = (0.8, -0.2, 4.0 / 105.0, -1.0 / 280.0)
KAPPA = 0.804
MU_X = 0.2195149727645171
BETA_C = 0.06672455060314922
GAMMA_C = 0.031090690869654894
FZ_CURV = 1.709921
PARAMS_UNPOL = (0.031091, 0.2137, 7.5957, 3.5876, 1.6382, 0.49294)
PARAMS_POL = (0.015545, 0.20548, 14.1189, 6.1977, 3.3662, 0.62517)
PARAMS_STIFF = (0.016887, 0.11125, 10.357, 3.6231, 0.88026, 0.49671)

F32 = jnp.float32
BF16 = jnp.bfloat16
NZ, NY, NX = 128, 256, 256
MZ, MY, MX = 256, 512, 512
ND = 128
HART = 16
OUT_ROWS = 24
BACK_ROWS = 25
PAIR = ND // 2
CELLS = NZ * NY * NX
Z_CHUNK = 32
XC_ROWS = 8
XC_AHEAD = 10
XC_SPREAD = 20
NORM = 1.0 / (MX * MY * MZ)
VMEM = pl.BlockSpec(memory_space=pltpu.VMEM)
SMEM = pl.BlockSpec(memory_space=pltpu.SMEM)
HBM = pl.BlockSpec(memory_space=pltpu.HBM)


def halves(m):
    m = np.asarray(m, np.float32)
    hi = m.astype(BF16)
    lo = (m - hi.astype(np.float32)).astype(BF16)
    return np.stack([hi, lo])


def y_forward():
    y, q = np.arange(NY), np.arange(ND)
    first = np.where(q < ND // 2, 4 * q + 1, 4 * q)
    rows = []
    for ky in (first, first + 1):
        angle = 2.0 * np.pi * (np.outer(ky, y) % MY) / MY
        paired = (ky == MY // 2)[:, None]
        rows += [np.cos(angle), np.where(paired, 1.0, -np.sin(angle))]
    return halves(np.concatenate(rows, 0))


def split(value):
    hi = value.astype(BF16)
    lo = (value - hi.astype(F32)).astype(BF16)
    return hi, lo


def dot1(a, b):
    return jnp.dot(a, b, preferred_element_type=F32)


def dot3(a_hi, a_lo, b_hi, b_lo):
    return dot1(a_hi, b_hi) + (dot1(a_lo, b_hi) + dot1(a_hi, b_lo))


def put_rows(ref, row, rows, value, count=ND, scale=1):
    for half in range(value.shape[1] // 128):
        ref[pl.ds(row + half, count, stride=rows * scale), :] = value[
            :, half * 128 : half * 128 + 128
        ]


def get_rows(ref, row, rows):
    return jnp.concatenate(
        [ref[pl.ds(row + half, ND, stride=rows), :] for half in range(2)], axis=1
    )


def iota(shape, dim):
    return lax.broadcasted_iota(jnp.int32, shape, dim)


def slope_parts(n):
    offset = iota((n, n), 1) - iota((n, n), 0)
    parts = []
    coefs = halves([c / HGRID for c in STENCIL]).astype(np.float32)
    for part in range(2):
        value = jnp.zeros((n, n), F32)
        for k in range(1, 5):
            c = float(coefs[part, k - 1])
            value = jnp.where(offset == k, c, jnp.where(offset == -k, -c, value))
        parts.append(value.astype(BF16))
    return parts


def parity_matrix(transposed):
    x, place = iota((NX, NX), int(transposed)), iota((NX, NX), 1 - int(transposed))
    return jnp.where(place == (x & 1) * (NX // 2) + (x >> 1), 1.0, 0.0).astype(BF16)


def cos_sin(product):
    turn = product.astype(jnp.int32) & 511
    quarter = (turn + 64) >> 7
    angle = (turn - 128 * quarter).astype(F32) * (2.0 * math.pi / 512.0)
    sq = angle * angle
    s = angle * (
        1.0 + sq * (-1.0 / 6.0 + sq * (1.0 / 120.0 + sq * (-1.0 / 5040.0 + sq * (1.0 / 362880.0))))
    )
    c = 1.0 + sq * (-0.5 + sq * (1.0 / 24.0 + sq * (-1.0 / 720.0 + sq * (1.0 / 40320.0))))
    odd = (quarter & 1) == 1
    c, s = jnp.where(odd, s, c), jnp.where(odd, c, s)
    return (
        jnp.where(((quarter + 1) & 2) == 2, -c, c),
        jnp.where((quarter & 2) == 2, -s, s),
    )


def put_parts(ref, index, rows, cols, value):
    hi, lo = split(value)
    ref[(*index, 0, rows, cols)] = hi
    ref[(*index, 1, rows, cols)] = lo


def put_rotation(ref, index, row, c, s, transposed):
    n, m = c.shape
    top, low = slice(row, row + n), slice(row + n, row + 2 * n)
    put_parts(ref, index, top, slice(0, m), c)
    put_parts(ref, index, low, slice(m, 2 * m), c)
    put_parts(ref, index, top, slice(m, 2 * m), -s if transposed else s)
    put_parts(ref, index, low, slice(0, m), s if transposed else -s)


def float_iota(shape, dim):
    return iota(shape, dim).astype(F32)


def tables_kernel(wx_ref, wz_ref, wzi_ref, wxi_ref, yb_ref, slope_ref, slope_z_ref):
    for parity in range(2):
        shape = (NX // 2, MX // 2)
        x = 2.0 * float_iota(shape, 0) + parity
        put_rotation(wx_ref, (parity,), 0, *cos_sin(x * float_iota(shape, 1)), True)
        shape = (MX // 2, NX // 2)
        x = 2.0 * float_iota(shape, 1) + parity
        put_rotation(wxi_ref, (parity,), 0, *cos_sin(x * float_iota(shape, 0)), False)
        shape = (NZ // 2, NZ)
        z = 4.0 * float_iota(shape, 0) + 2.0 * parity
        put_rotation(wzi_ref, (parity,), 0, *cos_sin(z * float_iota(shape, 1)), True)
    for chunk in range(NZ // Z_CHUNK):
        shape = (2 * Z_CHUNK, NZ)
        row = iota(shape, 0)
        kz = chunk * Z_CHUNK + jnp.where(row < Z_CHUNK, row, row + NZ - Z_CHUNK)
        angle = 2.0 * kz.astype(F32) * float_iota(shape, 1)
        put_rotation(wz_ref, (), chunk * 4 * Z_CHUNK, *cos_sin(angle), False)
    for slot in range(2):
        shape = (NY, ND)
        q = iota(shape, 1)
        ky = 4 * q + slot + jnp.where(q < ND // 2, 1, 0)
        c, s = cos_sin(ky.astype(F32) * float_iota(shape, 0))
        weight = jnp.where(ky == MY // 2, NORM, 2.0 * NORM)
        s = jnp.where(ky == MY // 2, -1.0, s)
        put_parts(yb_ref, (), slice(0, NY), slice(256 * slot, 256 * slot + 128), c * weight)
        put_parts(yb_ref, (), slice(0, NY), slice(256 * slot + 128, 256 * slot + 256), -s * weight)
    for part, value in enumerate(slope_parts(NY)):
        slope_ref[part] = value
    for part, value in enumerate(slope_parts(NZ)):
        slope_z_ref[part, :, 0:NZ] = value
        slope_z_ref[part, :, NZ : 2 * NZ] = value


def outward_kernel(
    dens_hbm, table_hbm, filt_hbm, out_hbm, plane_ref, dens_ref, table_ref, xc_ref, hart_ref, sems
):
    copies = [
        pltpu.make_async_copy(dens_hbm.at[0:NY, :], dens_ref.at[0:NY, :], sems.at[0]),
        pltpu.make_async_copy(dens_hbm.at[NY : 2 * NY, :], dens_ref.at[NY : 2 * NY, :], sems.at[1]),
        pltpu.make_async_copy(table_hbm, table_ref, sems.at[2]),
        pltpu.make_async_copy(filt_hbm.at[:, 0, :], plane_ref, sems.at[3]),
    ]
    for copy in copies:
        copy.start()
    slope = slope_parts(NY)
    parity = parity_matrix(False)
    for spin in range(2):
        copies[spin].wait()
        field = dens_ref[spin * NY : (spin + 1) * NY, :]
        grad = dot3(*slope, *split(field))
        for part in range(2):
            rows = slice(part * 128, part * 128 + 128)
            put_rows(xc_ref, spin * 4 + part * 2, HART, field[rows])
            put_rows(xc_ref, 8 + spin * 4 + part * 2, HART, grad[rows])
    leave_xc = pltpu.make_async_copy(
        xc_ref.reshape(ND, HART, 128), out_hbm.at[:, 0:HART, :], sems.at[4]
    )
    leave_xc.start()
    hi, lo = split(dens_ref[0:NY, :] + dens_ref[NY : 2 * NY, :])
    hi, lo = dot1(hi, parity), dot1(lo, parity)
    hi, lo = hi.astype(BF16), lo.astype(BF16)
    copies[2].wait()
    for s in range(4):
        rows = slice(s * ND, (s + 1) * ND)
        value = dot3(table_ref[0, rows, :], table_ref[1, rows, :], hi, lo)
        put_rows(hart_ref, s * 2, OUT_ROWS - HART, value)
    leave_hart = pltpu.make_async_copy(
        hart_ref.reshape(ND, OUT_ROWS - HART, 128), out_hbm.at[:, HART:OUT_ROWS, :], sems.at[5]
    )
    leave_hart.start()
    copies[3].wait()
    leave_xc.wait()
    leave_hart.wait()


def pw_piece(root, params):
    radius = root * root
    scale = 2.0 * params[0]
    series = root * (
        scale * params[2]
        + root * (scale * params[3] + root * (scale * params[4] + root * (scale * params[5])))
    )
    slope = root * (
        0.5 * scale * params[2]
        + root
        * (
            scale * params[3]
            + root * (1.5 * scale * params[4] + root * (2.0 * scale * params[5]))
        )
    )
    inv = 1.0 / (series * (series + 1.0))
    logarithm = jnp.log(1.0 + inv * (series + 1.0))
    front = -scale - (scale * params[1]) * radius
    value = front * logarithm
    deriv = (-scale * params[1]) * radius * logarithm - front * slope * inv
    return value, deriv


def exchange_piece(dens, inv_root, sigma):
    root = 2.0 * dens * inv_root * inv_root
    inv2 = inv_root * inv_root
    inv4 = inv2 * inv2
    reduced = sigma * (inv4 * inv4) * (1.0 / (3.0 * math.pi**2) ** (2.0 / 3.0))
    damp = 1.0 / (1.0 + (MU_X / KAPPA) * reduced)
    enhance = (1.0 + KAPPA) - KAPPA * damp
    front = -0.75 * (3.0 / math.pi) ** (1.0 / 3.0)
    damp_sq = MU_X * damp * damp
    energy = front * dens * root * enhance
    d_dens = (4.0 / 3.0 * front) * root * (enhance - 2.0 * reduced * damp_sq)
    d_sigma = (0.5 * front / (3.0 * math.pi**2) ** (2.0 / 3.0)) * damp_sq * inv4
    return energy, d_dens, d_sigma, root


def xc_point(up, down, sigma_uu, sigma_ud, sigma_dd):
    inv_up = jnp.exp(jnp.log(2.0 * up) * (-1.0 / 3.0))
    inv_down = jnp.exp(jnp.log(2.0 * down) * (-1.0 / 3.0))
    e_up, d_up, d_uu, root_up = exchange_piece(up, inv_up, sigma_uu)
    e_down, d_down, d_dd, root_down = exchange_piece(down, inv_down, sigma_dd)
    dens = up + down
    sixth = jnp.exp(jnp.log(dens) * (-1.0 / 6.0))
    inv_third = sixth * sixth
    third = dens * inv_third * inv_third
    inv_dens = inv_third * inv_third * inv_third
    zeta = (up - down) * inv_dens
    plus = 2.0 * up * inv_dens
    minus = 2.0 * down * inv_dens
    plus_cube = root_up * inv_third
    minus_cube = root_down * inv_third
    f_scale = 1.0 / (2.0 ** (4.0 / 3.0) - 2.0)
    f = (plus * plus_cube + minus * minus_cube - 2.0) * f_scale
    f_slope = (plus_cube - minus_cube) * (4.0 / 3.0 * f_scale)
    root = (3.0 / (4.0 * math.pi)) ** (1.0 / 6.0) * sixth
    e0, e0_d = pw_piece(root, PARAMS_UNPOL)
    e1, e1_d = pw_piece(root, PARAMS_POL)
    ac, ac_d = pw_piece(root, PARAMS_STIFF)
    z2 = zeta * zeta
    z3_4 = 4.0 * z2 * zeta
    z4 = z2 * z2
    one_z4 = (1.0 - z4) * (-1.0 / FZ_CURV)
    f_z4 = f * z4
    f_one = f * one_z4
    diff = e1 - e0
    local = e0 + ac * f_one + diff * f_z4
    local_r = e0_d + ac_d * f_one + (e1_d - e0_d) * f_z4
    fz3 = z3_4 * f
    local_z = ac * (f_slope * one_z4 + (1.0 / FZ_CURV) * fz3) + diff * (f_slope * z4 + fz3)
    phi = 0.5 * (plus_cube * plus_cube + minus_cube * minus_cube)
    inv_phi = 1.0 / phi
    phi_log_slope = (third * (1.0 / 3.0)) * (inv_up - inv_down) * inv_phi
    g3 = GAMMA_C * phi * phi * phi
    inv_g3 = (1.0 / GAMMA_C) * inv_phi * inv_phi * inv_phi
    grow = jnp.exp(-local * inv_g3)
    weight_a = (BETA_C / GAMMA_C) / (grow - 1.0)
    sigma = sigma_uu + 2.0 * sigma_ud + sigma_dd
    ct = math.pi / (16.0 * (3.0 * math.pi**2) ** (1.0 / 3.0))
    kt = ct * inv_third * inv_dens * inv_dens * inv_phi * inv_phi
    t2 = sigma * kt
    w = weight_a * t2
    num = 1.0 + w
    den = num + w * w
    add = (BETA_C / GAMMA_C) * t2 * num
    both = den + add
    inv_both = 1.0 / (den * both)
    h = g3 * jnp.log(1.0 + add * (inv_both * both))
    h_t = (BETA_C / GAMMA_C) * g3 * (1.0 + 2.0 * w) * inv_both
    h_a = -(w * w * w) * (2.0 + w) * grow * inv_both
    total = local + h
    ht_t2 = h_t * t2
    one_ha = 1.0 + h_a
    d_n = total - (1.0 / 3.0) * one_ha * local_r - (7.0 / 3.0) * ht_t2
    d_z = one_ha * local_z + phi_log_slope * (3.0 * (h - h_a * local) - 2.0 * ht_t2)
    d_sigma = dens * h_t * kt
    energy = e_up + e_down + dens * total
    return (
        energy,
        d_up + d_n + minus * d_z,
        d_down + d_n - plus * d_z,
        d_uu + d_sigma,
        2.0 * d_sigma,
        d_dd + d_sigma,
    )


def slope_along_z(slope_z_ref, hi, lo):
    both = jnp.concatenate([hi, lo], axis=0)
    return dot1(slope_z_ref[0], both) + dot1(slope_z_ref[1], both)


def slope_along_x(slope_ref, hi, lo):
    return -dot3(hi, lo, slope_ref[0], slope_ref[1])


def xc_steps(in_ref, slope_ref, slope_z_ref, out_ref, total_ref, dens, gz, gy, gx):
    def gradients(part):
        rows = slice(part * 128, part * 128 + 128)
        for spin in range(2):
            field = get_rows(in_ref, spin * 4 + part * 2, OUT_ROWS)
            dens[spin, rows, :] = field
            gy[spin, rows, :] = get_rows(in_ref, 8 + spin * 4 + part * 2, OUT_ROWS)
            hi, lo = split(field)
            gz[spin, rows, :] = slope_along_z(slope_z_ref, hi, lo)
            gx[spin, rows, :] = slope_along_x(slope_ref, hi, lo)

    def points(i):
        rows = slice(i * XC_ROWS, (i + 1) * XC_ROWS)
        zu, zd = gz[0, rows, :], gz[1, rows, :]
        yu, yd = gy[0, rows, :], gy[1, rows, :]
        xu, xd = gx[0, rows, :], gx[1, rows, :]
        energy, d_up, d_down, d_uu, d_ud, d_dd = xc_point(
            dens[0, rows, :],
            dens[1, rows, :],
            zu * zu + yu * yu + xu * xu,
            zu * zd + yu * yd + xu * xd,
            zd * zd + yd * yd + xd * xd,
        )
        dens[0, rows, :] = d_up
        dens[1, rows, :] = d_down
        for ref, gu, gd in ((gz, zu, zd), (gy, yu, yd), (gx, xu, xd)):
            ref[0, rows, :] = 2.0 * d_uu * gu + d_ud * gd
            ref[1, rows, :] = 2.0 * d_dd * gd + d_ud * gu
        folded = sum(energy[r : r + 8] for r in range(0, XC_ROWS, 8))
        total_ref[...] = folded if i == 0 else total_ref[...] + folded

    def divergence(part):
        rows = slice(part * 128, part * 128 + 128)
        for spin in range(2):
            div = slope_along_z(slope_z_ref, *split(gz[spin, rows, :]))
            div = div + slope_along_x(slope_ref, *split(gx[spin, rows, :]))
            put_rows(out_ref, spin * 4 + part * 2, BACK_ROWS, dens[spin, rows, :] - div)
            put_rows(out_ref, 8 + spin * 4 + part * 2, BACK_ROWS, gy[spin, rows, :])

    steps = []
    for part in range(2):
        steps.append(lambda part=part: gradients(part))
        for i in range(part * 128 // XC_ROWS, (part + 1) * 128 // XC_ROWS):
            steps.append(lambda i=i: points(i))
        steps.append(lambda part=part: divergence(part))
    return steps


def hartree_steps(
    in_ref, filt_ref, other_ref, weight_ref, wx_ref, wz_ref, wzi_ref, wxi_ref, out_ref, power_ref,
    xp, sums, back,
):
    def forward_x(slot, conjugate):
        parts = []
        for parity in range(2):
            base = HART + 4 * slot + parity
            real = in_ref[pl.ds(base, ND, stride=OUT_ROWS), :]
            imag = in_ref[pl.ds(base + 2, ND, stride=OUT_ROWS), :]
            both = jnp.concatenate([real, -imag if conjugate else imag], axis=1)
            parts.append(dot3(*split(both), wx_ref[parity, 0], wx_ref[parity, 1]))
        place = 2 if conjugate else slot
        for half, value in ((0, parts[0] + parts[1]), (1, parts[0] - parts[1])):
            cols = slice(half * 256, half * 256 + 256)
            hi, lo = split(value)
            xp[place, 0, 0:128, cols] = hi[:, 0:256]
            xp[place, 0, 128:256, cols] = hi[:, 256:512]
            xp[place, 1, 0:128, cols] = lo[:, 0:256]
            xp[place, 1, 128:256, cols] = lo[:, 256:512]

    def filtered(slot, c):
        rows = slice(c * 128, c * 128 + 128)
        spec = dot3(wz_ref[0, rows, :], wz_ref[1, rows, :], xp[slot, 0], xp[slot, 1])
        if slot == 0:
            mirror = dot3(wz_ref[0, rows, :], wz_ref[1, rows, :], xp[2, 0], xp[2, 1])
        planes = []
        for high in range(2):
            place = slice(high * NZ + c * Z_CHUNK, high * NZ + (c + 1) * Z_CHUNK)
            own = filt_ref[slot, place, :]
            if slot == 0:
                swap = (own - other_ref[place, :]) * weight_ref[2]
                planes.append((own - swap, swap))
            else:
                planes.append((own, None))
        acc = None
        for kind in range(2):
            pair = []
            for high in range(2):
                at = slice(kind * 64 + high * 32, kind * 64 + high * 32 + 32)
                value = spec[at] * planes[high][0]
                if slot == 0:
                    value = value + mirror[at] * planes[high][1]
                power = spec[at] * value
                power = power[0:8] + power[8:16] + (power[16:24] + power[24:32])
                acc = power if acc is None else acc + power
                pair.append(value)
            dest = slice(kind * NZ + c * Z_CHUNK, kind * NZ + (c + 1) * Z_CHUNK)
            for parity, value in ((0, pair[0] + pair[1]), (1, pair[0] - pair[1])):
                hi, lo = split(value)
                sums[slot, parity, 0, dest, :] = hi
                sums[slot, parity, 1, dest, :] = lo
        acc = weight_ref[slot] * acc
        power_ref[...] = acc if slot == 0 and c == 0 else power_ref[...] + acc

    def back_z(slot, parity):
        src = sums.at[slot, parity]
        grid = dot3(wzi_ref[parity, 0], wzi_ref[parity, 1], src[0], src[1])
        for sign in range(2):
            a, b = grid[:, 0:256], grid[:, 256:512]
            hi, lo = split(a + b if sign == 0 else a - b)
            for part, value in ((0, hi), (1, lo)):
                rows = slice(parity * 64, parity * 64 + 64)
                back[slot, sign, part, rows, 0:256] = value[0:64]
                back[slot, sign, part, rows, 256:512] = value[64:128]

    def back_x(slot, sign):
        src = back.at[slot, sign]
        value = dot3(src[0], src[1], wxi_ref[sign, 0], wxi_ref[sign, 1])
        for parity in range(2):
            for kind in range(2):
                put_rows(
                    out_ref,
                    parity * BACK_ROWS + HART + slot * 4 + kind * 2 + sign,
                    BACK_ROWS,
                    value[parity * 64 : parity * 64 + 64, kind * 128 : kind * 128 + 128],
                    count=64,
                    scale=2,
                )

    steps = []
    for slot in range(2):
        steps.append(lambda slot=slot: forward_x(slot, False))
        if slot == 0:
            steps.append(lambda: forward_x(0, True))
        for c in range(NZ // Z_CHUNK):
            steps.append(lambda slot=slot, c=c: filtered(slot, c))
        for parity in range(2):
            steps.append(lambda slot=slot, parity=parity: back_z(slot, parity))
        for sign in range(2):
            steps.append(lambda slot=slot, sign=sign: back_x(slot, sign))
    return steps


def middle_kernel(
    first_ref, weight_ref, in_ref, other_ref, slope_ref, slope_z_ref, filt_hbm, wx_hbm, wz_hbm, wzi_hbm,
    wxi_hbm, out_ref, filt_ref, wx_ref, wz_ref, wzi_ref, wxi_ref, dens, gz, gy, gx, xp, sums, back,
    total_ref, power_ref, sems,
):
    moves = [(wx_hbm, wx_ref), (wz_hbm, wz_ref)]
    moves += [
        (filt_hbm.at[:, first_ref[0] + slot, :], filt_ref.at[slot]) for slot in range(2)
    ]
    moves += [(wzi_hbm, wzi_ref), (wxi_hbm, wxi_ref)]
    copies = [
        pltpu.make_async_copy(source, target, sems.at[i]) for i, (source, target) in enumerate(moves)
    ]
    for copy in copies:
        copy.start()
    xc = xc_steps(in_ref, slope_ref, slope_z_ref, out_ref, total_ref, dens, gz, gy, gx)
    hartree = hartree_steps(
        in_ref, filt_ref, other_ref, weight_ref, wx_ref, wz_ref, wzi_ref, wxi_ref, out_ref,
        power_ref, xp, sums, back,
    )
    for step in xc[:XC_AHEAD]:
        step()
    xc = xc[XC_AHEAD:]
    done = 0
    waits = {0: copies[0:1], 2: copies[1:3], 6: copies[4:5], 8: copies[5:6], 11: copies[3:4]}
    for i, step in enumerate(hartree):
        for copy in waits.get(i, ()):
            copy.wait()
        step()
        upto = min(len(xc), -(-(i + 1) * len(xc) // XC_SPREAD))
        for other in xc[done:upto]:
            other()
        done = max(done, upto)
    for other in xc[done:]:
        other()
    energies = jnp.where(
        iota((ND, 128), 1) < 64, jnp.sum(total_ref[...]), jnp.sum(power_ref[...])
    )
    put_rows(out_ref, BACK_ROWS - 1, BACK_ROWS, energies)


def homeward_kernel(in_ref, yb_ref, slope_ref, out_ref, energy_ref):
    field = jnp.concatenate(
        [get_rows(in_ref, HART + 2 * s, BACK_ROWS) for s in range(4)], axis=0
    )
    grid = dot3(yb_ref[0], yb_ref[1], *split(field))
    hi, lo = split(grid)
    parity = parity_matrix(True)
    hartree = dot1(hi, parity) + dot1(lo, parity)
    for spin in range(2):
        flux, rest = (
            jnp.concatenate(
                [get_rows(in_ref, base + spin * 4 + part * 2, BACK_ROWS) for part in range(2)],
                axis=0,
            )
            for base in (8, 0)
        )
        rows = slice(spin * NY, (spin + 1) * NY)
        out_ref[rows, :] = rest + hartree - dot3(slope_ref[0], slope_ref[1], *split(flux))
    row = jnp.sum(in_ref[pl.ds(BACK_ROWS - 1, ND, stride=BACK_ROWS), :], axis=0, keepdims=True)
    first = iota((1, 128), 1) < 64
    energy_ref[0] = jnp.sum(jnp.where(first, row, 0.0)) * (1.0 / (64.0 * CELLS))
    energy_ref[1] = jnp.sum(jnp.where(first, 0.0, row)) * (0.5 * NORM / (64.0 * CELLS))


def call(kernel, outs, in_specs, flops, scratch=(), smem_out=(), hbm_out=(), limit=40):
    specs = [SMEM if i in smem_out else HBM if i in hbm_out else VMEM for i in range(len(outs))]
    return pl.pallas_call(
        kernel,
        out_shape=list(outs),
        in_specs=in_specs,
        out_specs=specs,
        scratch_shapes=list(scratch),
        cost_estimate=pl.CostEstimate(flops=flops, bytes_accessed=4 << 20, transcendentals=0),
        compiler_params=pltpu.CompilerParams(vmem_limit_bytes=limit << 20),
    )


def in_hbm(value):
    return pltpu.with_memory_space_constraint(value, pltpu.HBM)


def arr(*shape, dtype=F32):
    return jax.ShapeDtypeStruct(shape, dtype)


def exchange(value, rows, group):
    shaped = value.reshape(ND * rows // group, group, 128)
    out = lax.all_to_all(shaped, GZ, split_axis=0, concat_axis=0, tiled=True)
    return out.reshape(ND * rows, 128)


def per_device(density, kernel_hat):
    q = lax.axis_index(GZ)
    kernel_hat = in_hbm(kernel_hat)
    outward, plane = call(
        outward_kernel,
        [arr(ND, OUT_ROWS, 128), arr(MZ, MX)],
        [HBM, HBM, HBM],
        400_000_000,
        scratch=[
            pltpu.VMEM((2 * NY, NX), F32),
            pltpu.VMEM((2, 4 * ND, NY), BF16),
            pltpu.VMEM((ND * HART, 128), F32),
            pltpu.VMEM((ND * (OUT_ROWS - HART), 128), F32),
            pltpu.SemaphoreType.DMA((6,)),
        ],
        hbm_out=(0,),
    )(in_hbm(density.reshape(2 * NY, NX)), in_hbm(jnp.asarray(y_forward())), kernel_hat)
    other = lax.ppermute(plane, GZ, [(0, PAIR)])
    arrived = exchange(outward, OUT_ROWS, 8)
    shapes = [(2, 2, NX, MX), (2, 2 * MZ, 2 * NZ), (2, 2, NZ, 2 * NZ), (2, 2, MX, NX)]
    wx, wz, wzi, wxi, yb, slope, slope_z = call(
        tables_kernel,
        [arr(*shape, dtype=BF16) for shape in shapes]
        + [
            arr(2, NY, 4 * ND, dtype=BF16),
            arr(2, NY, NY, dtype=BF16),
            arr(2, NZ, 2 * NZ, dtype=BF16),
        ],
        [],
        2_000_000_000,
    )()
    start = jnp.where(q < ND // 2, 1, 0).astype(jnp.int32).reshape(1)
    weights = jnp.stack(
        [jnp.where(q == PAIR, 1.0, 2.0), jnp.full((), 2.0), jnp.where(q == PAIR, 0.5, 0.0)]
    ).astype(F32)
    field = pltpu.VMEM((2, 256, NX), F32)
    (back,) = call(
        middle_kernel,
        [arr(ND * BACK_ROWS, 128)],
        [SMEM, SMEM] + [VMEM] * 4 + [HBM] * 5,
        8_000_000_000,
        scratch=[pltpu.VMEM((2, MZ, MX), F32)]
        + [pltpu.VMEM(shape, BF16) for shape in shapes]
        + [field] * 4
        + [
            pltpu.VMEM((3, 2, 256, 512), BF16),
            pltpu.VMEM((2, 2, 2, 256, 512), BF16),
            pltpu.VMEM((2, 2, 2, 128, 512), BF16),
            pltpu.VMEM((8, NX), F32),
            pltpu.VMEM((8, MX), F32),
            pltpu.SemaphoreType.DMA((6,)),
        ],
    )(start, weights, arrived, other, slope, slope_z, kernel_hat, *map(in_hbm, (wx, wz, wzi, wxi)))
    returned = exchange(back, BACK_ROWS, 1)
    potential, energies = call(
        homeward_kernel,
        [arr(2 * NY, NX), arr(2)],
        [VMEM] * 3,
        1_000_000_000,
        smem_out=(1,),
    )(returned, yb, slope)
    return potential.reshape(2, 1, NY, NX), energies


def solution(mesh):
    torus = Mesh(mesh.devices.reshape(4, 4, 4, 2), GZ)
    placed = (P(None, GZ, None, None), P(None, GZ, None))
    return jax.shard_map(
        per_device,
        mesh=torus,
        in_specs=placed,
        out_specs=(P(None, GZ, None, None), P()),
        check_vma=False,
    )
```

```python
import math

import jax
import jax.numpy as jnp
import numpy as np
from jax import lax
from jax.experimental import pallas as pl
from jax.experimental.pallas import tpu as pltpu
from jax.sharding import Mesh
from jax.sharding import PartitionSpec as P

GZ = ("gz_0", "gz_1", "gz_2", "gz_3")
HGRID = 0.35
STENCIL = (0.8, -0.2, 4.0 / 105.0, -1.0 / 280.0)
KAPPA = 0.804
MU_X = 0.2195149727645171
BETA_C = 0.06672455060314922
GAMMA_C = 0.031090690869654894
FZ_CURV = 1.709921
PARAMS_UNPOL = (0.031091, 0.2137, 7.5957, 3.5876, 1.6382, 0.49294)
PARAMS_POL = (0.015545, 0.20548, 14.1189, 6.1977, 3.3662, 0.62517)
PARAMS_STIFF = (0.016887, 0.11125, 10.357, 3.6231, 0.88026, 0.49671)

F32 = jnp.float32
BF16 = jnp.bfloat16
NZ, NY, NX = 128, 256, 256
MZ, MY, MX = 256, 512, 512
ND = 128
HART = 16
OUT_ROWS = 24
BACK_ROWS = 25
PAIR = ND // 2
CELLS = NZ * NY * NX
Z_CHUNK = 32
XC_ROWS = 8
XC_AHEAD = 12
XC_SPREAD = 19
HART_ORDER = (
    "x00", "x01", "x10", "z00", "z01", "z02", "z03", "z10",
    "b00", "z11", "b01", "z12", "o00", "z13", "o01", "b10",
    "b11", "o10", "o11",
)
NORM = 1.0 / (MX * MY * MZ)
VMEM = pl.BlockSpec(memory_space=pltpu.VMEM)
SMEM = pl.BlockSpec(memory_space=pltpu.SMEM)
HBM = pl.BlockSpec(memory_space=pltpu.HBM)


def halves(m):
    m = np.asarray(m, np.float32)
    hi = m.astype(BF16)
    lo = (m - hi.astype(np.float32)).astype(BF16)
    return np.stack([hi, lo])


def y_forward():
    y, q = np.arange(NY), np.arange(ND)
    first = np.where(q < ND // 2, 4 * q + 1, 4 * q)
    rows = []
    for ky in (first, first + 1):
        angle = 2.0 * np.pi * (np.outer(ky, y) % MY) / MY
        paired = (ky == MY // 2)[:, None]
        rows += [np.cos(angle), np.where(paired, 1.0, -np.sin(angle))]
    return halves(np.concatenate(rows, 0))


def split(value):
    hi = value.astype(BF16)
    lo = (value - hi.astype(F32)).astype(BF16)
    return hi, lo


def dot1(a, b):
    return jnp.dot(a, b, preferred_element_type=F32)


def dot3(a_hi, a_lo, b_hi, b_lo):
    return dot1(a_hi, b_hi) + (dot1(a_lo, b_hi) + dot1(a_hi, b_lo))


def put_rows(ref, row, rows, value, count=ND, scale=1):
    for half in range(value.shape[1] // 128):
        ref[pl.ds(row + half, count, stride=rows * scale), :] = value[
            :, half * 128 : half * 128 + 128
        ]


def get_rows(ref, row, rows):
    return jnp.concatenate(
        [ref[pl.ds(row + half, ND, stride=rows), :] for half in range(2)], axis=1
    )


def iota(shape, dim):
    return lax.broadcasted_iota(jnp.int32, shape, dim)


def slope_parts(n):
    offset = iota((n, n), 1) - iota((n, n), 0)
    parts = []
    coefs = halves([c / HGRID for c in STENCIL]).astype(np.float32)
    for part in range(2):
        value = jnp.zeros((n, n), F32)
        for k in range(1, 5):
            c = float(coefs[part, k - 1])
            value = jnp.where(offset == k, c, jnp.where(offset == -k, -c, value))
        parts.append(value.astype(BF16))
    return parts


def parity_matrix(transposed):
    x, place = iota((NX, NX), int(transposed)), iota((NX, NX), 1 - int(transposed))
    return jnp.where(place == (x & 1) * (NX // 2) + (x >> 1), 1.0, 0.0).astype(BF16)


def cos_sin(product):
    turn = product.astype(jnp.int32) & 511
    quarter = (turn + 64) >> 7
    angle = (turn - 128 * quarter).astype(F32) * (2.0 * math.pi / 512.0)
    sq = angle * angle
    s = angle * (
        1.0 + sq * (-1.0 / 6.0 + sq * (1.0 / 120.0 + sq * (-1.0 / 5040.0 + sq * (1.0 / 362880.0))))
    )
    c = 1.0 + sq * (-0.5 + sq * (1.0 / 24.0 + sq * (-1.0 / 720.0 + sq * (1.0 / 40320.0))))
    odd = (quarter & 1) == 1
    c, s = jnp.where(odd, s, c), jnp.where(odd, c, s)
    return (
        jnp.where(((quarter + 1) & 2) == 2, -c, c),
        jnp.where((quarter & 2) == 2, -s, s),
    )


def put_parts(ref, index, rows, cols, value):
    hi, lo = split(value)
    ref[(*index, 0, rows, cols)] = hi
    ref[(*index, 1, rows, cols)] = lo


def put_rotation(ref, index, row, c, s, transposed):
    n, m = c.shape
    top, low = slice(row, row + n), slice(row + n, row + 2 * n)
    put_parts(ref, index, top, slice(0, m), c)
    put_parts(ref, index, low, slice(m, 2 * m), c)
    put_parts(ref, index, top, slice(m, 2 * m), -s if transposed else s)
    put_parts(ref, index, low, slice(0, m), s if transposed else -s)


def float_iota(shape, dim):
    return iota(shape, dim).astype(F32)


def tables_kernel(wx_ref, wz_ref, wzi_ref, wxi_ref, yb_ref, slope_ref, slope_z_ref):
    for parity in range(2):
        shape = (NX // 2, MX // 2)
        x = 2.0 * float_iota(shape, 0) + parity
        put_rotation(wx_ref, (parity,), 0, *cos_sin(x * float_iota(shape, 1)), True)
        shape = (MX // 2, NX // 2)
        x = 2.0 * float_iota(shape, 1) + parity
        put_rotation(wxi_ref, (parity,), 0, *cos_sin(x * float_iota(shape, 0)), False)
        shape = (NZ // 2, NZ)
        z = 4.0 * float_iota(shape, 0) + 2.0 * parity
        put_rotation(wzi_ref, (parity,), 0, *cos_sin(z * float_iota(shape, 1)), True)
    for chunk in range(NZ // Z_CHUNK):
        shape = (2 * Z_CHUNK, NZ)
        row = iota(shape, 0)
        kz = chunk * Z_CHUNK + jnp.where(row < Z_CHUNK, row, row + NZ - Z_CHUNK)
        angle = 2.0 * kz.astype(F32) * float_iota(shape, 1)
        put_rotation(wz_ref, (), chunk * 4 * Z_CHUNK, *cos_sin(angle), False)
    for slot in range(2):
        shape = (NY, ND)
        q = iota(shape, 1)
        ky = 4 * q + slot + jnp.where(q < ND // 2, 1, 0)
        c, s = cos_sin(ky.astype(F32) * float_iota(shape, 0))
        weight = jnp.where(ky == MY // 2, NORM, 2.0 * NORM)
        s = jnp.where(ky == MY // 2, -1.0, s)
        put_parts(yb_ref, (), slice(0, NY), slice(256 * slot, 256 * slot + 128), c * weight)
        put_parts(yb_ref, (), slice(0, NY), slice(256 * slot + 128, 256 * slot + 256), -s * weight)
    for part, value in enumerate(slope_parts(NY)):
        slope_ref[part] = value
    for part, value in enumerate(slope_parts(NZ)):
        slope_z_ref[part, :, 0:NZ] = value
        slope_z_ref[part, :, NZ : 2 * NZ] = value


def plane_kernel(filt_hbm, out_ref, sem):
    copy = pltpu.make_async_copy(filt_hbm.at[:, 0, :], out_ref, sem)
    copy.start()
    copy.wait()


def outward_kernel(dens_hbm, table_hbm, out_ref, dens_ref, table_ref, sems):
    dens_copy = pltpu.make_async_copy(dens_hbm, dens_ref, sems.at[0])
    table_copy = pltpu.make_async_copy(table_hbm, table_ref, sems.at[1])
    dens_copy.start()
    table_copy.start()
    slope = slope_parts(NY)
    parity = parity_matrix(False)
    dens_copy.wait()
    for spin in range(2):
        field = dens_ref[spin * NY : (spin + 1) * NY, :]
        grad = dot3(*slope, *split(field))
        for part in range(2):
            rows = slice(part * 128, part * 128 + 128)
            put_rows(out_ref, spin * 4 + part * 2, OUT_ROWS, field[rows])
            put_rows(out_ref, 8 + spin * 4 + part * 2, OUT_ROWS, grad[rows])
    hi, lo = split(dens_ref[0:NY, :] + dens_ref[NY : 2 * NY, :])
    hi, lo = dot1(hi, parity), dot1(lo, parity)
    hi, lo = hi.astype(BF16), lo.astype(BF16)
    table_copy.wait()
    for s in range(4):
        rows = slice(s * ND, (s + 1) * ND)
        value = dot3(table_ref[0, rows, :], table_ref[1, rows, :], hi, lo)
        put_rows(out_ref, HART + s * 2, OUT_ROWS, value)


LN2 = math.log(2.0)


def pw_piece(powers, params):
    root, radius, cube, square = powers
    scale = 2.0 * params[0]
    t1, t2 = (scale * params[2]) * root, (scale * params[3]) * radius
    t3, t4 = (scale * params[4]) * cube, (scale * params[5]) * square
    series = (t1 + t2) + (t3 + t4)
    slope = (series + t4) + 0.5 * (t3 - t1)
    more = series + 1.0
    inv = 1.0 / (series * more)
    logarithm = jnp.log(1.0 + inv * more)
    tilt = (-scale * params[1]) * radius
    front = tilt - scale
    return front * logarithm, tilt * logarithm - (front * slope) * inv


def exchange_piece(twice, inv_root, sigma):
    inv2 = inv_root * inv_root
    inv4 = inv2 * inv2
    root = twice * inv2
    front = -0.75 * (3.0 / math.pi) ** (1.0 / 3.0)
    unit = 1.0 / (3.0 * math.pi**2) ** (2.0 / 3.0)
    damp = 1.0 / (1.0 + (MU_X / KAPPA * unit) * sigma * (inv4 * inv4))
    gain = KAPPA - KAPPA * damp
    scaled = front * root
    energy = twice * scaled * (1.0 + gain)
    d_dens = scaled * (4.0 / 3.0 + gain * (4.0 / 3.0 - (8.0 / 3.0) * damp))
    d_sigma = (front * MU_X * unit) * (damp * damp) * inv4
    return energy, d_dens, d_sigma, root


def xc_point(up, down, sigma_uu, sigma_ud, sigma_dd):
    twice_up, twice_down = up + up, down + down
    inv_up = jnp.exp2(jnp.log(twice_up) * (-1.0 / (3.0 * LN2)))
    inv_down = jnp.exp2(jnp.log(twice_down) * (-1.0 / (3.0 * LN2)))
    e_up, d_up, d_uu, root_up = exchange_piece(twice_up, inv_up, sigma_uu)
    e_down, d_down, d_dd, root_down = exchange_piece(twice_down, inv_down, sigma_dd)
    dens = up + down
    sixth = jnp.exp2(jnp.log(dens) * (-1.0 / (6.0 * LN2)))
    inv_third = sixth * sixth
    inv_two = inv_third * inv_third
    third = dens * inv_two
    inv_dens = inv_two * inv_third
    plus = twice_up * inv_dens
    minus = twice_down * inv_dens
    zeta = 0.5 * (plus - minus)
    plus_cube = root_up * inv_third
    minus_cube = root_down * inv_third
    f_scale = 1.0 / (2.0 ** (4.0 / 3.0) - 2.0)
    f = (plus * plus_cube + minus * minus_cube) * f_scale - 2.0 * f_scale
    f_slope = (plus_cube - minus_cube) * (4.0 / 3.0 * f_scale)
    root = (3.0 / (4.0 * math.pi)) ** (1.0 / 6.0) * sixth
    radius = root * root
    powers = (root, radius, radius * root, radius * radius)
    e0, e0_d = pw_piece(powers, PARAMS_UNPOL)
    e1, e1_d = pw_piece(powers, PARAMS_POL)
    ac, ac_d = pw_piece(powers, PARAMS_STIFF)
    z2 = zeta * zeta
    z4 = z2 * z2
    one_z4 = z4 * (1.0 / FZ_CURV) - 1.0 / FZ_CURV
    f_z4 = f * z4
    f_one = f * one_z4
    diff = e1 - e0
    local = e0 + ac * f_one + diff * f_z4
    local_r = e0_d + ac_d * f_one + (e1_d - e0_d) * f_z4
    local_z = (ac * one_z4 + diff * z4) * f_slope + (ac * (1.0 / FZ_CURV) + diff) * (
        4.0 * f * z2 * zeta
    )
    phi2 = plus_cube * plus_cube + minus_cube * minus_cube
    inv_phi2 = 1.0 / phi2
    inv_sq = inv_phi2 * inv_phi2
    phi_log_slope = (third * (inv_up - inv_down)) * ((2.0 / 3.0) * inv_phi2)
    g3 = (GAMMA_C / 8.0) * (phi2 * phi2) * phi2
    grow = jnp.exp2(local * (inv_sq * inv_phi2) * (-8.0 / (GAMMA_C * LN2)))
    weight_a = (BETA_C / GAMMA_C) / (grow - 1.0)
    sigma = (sigma_uu + sigma_dd) + (sigma_ud + sigma_ud)
    ct = 4.0 * math.pi / (16.0 * (3.0 * math.pi**2) ** (1.0 / 3.0))
    kt = (ct * inv_third) * (inv_dens * inv_dens) * inv_sq
    t2 = sigma * kt
    w = weight_a * t2
    num = 1.0 + w
    den = num + w * w
    add = (BETA_C / GAMMA_C) * t2 * num
    both = den + add
    inv_both = 1.0 / (den * both)
    h = g3 * jnp.log(1.0 + add * (inv_both * both))
    h_t = ((BETA_C / GAMMA_C) * g3) * ((num + w) * inv_both)
    h_a = -((w * w) * w) * ((1.0 + num) * grow) * inv_both
    total = local + h
    ht_t2 = h_t * t2
    one_ha = 1.0 + h_a
    d_n = total - one_ha * ((1.0 / 3.0) * local_r) - (7.0 / 3.0) * ht_t2
    d_z = one_ha * local_z + phi_log_slope * (3.0 * (h - h_a * local) - (ht_t2 + ht_t2))
    d_sigma = 2.0 * (dens * h_t * kt)
    energy = 0.5 * (e_up + e_down) + dens * total
    return (
        energy,
        d_up + d_n + minus * d_z,
        d_down + d_n - plus * d_z,
        d_uu + d_sigma,
        d_sigma,
        d_dd + d_sigma,
    )


def slope_along_z(slope_z_ref, hi, lo):
    both = jnp.concatenate([hi, lo], axis=0)
    return dot1(slope_z_ref[0], both) + dot1(slope_z_ref[1], both)


def slope_along_x(slope_ref, hi, lo):
    return -dot3(hi, lo, slope_ref[0], slope_ref[1])


def xc_steps(in_ref, slope_ref, slope_z_ref, out_ref, total_ref, dens, gz, gy, gx):
    def gradients(part):
        rows = slice(part * 128, part * 128 + 128)
        for spin in range(2):
            field = get_rows(in_ref, spin * 4 + part * 2, OUT_ROWS)
            dens[spin, rows, :] = field
            gy[spin, rows, :] = get_rows(in_ref, 8 + spin * 4 + part * 2, OUT_ROWS)
            hi, lo = split(field)
            gz[spin, rows, :] = slope_along_z(slope_z_ref, hi, lo)
            gx[spin, rows, :] = slope_along_x(slope_ref, hi, lo)

    def points(i):
        rows = slice(i * XC_ROWS, (i + 1) * XC_ROWS)
        zu, zd = gz[0, rows, :], gz[1, rows, :]
        yu, yd = gy[0, rows, :], gy[1, rows, :]
        xu, xd = gx[0, rows, :], gx[1, rows, :]
        energy, d_up, d_down, d_uu, d_ud, d_dd = xc_point(
            dens[0, rows, :],
            dens[1, rows, :],
            zu * zu + yu * yu + xu * xu,
            zu * zd + yu * yd + xu * xd,
            zd * zd + yd * yd + xd * xd,
        )
        dens[0, rows, :] = d_up
        dens[1, rows, :] = d_down
        for ref, gu, gd in ((gz, zu, zd), (gy, yu, yd), (gx, xu, xd)):
            ref[0, rows, :] = d_uu * gu + d_ud * gd
            ref[1, rows, :] = d_dd * gd + d_ud * gu
        folded = sum(energy[r : r + 8] for r in range(0, XC_ROWS, 8))
        total_ref[...] = folded if i == 0 else total_ref[...] + folded

    def divergence(part):
        rows = slice(part * 128, part * 128 + 128)
        for spin in range(2):
            div = slope_along_z(slope_z_ref, *split(gz[spin, rows, :]))
            div = div + slope_along_x(slope_ref, *split(gx[spin, rows, :]))
            put_rows(out_ref, spin * 4 + part * 2, BACK_ROWS, dens[spin, rows, :] - div)
            put_rows(out_ref, 8 + spin * 4 + part * 2, BACK_ROWS, gy[spin, rows, :])

    steps = []
    for part in range(2):
        steps.append(lambda part=part: gradients(part))
        for i in range(part * 128 // XC_ROWS, (part + 1) * 128 // XC_ROWS):
            steps.append(lambda i=i: points(i))
        steps.append(lambda part=part: divergence(part))
    return steps


def hartree_steps(
    in_ref, filt_ref, other_ref, weight_ref, wx_ref, wz_ref, wzi_ref, wxi_ref, out_ref, power_ref,
    xp, sums, back,
):
    def forward_x(slot, conjugate):
        parts = []
        for parity in range(2):
            base = HART + 4 * slot + parity
            real = in_ref[pl.ds(base, ND, stride=OUT_ROWS), :]
            imag = in_ref[pl.ds(base + 2, ND, stride=OUT_ROWS), :]
            both = jnp.concatenate([real, -imag if conjugate else imag], axis=1)
            parts.append(dot3(*split(both), wx_ref[parity, 0], wx_ref[parity, 1]))
        place = 2 if conjugate else slot
        for half, value in ((0, parts[0] + parts[1]), (1, parts[0] - parts[1])):
            cols = slice(half * 256, half * 256 + 256)
            hi, lo = split(value)
            xp[place, 0, 0:128, cols] = hi[:, 0:256]
            xp[place, 0, 128:256, cols] = hi[:, 256:512]
            xp[place, 1, 0:128, cols] = lo[:, 0:256]
            xp[place, 1, 128:256, cols] = lo[:, 256:512]

    def filtered(slot, c):
        rows = slice(c * 128, c * 128 + 128)
        spec = dot3(wz_ref[0, rows, :], wz_ref[1, rows, :], xp[slot, 0], xp[slot, 1])
        if slot == 0:
            mirror = dot3(wz_ref[0, rows, :], wz_ref[1, rows, :], xp[2, 0], xp[2, 1])
        planes = []
        for high in range(2):
            place = slice(high * NZ + c * Z_CHUNK, high * NZ + (c + 1) * Z_CHUNK)
            own = filt_ref[slot, place, :]
            if slot == 0:
                swap = (own - other_ref[place, :]) * weight_ref[2]
                planes.append((own - swap, swap))
            else:
                planes.append((own, None))
        acc = None
        first = slot == 0 and c == 0
        for kind in range(2):
            pair = []
            for high in range(2):
                at = slice(kind * 64 + high * 32, kind * 64 + high * 32 + 32)
                value = spec[at] * planes[high][0]
                if slot == 0:
                    value = value + mirror[at] * planes[high][1]
                power = spec[at] * value
                power = power[0:8] + power[8:16] + (power[16:24] + power[24:32])
                acc = power if acc is None else acc + power
                pair.append(value)
            dest = slice(kind * NZ + c * Z_CHUNK, kind * NZ + (c + 1) * Z_CHUNK)
            for parity, value in ((0, pair[0] + pair[1]), (1, pair[0] - pair[1])):
                hi, lo = split(value)
                sums[slot, parity, 0, dest, :] = hi
                sums[slot, parity, 1, dest, :] = lo
        acc = weight_ref[slot] * acc
        power_ref[...] = acc if first else power_ref[...] + acc

    def back_z(slot, parity):
        src = sums.at[slot, parity]
        grid = dot3(wzi_ref[parity, 0], wzi_ref[parity, 1], src[0], src[1])
        for sign in range(2):
            a, b = grid[:, 0:256], grid[:, 256:512]
            hi, lo = split(a + b if sign == 0 else a - b)
            for part, value in ((0, hi), (1, lo)):
                rows = slice(parity * 64, parity * 64 + 64)
                back[slot, sign, part, rows, 0:256] = value[0:64]
                back[slot, sign, part, rows, 256:512] = value[64:128]

    def back_x(slot, sign):
        src = back.at[slot, sign]
        value = dot3(src[0], src[1], wxi_ref[sign, 0], wxi_ref[sign, 1])
        for parity in range(2):
            for kind in range(2):
                put_rows(
                    out_ref,
                    parity * BACK_ROWS + HART + slot * 4 + kind * 2 + sign,
                    BACK_ROWS,
                    value[parity * 64 : parity * 64 + 64, kind * 128 : kind * 128 + 128],
                    count=64,
                    scale=2,
                )

    kinds = {
        "x": lambda slot, i: forward_x(slot, i == 1),
        "z": filtered,
        "b": back_z,
        "o": back_x,
    }
    return [
        (name, lambda name=name: kinds[name[0]](int(name[1]), int(name[2])))
        for name in HART_ORDER
    ]


def middle_kernel(
    first_ref, weight_ref, in_ref, other_ref, slope_ref, slope_z_ref, filt_hbm, wx_hbm, wz_hbm, wzi_hbm,
    wxi_hbm, out_ref, filt_ref, wx_ref, wz_ref, wzi_ref, wxi_ref, dens, gz, gy, gx, xp, sums, back,
    total_ref, power_ref, sems,
):
    moves = [(wx_hbm, wx_ref), (wz_hbm, wz_ref)]
    moves += [
        (filt_hbm.at[:, first_ref[0] + slot, :], filt_ref.at[slot]) for slot in range(2)
    ]
    moves += [(wzi_hbm, wzi_ref), (wxi_hbm, wxi_ref)]
    copies = [
        pltpu.make_async_copy(source, target, sems.at[i]) for i, (source, target) in enumerate(moves)
    ]
    for copy in copies:
        copy.start()
    xc = xc_steps(in_ref, slope_ref, slope_z_ref, out_ref, total_ref, dens, gz, gy, gx)
    hartree = hartree_steps(
        in_ref, filt_ref, other_ref, weight_ref, wx_ref, wz_ref, wzi_ref, wxi_ref, out_ref,
        power_ref, xp, sums, back,
    )
    for step in xc[:XC_AHEAD]:
        step()
    xc = xc[XC_AHEAD:]
    done = 0
    waits = {"x00": (0,), "z00": (1, 2), "z10": (3,), "b00": (4,), "o00": (5,)}
    for i, (name, step) in enumerate(hartree):
        for copy in waits.get(name, ()):
            copies[copy].wait()
        step()
        upto = min(len(xc), -(-(i + 1) * len(xc) // XC_SPREAD))
        for other in xc[done:upto]:
            other()
        done = max(done, upto)
    for other in xc[done:]:
        other()
    energies = jnp.where(
        iota((ND, 128), 1) < 64, jnp.sum(total_ref[...]), jnp.sum(power_ref[...])
    )
    put_rows(out_ref, BACK_ROWS - 1, BACK_ROWS, energies)


def homeward_kernel(in_ref, yb_ref, slope_ref, out_ref, energy_ref):
    field = jnp.concatenate(
        [get_rows(in_ref, HART + 2 * s, BACK_ROWS) for s in range(4)], axis=0
    )
    grid = dot3(yb_ref[0], yb_ref[1], *split(field))
    hi, lo = split(grid)
    parity = parity_matrix(True)
    hartree = dot1(hi, parity) + dot1(lo, parity)
    for spin in range(2):
        flux, rest = (
            jnp.concatenate(
                [get_rows(in_ref, base + spin * 4 + part * 2, BACK_ROWS) for part in range(2)],
                axis=0,
            )
            for base in (8, 0)
        )
        rows = slice(spin * NY, (spin + 1) * NY)
        out_ref[rows, :] = rest + hartree - dot3(slope_ref[0], slope_ref[1], *split(flux))
    row = jnp.sum(in_ref[pl.ds(BACK_ROWS - 1, ND, stride=BACK_ROWS), :], axis=0, keepdims=True)
    first = iota((1, 128), 1) < 64
    energy_ref[0] = jnp.sum(jnp.where(first, row, 0.0)) * (1.0 / (64.0 * CELLS))
    energy_ref[1] = jnp.sum(jnp.where(first, 0.0, row)) * (0.5 * NORM / (64.0 * CELLS))


def call(kernel, outs, in_specs, flops, scratch=(), smem_out=(), limit=40, flags=None):
    specs = [SMEM if i in smem_out else VMEM for i in range(len(outs))]
    return pl.pallas_call(
        kernel,
        out_shape=list(outs),
        in_specs=in_specs,
        out_specs=specs,
        scratch_shapes=list(scratch),
        cost_estimate=pl.CostEstimate(flops=flops, bytes_accessed=4 << 20, transcendentals=0),
        compiler_params=pltpu.CompilerParams(vmem_limit_bytes=limit << 20, flags=flags),
        name=kernel.__name__,
    )


def in_hbm(value):
    return pltpu.with_memory_space_constraint(value, pltpu.HBM)


def arr(*shape, dtype=F32):
    return jax.ShapeDtypeStruct(shape, dtype)


def exchange(value, rows, group):
    shaped = value.reshape(ND * rows // group, group, 128)
    out = lax.all_to_all(shaped, GZ, split_axis=0, concat_axis=0, tiled=True)
    return out.reshape(ND * rows, 128)


def per_device(density, kernel_hat):
    q = lax.axis_index(GZ)
    (outward,) = call(
        outward_kernel,
        [arr(ND * OUT_ROWS, 128)],
        [HBM, HBM],
        400_000_000,
        scratch=[
            pltpu.VMEM((2 * NY, NX), F32),
            pltpu.VMEM((2, 4 * ND, NY), BF16),
            pltpu.SemaphoreType.DMA((2,)),
        ],
    )(in_hbm(density.reshape(2 * NY, NX)), in_hbm(jnp.asarray(y_forward())))
    outward, kernel_hat = lax.optimization_barrier((outward, in_hbm(kernel_hat)))
    kernel_hat = in_hbm(kernel_hat)
    arrived = exchange(outward, OUT_ROWS, 8)
    (plane,) = call(
        plane_kernel, [arr(MZ, MX)], [HBM], 1_000_000, scratch=[pltpu.SemaphoreType.DMA(())]
    )(kernel_hat)
    other = lax.ppermute(plane, GZ, [(0, PAIR)])
    shapes = [(2, 2, NX, MX), (2, 2 * MZ, 2 * NZ), (2, 2, NZ, 2 * NZ), (2, 2, MX, NX)]
    wx, wz, wzi, wxi, yb, slope, slope_z = call(
        tables_kernel,
        [arr(*shape, dtype=BF16) for shape in shapes]
        + [
            arr(2, NY, 4 * ND, dtype=BF16),
            arr(2, NY, NY, dtype=BF16),
            arr(2, NZ, 2 * NZ, dtype=BF16),
        ],
        [],
        2_000_000_000,
    )()
    start = jnp.where(q < ND // 2, 1, 0).astype(jnp.int32).reshape(1)
    weights = jnp.stack(
        [jnp.where(q == PAIR, 1.0, 2.0), jnp.full((), 2.0), jnp.where(q == PAIR, 0.5, 0.0)]
    ).astype(F32)
    field = pltpu.VMEM((2, 256, NX), F32)
    (back,) = call(
        middle_kernel,
        [arr(ND * BACK_ROWS, 128)],
        [SMEM, SMEM] + [VMEM] * 4 + [HBM] * 5,
        8_000_000_000,
        scratch=[pltpu.VMEM((2, MZ, MX), F32)]
        + [pltpu.VMEM(shape, BF16) for shape in shapes]
        + [field] * 4
        + [
            pltpu.VMEM((3, 2, 256, 512), BF16),
            pltpu.VMEM((2, 2, 2, 256, 512), BF16),
            pltpu.VMEM((2, 2, 2, 128, 512), BF16),
            pltpu.VMEM((8, NX), F32),
            pltpu.VMEM((8, MX), F32),
            pltpu.SemaphoreType.DMA((6,)),
        ],
    )(start, weights, arrived, other, slope, slope_z, kernel_hat, *map(in_hbm, (wx, wz, wzi, wxi)))
    returned = exchange(back, BACK_ROWS, 1)
    potential, energies = call(
        homeward_kernel,
        [arr(2 * NY, NX), arr(2)],
        [VMEM] * 3,
        1_000_000_000,
        smem_out=(1,),
    )(returned, yb, slope)
    return potential.reshape(2, 1, NY, NX), energies


def solution(mesh):
    torus = Mesh(mesh.devices.reshape(4, 4, 4, 2), GZ)
    placed = (P(None, GZ, None, None), P(None, GZ, None))
    return jax.shard_map(
        per_device,
        mesh=torus,
        in_specs=placed,
        out_specs=(P(None, GZ, None, None), P()),
        check_vma=False,
    )
```

```python
import math

import jax
import jax.numpy as jnp
import numpy as np
from jax import lax
from jax.experimental import pallas as pl
from jax.experimental.pallas import tpu as pltpu
from jax.sharding import Mesh
from jax.sharding import PartitionSpec as P

GZ = ("gz_0", "gz_1", "gz_2", "gz_3")
BLOCKS = ("gz_3", "gz_0", "gz_1", "gz_2")
HGRID = 0.35
STENCIL = (0.8, -0.2, 4.0 / 105.0, -1.0 / 280.0)
KAPPA = 0.804
MU_X = 0.2195149727645171
BETA_C = 0.06672455060314922
GAMMA_C = 0.031090690869654894
FZ_CURV = 1.709921
PARAMS_UNPOL = (0.031091, 0.2137, 7.5957, 3.5876, 1.6382, 0.49294)
PARAMS_POL = (0.015545, 0.20548, 14.1189, 6.1977, 3.3662, 0.62517)
PARAMS_STIFF = (0.016887, 0.11125, 10.357, 3.6231, 0.88026, 0.49671)

F32 = jnp.float32
BF16 = jnp.bfloat16
NZ, NY, NX = 128, 256, 256
MZ, MY, MX = 256, 512, 512
ND = 128
HART = 16
OUT_ROWS = 24
BACK_ROWS = 25
PAIR = ND // 2
CELLS = NZ * NY * NX
Z_CHUNK = 32
XC_ROWS = 8
XC_AHEAD = 12
XC_SPREAD = 19
HART_ORDER = (
    "x00", "x01", "x10", "z00", "z01", "z02", "z03", "z10",
    "b00", "z11", "b01", "z12", "o00", "z13", "o01", "b10",
    "b11", "o10", "o11",
)
NORM = 1.0 / (MX * MY * MZ)
VMEM = pl.BlockSpec(memory_space=pltpu.VMEM)
SMEM = pl.BlockSpec(memory_space=pltpu.SMEM)
HBM = pl.BlockSpec(memory_space=pltpu.HBM)


def halves(m):
    m = np.asarray(m, np.float32)
    hi = m.astype(BF16)
    lo = (m - hi.astype(np.float32)).astype(BF16)
    return np.stack([hi, lo])


def device_of(block):
    return (block & (ND // 2 - 1)) * 2 + (block >> 6)


def y_forward():
    y, q = np.arange(NY), device_of(np.arange(ND))
    first = np.where(q < ND // 2, 4 * q + 1, 4 * q)
    rows = []
    for ky in (first, first + 1):
        angle = 2.0 * np.pi * (np.outer(ky, y) % MY) / MY
        paired = (ky == MY // 2)[:, None]
        rows += [np.cos(angle), np.where(paired, 1.0, -np.sin(angle))]
    return halves(np.concatenate(rows, 0))


def split(value):
    hi = value.astype(BF16)
    lo = (value - hi.astype(F32)).astype(BF16)
    return hi, lo


def dot1(a, b):
    return jnp.dot(a, b, preferred_element_type=F32)


def dot3(a_hi, a_lo, b_hi, b_lo):
    return dot1(a_hi, b_hi) + (dot1(a_lo, b_hi) + dot1(a_hi, b_lo))


def put_rows(ref, row, rows, value, count=ND):
    for half in range(value.shape[1] // 128):
        ref[pl.ds(row + half, count, stride=rows), :] = value[
            :, half * 128 : half * 128 + 128
        ]


def get_rows(ref, row, rows):
    return jnp.concatenate(
        [ref[pl.ds(row + half, ND, stride=rows), :] for half in range(2)], axis=1
    )


def iota(shape, dim):
    return lax.broadcasted_iota(jnp.int32, shape, dim)


def slope_parts(n, place=lambda i: i):
    offset = place(iota((n, n), 1)) - place(iota((n, n), 0))
    parts = []
    coefs = halves([c / HGRID for c in STENCIL]).astype(np.float32)
    for part in range(2):
        value = jnp.zeros((n, n), F32)
        for k in range(1, 5):
            c = float(coefs[part, k - 1])
            value = jnp.where(offset == k, c, jnp.where(offset == -k, -c, value))
        parts.append(value.astype(BF16))
    return parts


def parity_matrix(transposed):
    x, place = iota((NX, NX), int(transposed)), iota((NX, NX), 1 - int(transposed))
    return jnp.where(place == (x & 1) * (NX // 2) + (x >> 1), 1.0, 0.0).astype(BF16)


def cos_sin(product):
    turn = product.astype(jnp.int32) & 511
    quarter = (turn + 64) >> 7
    angle = (turn - 128 * quarter).astype(F32) * (2.0 * math.pi / 512.0)
    sq = angle * angle
    s = angle * (
        1.0 + sq * (-1.0 / 6.0 + sq * (1.0 / 120.0 + sq * (-1.0 / 5040.0 + sq * (1.0 / 362880.0))))
    )
    c = 1.0 + sq * (-0.5 + sq * (1.0 / 24.0 + sq * (-1.0 / 720.0 + sq * (1.0 / 40320.0))))
    odd = (quarter & 1) == 1
    c, s = jnp.where(odd, s, c), jnp.where(odd, c, s)
    return (
        jnp.where(((quarter + 1) & 2) == 2, -c, c),
        jnp.where((quarter & 2) == 2, -s, s),
    )


def put_parts(ref, index, rows, cols, value):
    hi, lo = split(value)
    ref[(*index, 0, rows, cols)] = hi
    ref[(*index, 1, rows, cols)] = lo


def put_rotation(ref, index, row, c, s, transposed):
    n, m = c.shape
    top, low = slice(row, row + n), slice(row + n, row + 2 * n)
    put_parts(ref, index, top, slice(0, m), c)
    put_parts(ref, index, low, slice(m, 2 * m), c)
    put_parts(ref, index, top, slice(m, 2 * m), -s if transposed else s)
    put_parts(ref, index, low, slice(0, m), s if transposed else -s)


def float_iota(shape, dim):
    return iota(shape, dim).astype(F32)


def tables_kernel(wx_ref, wz_ref, wzi_ref, wxi_ref, yb_ref, slope_ref, slope_z_ref):
    for parity in range(2):
        shape = (NX // 2, MX // 2)
        x = 2.0 * float_iota(shape, 0) + parity
        put_rotation(wx_ref, (parity,), 0, *cos_sin(x * float_iota(shape, 1)), True)
        shape = (MX // 2, NX // 2)
        x = 2.0 * float_iota(shape, 1) + parity
        put_rotation(wxi_ref, (parity,), 0, *cos_sin(x * float_iota(shape, 0)), False)
        shape = (NZ // 2, NZ)
        z = 4.0 * float_iota(shape, 0) + 2.0 * parity
        put_rotation(wzi_ref, (parity,), 0, *cos_sin(z * float_iota(shape, 1)), True)
    for chunk in range(NZ // Z_CHUNK):
        shape = (2 * Z_CHUNK, NZ)
        row = iota(shape, 0)
        kz = chunk * Z_CHUNK + jnp.where(row < Z_CHUNK, row, row + NZ - Z_CHUNK)
        angle = 2.0 * kz.astype(F32) * device_of(iota(shape, 1)).astype(F32)
        put_rotation(wz_ref, (), chunk * 4 * Z_CHUNK, *cos_sin(angle), False)
    for slot in range(2):
        shape = (NY, ND)
        q = device_of(iota(shape, 1))
        ky = 4 * q + slot + jnp.where(q < ND // 2, 1, 0)
        c, s = cos_sin(ky.astype(F32) * float_iota(shape, 0))
        weight = jnp.where(ky == MY // 2, NORM, 2.0 * NORM)
        s = jnp.where(ky == MY // 2, -1.0, s)
        put_parts(yb_ref, (), slice(0, NY), slice(256 * slot, 256 * slot + 128), c * weight)
        put_parts(yb_ref, (), slice(0, NY), slice(256 * slot + 128, 256 * slot + 256), -s * weight)
    for part, value in enumerate(slope_parts(NY)):
        slope_ref[part] = value
    for part, value in enumerate(slope_parts(NZ, device_of)):
        slope_z_ref[part, :, 0:NZ] = value
        slope_z_ref[part, :, NZ : 2 * NZ] = value


def plane_kernel(filt_hbm, out_ref, sem):
    copy = pltpu.make_async_copy(filt_hbm.at[:, 0, :], out_ref, sem)
    copy.start()
    copy.wait()


def outward_kernel(dens_hbm, table_hbm, out_ref, dens_ref, table_ref, sems):
    dens_copy = pltpu.make_async_copy(dens_hbm, dens_ref, sems.at[0])
    table_copy = pltpu.make_async_copy(table_hbm, table_ref, sems.at[1])
    dens_copy.start()
    table_copy.start()
    slope = slope_parts(NY)
    parity = parity_matrix(False)
    dens_copy.wait()
    for spin in range(2):
        field = dens_ref[spin * NY : (spin + 1) * NY, :]
        grad = dot3(*slope, *split(field))
        for part in range(2):
            rows = slice(part * 128, part * 128 + 128)
            put_rows(out_ref, spin * 4 + part * 2, OUT_ROWS, field[rows])
            put_rows(out_ref, 8 + spin * 4 + part * 2, OUT_ROWS, grad[rows])
    hi, lo = split(dens_ref[0:NY, :] + dens_ref[NY : 2 * NY, :])
    hi, lo = dot1(hi, parity), dot1(lo, parity)
    hi, lo = hi.astype(BF16), lo.astype(BF16)
    table_copy.wait()
    for s in range(4):
        rows = slice(s * ND, (s + 1) * ND)
        value = dot3(table_ref[0, rows, :], table_ref[1, rows, :], hi, lo)
        put_rows(out_ref, HART + s * 2, OUT_ROWS, value)


LN2 = math.log(2.0)


def pw_piece(powers, params):
    root, radius, cube, square = powers
    scale = 2.0 * params[0]
    t1, t2 = (scale * params[2]) * root, (scale * params[3]) * radius
    t3, t4 = (scale * params[4]) * cube, (scale * params[5]) * square
    series = (t1 + t2) + (t3 + t4)
    slope = (series + t4) + 0.5 * (t3 - t1)
    more = series + 1.0
    inv = 1.0 / (series * more)
    logarithm = jnp.log(1.0 + inv * more)
    tilt = (-scale * params[1]) * radius
    front = tilt - scale
    return front * logarithm, tilt * logarithm - (front * slope) * inv


def exchange_piece(twice, inv_root, sigma):
    inv2 = inv_root * inv_root
    inv4 = inv2 * inv2
    root = twice * inv2
    front = -0.75 * (3.0 / math.pi) ** (1.0 / 3.0)
    unit = 1.0 / (3.0 * math.pi**2) ** (2.0 / 3.0)
    damp = 1.0 / (1.0 + (MU_X / KAPPA * unit) * sigma * (inv4 * inv4))
    gain = KAPPA - KAPPA * damp
    scaled = front * root
    energy = twice * scaled * (1.0 + gain)
    d_dens = scaled * (4.0 / 3.0 + gain * (4.0 / 3.0 - (8.0 / 3.0) * damp))
    d_sigma = (front * MU_X * unit) * (damp * damp) * inv4
    return energy, d_dens, d_sigma, root


def xc_point(up, down, sigma_uu, sigma_ud, sigma_dd):
    twice_up, twice_down = up + up, down + down
    inv_up = jnp.exp2(jnp.log(twice_up) * (-1.0 / (3.0 * LN2)))
    inv_down = jnp.exp2(jnp.log(twice_down) * (-1.0 / (3.0 * LN2)))
    e_up, d_up, d_uu, root_up = exchange_piece(twice_up, inv_up, sigma_uu)
    e_down, d_down, d_dd, root_down = exchange_piece(twice_down, inv_down, sigma_dd)
    dens = up + down
    sixth = jnp.exp2(jnp.log(dens) * (-1.0 / (6.0 * LN2)))
    inv_third = sixth * sixth
    inv_two = inv_third * inv_third
    third = dens * inv_two
    inv_dens = inv_two * inv_third
    plus = twice_up * inv_dens
    minus = twice_down * inv_dens
    zeta = 0.5 * (plus - minus)
    plus_cube = root_up * inv_third
    minus_cube = root_down * inv_third
    f_scale = 1.0 / (2.0 ** (4.0 / 3.0) - 2.0)
    f = (plus * plus_cube + minus * minus_cube) * f_scale - 2.0 * f_scale
    f_slope = (plus_cube - minus_cube) * (4.0 / 3.0 * f_scale)
    root = (3.0 / (4.0 * math.pi)) ** (1.0 / 6.0) * sixth
    radius = root * root
    powers = (root, radius, radius * root, radius * radius)
    e0, e0_d = pw_piece(powers, PARAMS_UNPOL)
    e1, e1_d = pw_piece(powers, PARAMS_POL)
    ac, ac_d = pw_piece(powers, PARAMS_STIFF)
    z2 = zeta * zeta
    z4 = z2 * z2
    one_z4 = z4 * (1.0 / FZ_CURV) - 1.0 / FZ_CURV
    f_z4 = f * z4
    f_one = f * one_z4
    diff = e1 - e0
    local = e0 + ac * f_one + diff * f_z4
    local_r = e0_d + ac_d * f_one + (e1_d - e0_d) * f_z4
    local_z = (ac * one_z4 + diff * z4) * f_slope + (ac * (1.0 / FZ_CURV) + diff) * (
        4.0 * f * z2 * zeta
    )
    phi2 = plus_cube * plus_cube + minus_cube * minus_cube
    inv_phi2 = 1.0 / phi2
    inv_sq = inv_phi2 * inv_phi2
    phi_log_slope = (third * (inv_up - inv_down)) * ((2.0 / 3.0) * inv_phi2)
    g3 = (GAMMA_C / 8.0) * (phi2 * phi2) * phi2
    grow = jnp.exp2(local * (inv_sq * inv_phi2) * (-8.0 / (GAMMA_C * LN2)))
    weight_a = (BETA_C / GAMMA_C) / (grow - 1.0)
    sigma = (sigma_uu + sigma_dd) + (sigma_ud + sigma_ud)
    ct = 4.0 * math.pi / (16.0 * (3.0 * math.pi**2) ** (1.0 / 3.0))
    kt = (ct * inv_third) * (inv_dens * inv_dens) * inv_sq
    t2 = sigma * kt
    w = weight_a * t2
    num = 1.0 + w
    den = num + w * w
    add = (BETA_C / GAMMA_C) * t2 * num
    both = den + add
    inv_both = 1.0 / (den * both)
    h = g3 * jnp.log(1.0 + add * (inv_both * both))
    h_t = ((BETA_C / GAMMA_C) * g3) * ((num + w) * inv_both)
    h_a = -((w * w) * w) * ((1.0 + num) * grow) * inv_both
    total = local + h
    ht_t2 = h_t * t2
    one_ha = 1.0 + h_a
    d_n = total - one_ha * ((1.0 / 3.0) * local_r) - (7.0 / 3.0) * ht_t2
    d_z = one_ha * local_z + phi_log_slope * (3.0 * (h - h_a * local) - (ht_t2 + ht_t2))
    d_sigma = 2.0 * (dens * h_t * kt)
    energy = 0.5 * (e_up + e_down) + dens * total
    return (
        energy,
        d_up + d_n + minus * d_z,
        d_down + d_n - plus * d_z,
        d_uu + d_sigma,
        d_sigma,
        d_dd + d_sigma,
    )


def slope_along_z(slope_z_ref, hi, lo):
    both = jnp.concatenate([hi, lo], axis=0)
    return dot1(slope_z_ref[0], both) + dot1(slope_z_ref[1], both)


def slope_along_x(slope_ref, hi, lo):
    return -dot3(hi, lo, slope_ref[0], slope_ref[1])


def xc_steps(in_ref, slope_ref, slope_z_ref, out_ref, total_ref, dens, gz, gy, gx):
    def gradients(part):
        rows = slice(part * 128, part * 128 + 128)
        for spin in range(2):
            field = get_rows(in_ref, spin * 4 + part * 2, OUT_ROWS)
            dens[spin, rows, :] = field
            gy[spin, rows, :] = get_rows(in_ref, 8 + spin * 4 + part * 2, OUT_ROWS)
            hi, lo = split(field)
            gz[spin, rows, :] = slope_along_z(slope_z_ref, hi, lo)
            gx[spin, rows, :] = slope_along_x(slope_ref, hi, lo)

    def points(i):
        rows = slice(i * XC_ROWS, (i + 1) * XC_ROWS)
        zu, zd = gz[0, rows, :], gz[1, rows, :]
        yu, yd = gy[0, rows, :], gy[1, rows, :]
        xu, xd = gx[0, rows, :], gx[1, rows, :]
        energy, d_up, d_down, d_uu, d_ud, d_dd = xc_point(
            dens[0, rows, :],
            dens[1, rows, :],
            zu * zu + yu * yu + xu * xu,
            zu * zd + yu * yd + xu * xd,
            zd * zd + yd * yd + xd * xd,
        )
        dens[0, rows, :] = d_up
        dens[1, rows, :] = d_down
        for ref, gu, gd in ((gz, zu, zd), (gy, yu, yd), (gx, xu, xd)):
            ref[0, rows, :] = d_uu * gu + d_ud * gd
            ref[1, rows, :] = d_dd * gd + d_ud * gu
        folded = sum(energy[r : r + 8] for r in range(0, XC_ROWS, 8))
        total_ref[...] = folded if i == 0 else total_ref[...] + folded

    def divergence(part):
        rows = slice(part * 128, part * 128 + 128)
        for spin in range(2):
            div = slope_along_z(slope_z_ref, *split(gz[spin, rows, :]))
            div = div + slope_along_x(slope_ref, *split(gx[spin, rows, :]))
            put_rows(out_ref, spin * 4 + part * 2, BACK_ROWS, dens[spin, rows, :] - div)
            put_rows(out_ref, 8 + spin * 4 + part * 2, BACK_ROWS, gy[spin, rows, :])

    steps = []
    for part in range(2):
        steps.append(lambda part=part: gradients(part))
        for i in range(part * 128 // XC_ROWS, (part + 1) * 128 // XC_ROWS):
            steps.append(lambda i=i: points(i))
        steps.append(lambda part=part: divergence(part))
    return steps


def hartree_steps(
    in_ref, filt_ref, other_ref, weight_ref, wx_ref, wz_ref, wzi_ref, wxi_ref, out_ref, power_ref,
    xp, sums, back,
):
    def forward_x(slot, conjugate):
        parts = []
        for parity in range(2):
            base = HART + 4 * slot + parity
            real = in_ref[pl.ds(base, ND, stride=OUT_ROWS), :]
            imag = in_ref[pl.ds(base + 2, ND, stride=OUT_ROWS), :]
            both = jnp.concatenate([real, -imag if conjugate else imag], axis=1)
            parts.append(dot3(*split(both), wx_ref[parity, 0], wx_ref[parity, 1]))
        place = 2 if conjugate else slot
        for half, value in ((0, parts[0] + parts[1]), (1, parts[0] - parts[1])):
            cols = slice(half * 256, half * 256 + 256)
            hi, lo = split(value)
            xp[place, 0, 0:128, cols] = hi[:, 0:256]
            xp[place, 0, 128:256, cols] = hi[:, 256:512]
            xp[place, 1, 0:128, cols] = lo[:, 0:256]
            xp[place, 1, 128:256, cols] = lo[:, 256:512]

    def filtered(slot, c):
        rows = slice(c * 128, c * 128 + 128)
        spec = dot3(wz_ref[0, rows, :], wz_ref[1, rows, :], xp[slot, 0], xp[slot, 1])
        if slot == 0:
            mirror = dot3(wz_ref[0, rows, :], wz_ref[1, rows, :], xp[2, 0], xp[2, 1])
        planes = []
        for high in range(2):
            place = slice(high * NZ + c * Z_CHUNK, high * NZ + (c + 1) * Z_CHUNK)
            own = filt_ref[slot, place, :]
            if slot == 0:
                swap = (own - other_ref[place, :]) * weight_ref[2]
                planes.append((own - swap, swap))
            else:
                planes.append((own, None))
        acc = None
        first = slot == 0 and c == 0
        for kind in range(2):
            pair = []
            for high in range(2):
                at = slice(kind * 64 + high * 32, kind * 64 + high * 32 + 32)
                value = spec[at] * planes[high][0]
                if slot == 0:
                    value = value + mirror[at] * planes[high][1]
                power = spec[at] * value
                power = power[0:8] + power[8:16] + (power[16:24] + power[24:32])
                acc = power if acc is None else acc + power
                pair.append(value)
            dest = slice(kind * NZ + c * Z_CHUNK, kind * NZ + (c + 1) * Z_CHUNK)
            for parity, value in ((0, pair[0] + pair[1]), (1, pair[0] - pair[1])):
                hi, lo = split(value)
                sums[slot, parity, 0, dest, :] = hi
                sums[slot, parity, 1, dest, :] = lo
        acc = weight_ref[slot] * acc
        power_ref[...] = acc if first else power_ref[...] + acc

    def back_z(slot, parity):
        src = sums.at[slot, parity]
        grid = dot3(wzi_ref[parity, 0], wzi_ref[parity, 1], src[0], src[1])
        for sign in range(2):
            a, b = grid[:, 0:256], grid[:, 256:512]
            hi, lo = split(a + b if sign == 0 else a - b)
            for part, value in ((0, hi), (1, lo)):
                rows = slice(parity * 64, parity * 64 + 64)
                back[slot, sign, part, rows, 0:256] = value[0:64]
                back[slot, sign, part, rows, 256:512] = value[64:128]

    def back_x(slot, sign):
        src = back.at[slot, sign]
        value = dot3(src[0], src[1], wxi_ref[sign, 0], wxi_ref[sign, 1])
        for parity in range(2):
            for kind in range(2):
                put_rows(
                    out_ref,
                    parity * 64 * BACK_ROWS + HART + slot * 4 + kind * 2 + sign,
                    BACK_ROWS,
                    value[parity * 64 : parity * 64 + 64, kind * 128 : kind * 128 + 128],
                    count=64,
                )

    kinds = {
        "x": lambda slot, i: forward_x(slot, i == 1),
        "z": filtered,
        "b": back_z,
        "o": back_x,
    }
    return [
        (name, lambda name=name: kinds[name[0]](int(name[1]), int(name[2])))
        for name in HART_ORDER
    ]


def middle_kernel(
    first_ref, weight_ref, in_ref, other_ref, slope_ref, slope_z_ref, filt_hbm, wx_hbm, wz_hbm, wzi_hbm,
    wxi_hbm, out_ref, filt_ref, wx_ref, wz_ref, wzi_ref, wxi_ref, dens, gz, gy, gx, xp, sums, back,
    total_ref, power_ref, sems,
):
    moves = [(wx_hbm, wx_ref), (wz_hbm, wz_ref)]
    moves += [
        (filt_hbm.at[:, first_ref[0] + slot, :], filt_ref.at[slot]) for slot in range(2)
    ]
    moves += [(wzi_hbm, wzi_ref), (wxi_hbm, wxi_ref)]
    copies = [
        pltpu.make_async_copy(source, target, sems.at[i]) for i, (source, target) in enumerate(moves)
    ]
    for copy in copies:
        copy.start()
    xc = xc_steps(in_ref, slope_ref, slope_z_ref, out_ref, total_ref, dens, gz, gy, gx)
    hartree = hartree_steps(
        in_ref, filt_ref, other_ref, weight_ref, wx_ref, wz_ref, wzi_ref, wxi_ref, out_ref,
        power_ref, xp, sums, back,
    )
    for step in xc[:XC_AHEAD]:
        step()
    xc = xc[XC_AHEAD:]
    done = 0
    waits = {"x00": (0,), "z00": (1, 2), "z10": (3,), "b00": (4,), "o00": (5,)}
    for i, (name, step) in enumerate(hartree):
        for copy in waits.get(name, ()):
            copies[copy].wait()
        step()
        upto = min(len(xc), -(-(i + 1) * len(xc) // XC_SPREAD))
        for other in xc[done:upto]:
            other()
        done = max(done, upto)
    for other in xc[done:]:
        other()
    energies = jnp.where(
        iota((ND, 128), 1) < 64, jnp.sum(total_ref[...]), jnp.sum(power_ref[...])
    )
    put_rows(out_ref, BACK_ROWS - 1, BACK_ROWS, energies)


def homeward_kernel(in_ref, yb_ref, slope_ref, out_ref, energy_ref):
    field = jnp.concatenate(
        [get_rows(in_ref, HART + 2 * s, BACK_ROWS) for s in range(4)], axis=0
    )
    grid = dot3(yb_ref[0], yb_ref[1], *split(field))
    hi, lo = split(grid)
    parity = parity_matrix(True)
    hartree = dot1(hi, parity) + dot1(lo, parity)
    for spin in range(2):
        flux, rest = (
            jnp.concatenate(
                [get_rows(in_ref, base + spin * 4 + part * 2, BACK_ROWS) for part in range(2)],
                axis=0,
            )
            for base in (8, 0)
        )
        rows = slice(spin * NY, (spin + 1) * NY)
        out_ref[rows, :] = rest + hartree - dot3(slope_ref[0], slope_ref[1], *split(flux))
    row = jnp.sum(in_ref[pl.ds(BACK_ROWS - 1, ND, stride=BACK_ROWS), :], axis=0, keepdims=True)
    first = iota((1, 128), 1) < 64
    energy_ref[0] = jnp.sum(jnp.where(first, row, 0.0)) * (1.0 / (64.0 * CELLS))
    energy_ref[1] = jnp.sum(jnp.where(first, 0.0, row)) * (0.5 * NORM / (64.0 * CELLS))


def call(kernel, outs, in_specs, flops, scratch=(), smem_out=(), limit=40, flags=None):
    specs = [SMEM if i in smem_out else VMEM for i in range(len(outs))]
    return pl.pallas_call(
        kernel,
        out_shape=list(outs),
        in_specs=in_specs,
        out_specs=specs,
        scratch_shapes=list(scratch),
        cost_estimate=pl.CostEstimate(flops=flops, bytes_accessed=4 << 20, transcendentals=0),
        compiler_params=pltpu.CompilerParams(vmem_limit_bytes=limit << 20, flags=flags),
        name=kernel.__name__,
    )


def in_hbm(value):
    return pltpu.with_memory_space_constraint(value, pltpu.HBM)


def arr(*shape, dtype=F32):
    return jax.ShapeDtypeStruct(shape, dtype)


def exchange(value, rows, group):
    shaped = value.reshape(ND * rows // group, group, 128)
    out = lax.all_to_all(shaped, BLOCKS, split_axis=0, concat_axis=0, tiled=True)
    return out.reshape(ND * rows, 128)


def per_device(density, kernel_hat):
    q = lax.axis_index(GZ)
    (outward,) = call(
        outward_kernel,
        [arr(ND * OUT_ROWS, 128)],
        [HBM, HBM],
        400_000_000,
        scratch=[
            pltpu.VMEM((2 * NY, NX), F32),
            pltpu.VMEM((2, 4 * ND, NY), BF16),
            pltpu.SemaphoreType.DMA((2,)),
        ],
    )(in_hbm(density.reshape(2 * NY, NX)), in_hbm(jnp.asarray(y_forward())))
    outward, kernel_hat = lax.optimization_barrier((outward, in_hbm(kernel_hat)))
    kernel_hat = in_hbm(kernel_hat)
    arrived = exchange(outward, OUT_ROWS, 8)
    (plane,) = call(
        plane_kernel, [arr(MZ, MX)], [HBM], 1_000_000, scratch=[pltpu.SemaphoreType.DMA(())]
    )(kernel_hat)
    other = lax.ppermute(plane, GZ, [(0, PAIR)])
    shapes = [(2, 2, NX, MX), (2, 2 * MZ, 2 * NZ), (2, 2, NZ, 2 * NZ), (2, 2, MX, NX)]
    wx, wz, wzi, wxi, yb, slope, slope_z = call(
        tables_kernel,
        [arr(*shape, dtype=BF16) for shape in shapes]
        + [
            arr(2, NY, 4 * ND, dtype=BF16),
            arr(2, NY, NY, dtype=BF16),
            arr(2, NZ, 2 * NZ, dtype=BF16),
        ],
        [],
        2_000_000_000,
    )()
    start = jnp.where(q < ND // 2, 1, 0).astype(jnp.int32).reshape(1)
    weights = jnp.stack(
        [jnp.where(q == PAIR, 1.0, 2.0), jnp.full((), 2.0), jnp.where(q == PAIR, 0.5, 0.0)]
    ).astype(F32)
    field = pltpu.VMEM((2, 256, NX), F32)
    (back,) = call(
        middle_kernel,
        [arr(ND * BACK_ROWS, 128)],
        [SMEM, SMEM] + [VMEM] * 4 + [HBM] * 5,
        8_000_000_000,
        scratch=[pltpu.VMEM((2, MZ, MX), F32)]
        + [pltpu.VMEM(shape, BF16) for shape in shapes]
        + [field] * 4
        + [
            pltpu.VMEM((3, 2, 256, 512), BF16),
            pltpu.VMEM((2, 2, 2, 256, 512), BF16),
            pltpu.VMEM((2, 2, 2, 128, 512), BF16),
            pltpu.VMEM((8, NX), F32),
            pltpu.VMEM((8, MX), F32),
            pltpu.SemaphoreType.DMA((6,)),
        ],
    )(start, weights, arrived, other, slope, slope_z, kernel_hat, *map(in_hbm, (wx, wz, wzi, wxi)))
    returned = exchange(back, BACK_ROWS, 1)
    potential, energies = call(
        homeward_kernel,
        [arr(2 * NY, NX), arr(2)],
        [VMEM] * 3,
        1_000_000_000,
        smem_out=(1,),
    )(returned, yb, slope)
    return potential.reshape(2, 1, NY, NX), energies


def solution(mesh):
    torus = Mesh(mesh.devices.reshape(4, 4, 4, 2), GZ)
    placed = (P(None, GZ, None, None), P(None, GZ, None))
    return jax.shard_map(
        per_device,
        mesh=torus,
        in_specs=placed,
        out_specs=(P(None, GZ, None, None), P()),
        check_vma=False,
    )
```

```python
import math

import jax
import jax.numpy as jnp
import numpy as np
from jax import lax
from jax.experimental import pallas as pl
from jax.experimental.pallas import tpu as pltpu
from jax.sharding import Mesh
from jax.sharding import PartitionSpec as P

GZ = ("gz_0", "gz_1", "gz_2", "gz_3")
BLOCKS = ("gz_3", "gz_0", "gz_1", "gz_2")
HGRID = 0.35
STENCIL = (0.8, -0.2, 4.0 / 105.0, -1.0 / 280.0)
KAPPA = 0.804
MU_X = 0.2195149727645171
BETA_C = 0.06672455060314922
GAMMA_C = 0.031090690869654894
FZ_CURV = 1.709921
PARAMS_UNPOL = (0.031091, 0.2137, 7.5957, 3.5876, 1.6382, 0.49294)
PARAMS_POL = (0.015545, 0.20548, 14.1189, 6.1977, 3.3662, 0.62517)
PARAMS_STIFF = (0.016887, 0.11125, 10.357, 3.6231, 0.88026, 0.49671)

F32 = jnp.float32
BF16 = jnp.bfloat16
NZ, NY, NX = 128, 256, 256
MZ, MY, MX = 256, 512, 512
ND = 128
HART = 16
OUT_ROWS = 24
BACK_ROWS = 25
PAIR = ND // 2
CELLS = NZ * NY * NX
Z_CHUNK = 32
XC_ROWS = 8
XC_AHEAD = 12
XC_SPREAD = 19
HART_ORDER = (
    "x00", "x01", "x10", "z00", "z01", "z02", "z03", "z10",
    "b00", "z11", "b01", "z12", "o00", "z13", "o01", "b10",
    "b11", "o10", "o11",
)
NORM = 1.0 / (MX * MY * MZ)
VMEM = pl.BlockSpec(memory_space=pltpu.VMEM)
SMEM = pl.BlockSpec(memory_space=pltpu.SMEM)
HBM = pl.BlockSpec(memory_space=pltpu.HBM)


def halves(m):
    m = np.asarray(m, np.float32)
    hi = m.astype(BF16)
    lo = (m - hi.astype(np.float32)).astype(BF16)
    return np.stack([hi, lo])


def device_of(block):
    return (block & (ND // 2 - 1)) * 2 + (block >> 6)


def y_forward():
    y, q = np.arange(NY), device_of(np.arange(ND))
    first = np.where(q < ND // 2, 4 * q + 1, 4 * q)
    rows = []
    for ky in (first, first + 1):
        angle = 2.0 * np.pi * (np.outer(ky, y) % MY) / MY
        paired = (ky == MY // 2)[:, None]
        rows += [np.cos(angle), np.where(paired, 1.0, -np.sin(angle))]
    return halves(np.concatenate(rows, 0))


def split(value):
    hi = value.astype(BF16)
    lo = (value - hi.astype(F32)).astype(BF16)
    return hi, lo


def dot1(a, b):
    return jnp.dot(a, b, preferred_element_type=F32)


def dot3(a_hi, a_lo, b_hi, b_lo):
    return dot1(a_hi, b_hi) + (dot1(a_lo, b_hi) + dot1(a_hi, b_lo))


def put_rows(ref, row, rows, value, count=ND):
    for half in range(value.shape[1] // 128):
        ref[pl.ds(row + half, count, stride=rows), :] = value[
            :, half * 128 : half * 128 + 128
        ]


def put_back(ref, row, value):
    for core in range(2):
        put_rows(ref, core * BACK_ROWS + row, 2 * BACK_ROWS, value[core * 64 : core * 64 + 64], 64)


def get_back(ref, row):
    return jnp.concatenate(
        [
            jnp.concatenate(
                [
                    ref[pl.ds(core * BACK_ROWS + row + half, 64, stride=2 * BACK_ROWS), :]
                    for half in range(2)
                ],
                axis=1,
            )
            for core in range(2)
        ],
        axis=0,
    )


def get_rows(ref, row, rows):
    return jnp.concatenate(
        [ref[pl.ds(row + half, ND, stride=rows), :] for half in range(2)], axis=1
    )


def iota(shape, dim):
    return lax.broadcasted_iota(jnp.int32, shape, dim)


def slope_parts(n, place=lambda i: i):
    offset = place(iota((n, n), 1)) - place(iota((n, n), 0))
    parts = []
    coefs = halves([c / HGRID for c in STENCIL]).astype(np.float32)
    for part in range(2):
        value = jnp.zeros((n, n), F32)
        for k in range(1, 5):
            c = float(coefs[part, k - 1])
            value = jnp.where(offset == k, c, jnp.where(offset == -k, -c, value))
        parts.append(value.astype(BF16))
    return parts


def parity_matrix(transposed):
    x, place = iota((NX, NX), int(transposed)), iota((NX, NX), 1 - int(transposed))
    return jnp.where(place == (x & 1) * (NX // 2) + (x >> 1), 1.0, 0.0).astype(BF16)


def cos_sin(product):
    turn = product.astype(jnp.int32) & 511
    quarter = (turn + 64) >> 7
    angle = (turn - 128 * quarter).astype(F32) * (2.0 * math.pi / 512.0)
    sq = angle * angle
    s = angle * (
        1.0 + sq * (-1.0 / 6.0 + sq * (1.0 / 120.0 + sq * (-1.0 / 5040.0 + sq * (1.0 / 362880.0))))
    )
    c = 1.0 + sq * (-0.5 + sq * (1.0 / 24.0 + sq * (-1.0 / 720.0 + sq * (1.0 / 40320.0))))
    odd = (quarter & 1) == 1
    c, s = jnp.where(odd, s, c), jnp.where(odd, c, s)
    return (
        jnp.where(((quarter + 1) & 2) == 2, -c, c),
        jnp.where((quarter & 2) == 2, -s, s),
    )


def put_parts(ref, index, rows, cols, value):
    hi, lo = split(value)
    ref[(*index, 0, rows, cols)] = hi
    ref[(*index, 1, rows, cols)] = lo


def put_rotation(ref, index, row, c, s, transposed):
    n, m = c.shape
    top, low = slice(row, row + n), slice(row + n, row + 2 * n)
    put_parts(ref, index, top, slice(0, m), c)
    put_parts(ref, index, low, slice(m, 2 * m), c)
    put_parts(ref, index, top, slice(m, 2 * m), -s if transposed else s)
    put_parts(ref, index, low, slice(0, m), s if transposed else -s)


def float_iota(shape, dim):
    return iota(shape, dim).astype(F32)


def tables_kernel(wx_ref, wz_ref, wzi_ref, wxi_ref, yb_ref, slope_ref, slope_z_ref):
    for parity in range(2):
        shape = (NX // 2, MX // 2)
        x = 2.0 * float_iota(shape, 0) + parity
        put_rotation(wx_ref, (parity,), 0, *cos_sin(x * float_iota(shape, 1)), True)
        shape = (MX // 2, NX // 2)
        x = 2.0 * float_iota(shape, 1) + parity
        put_rotation(wxi_ref, (parity,), 0, *cos_sin(x * float_iota(shape, 0)), False)
        shape = (NZ // 2, NZ)
        z = 4.0 * float_iota(shape, 0) + 2.0 * parity
        put_rotation(wzi_ref, (parity,), 0, *cos_sin(z * float_iota(shape, 1)), True)
    for chunk in range(NZ // Z_CHUNK):
        shape = (2 * Z_CHUNK, NZ)
        row = iota(shape, 0)
        kz = chunk * Z_CHUNK + jnp.where(row < Z_CHUNK, row, row + NZ - Z_CHUNK)
        angle = 2.0 * kz.astype(F32) * device_of(iota(shape, 1)).astype(F32)
        put_rotation(wz_ref, (), chunk * 4 * Z_CHUNK, *cos_sin(angle), False)
    for slot in range(2):
        shape = (NY, ND)
        q = device_of(iota(shape, 1))
        ky = 4 * q + slot + jnp.where(q < ND // 2, 1, 0)
        c, s = cos_sin(ky.astype(F32) * float_iota(shape, 0))
        weight = jnp.where(ky == MY // 2, NORM, 2.0 * NORM)
        s = jnp.where(ky == MY // 2, -1.0, s)
        put_parts(yb_ref, (), slice(0, NY), slice(256 * slot, 256 * slot + 128), c * weight)
        put_parts(yb_ref, (), slice(0, NY), slice(256 * slot + 128, 256 * slot + 256), -s * weight)
    for part, value in enumerate(slope_parts(NY)):
        slope_ref[part] = value
    for part, value in enumerate(slope_parts(NZ, device_of)):
        slope_z_ref[part, :, 0:NZ] = value
        slope_z_ref[part, :, NZ : 2 * NZ] = value


def plane_kernel(filt_hbm, out_ref, sem):
    copy = pltpu.make_async_copy(filt_hbm.at[:, 0, :], out_ref, sem)
    copy.start()
    copy.wait()


def outward_kernel(dens_hbm, table_hbm, out_ref, dens_ref, table_ref, sems):
    dens_copy = pltpu.make_async_copy(dens_hbm, dens_ref, sems.at[0])
    table_copy = pltpu.make_async_copy(table_hbm, table_ref, sems.at[1])
    dens_copy.start()
    table_copy.start()
    slope = slope_parts(NY)
    parity = parity_matrix(False)
    dens_copy.wait()
    for spin in range(2):
        field = dens_ref[spin * NY : (spin + 1) * NY, :]
        grad = dot3(*slope, *split(field))
        for part in range(2):
            rows = slice(part * 128, part * 128 + 128)
            put_rows(out_ref, spin * 4 + part * 2, OUT_ROWS, field[rows])
            put_rows(out_ref, 8 + spin * 4 + part * 2, OUT_ROWS, grad[rows])
    hi, lo = split(dens_ref[0:NY, :] + dens_ref[NY : 2 * NY, :])
    hi, lo = dot1(hi, parity), dot1(lo, parity)
    hi, lo = hi.astype(BF16), lo.astype(BF16)
    table_copy.wait()
    for s in range(4):
        rows = slice(s * ND, (s + 1) * ND)
        value = dot3(table_ref[0, rows, :], table_ref[1, rows, :], hi, lo)
        put_rows(out_ref, HART + s * 2, OUT_ROWS, value)


LN2 = math.log(2.0)


def pw_piece(powers, params):
    root, radius, cube, square = powers
    scale = 2.0 * params[0]
    t1, t2 = (scale * params[2]) * root, (scale * params[3]) * radius
    t3, t4 = (scale * params[4]) * cube, (scale * params[5]) * square
    series = (t1 + t2) + (t3 + t4)
    slope = (series + t4) + 0.5 * (t3 - t1)
    more = series + 1.0
    inv = 1.0 / (series * more)
    logarithm = jnp.log(1.0 + inv * more)
    tilt = (-scale * params[1]) * radius
    front = tilt - scale
    return front * logarithm, tilt * logarithm - (front * slope) * inv


def exchange_piece(twice, inv_root, sigma):
    inv2 = inv_root * inv_root
    inv4 = inv2 * inv2
    root = twice * inv2
    front = -0.75 * (3.0 / math.pi) ** (1.0 / 3.0)
    unit = 1.0 / (3.0 * math.pi**2) ** (2.0 / 3.0)
    damp = 1.0 / (1.0 + (MU_X / KAPPA * unit) * sigma * (inv4 * inv4))
    gain = KAPPA - KAPPA * damp
    scaled = front * root
    energy = twice * scaled * (1.0 + gain)
    d_dens = scaled * (4.0 / 3.0 + gain * (4.0 / 3.0 - (8.0 / 3.0) * damp))
    d_sigma = (front * MU_X * unit) * (damp * damp) * inv4
    return energy, d_dens, d_sigma, root


def xc_point(up, down, sigma_uu, sigma_ud, sigma_dd):
    twice_up, twice_down = up + up, down + down
    inv_up = jnp.exp2(jnp.log(twice_up) * (-1.0 / (3.0 * LN2)))
    inv_down = jnp.exp2(jnp.log(twice_down) * (-1.0 / (3.0 * LN2)))
    e_up, d_up, d_uu, root_up = exchange_piece(twice_up, inv_up, sigma_uu)
    e_down, d_down, d_dd, root_down = exchange_piece(twice_down, inv_down, sigma_dd)
    dens = up + down
    sixth = jnp.exp2(jnp.log(dens) * (-1.0 / (6.0 * LN2)))
    inv_third = sixth * sixth
    inv_two = inv_third * inv_third
    third = dens * inv_two
    inv_dens = inv_two * inv_third
    plus = twice_up * inv_dens
    minus = twice_down * inv_dens
    zeta = 0.5 * (plus - minus)
    plus_cube = root_up * inv_third
    minus_cube = root_down * inv_third
    f_scale = 1.0 / (2.0 ** (4.0 / 3.0) - 2.0)
    f = (plus * plus_cube + minus * minus_cube) * f_scale - 2.0 * f_scale
    f_slope = (plus_cube - minus_cube) * (4.0 / 3.0 * f_scale)
    root = (3.0 / (4.0 * math.pi)) ** (1.0 / 6.0) * sixth
    radius = root * root
    powers = (root, radius, radius * root, radius * radius)
    e0, e0_d = pw_piece(powers, PARAMS_UNPOL)
    e1, e1_d = pw_piece(powers, PARAMS_POL)
    ac, ac_d = pw_piece(powers, PARAMS_STIFF)
    z2 = zeta * zeta
    z4 = z2 * z2
    one_z4 = z4 * (1.0 / FZ_CURV) - 1.0 / FZ_CURV
    f_z4 = f * z4
    f_one = f * one_z4
    diff = e1 - e0
    local = e0 + ac * f_one + diff * f_z4
    local_r = e0_d + ac_d * f_one + (e1_d - e0_d) * f_z4
    local_z = (ac * one_z4 + diff * z4) * f_slope + (ac * (1.0 / FZ_CURV) + diff) * (
        4.0 * f * z2 * zeta
    )
    phi2 = plus_cube * plus_cube + minus_cube * minus_cube
    inv_phi2 = 1.0 / phi2
    inv_sq = inv_phi2 * inv_phi2
    phi_log_slope = (third * (inv_up - inv_down)) * ((2.0 / 3.0) * inv_phi2)
    g3 = (GAMMA_C / 8.0) * (phi2 * phi2) * phi2
    grow = jnp.exp2(local * (inv_sq * inv_phi2) * (-8.0 / (GAMMA_C * LN2)))
    weight_a = (BETA_C / GAMMA_C) / (grow - 1.0)
    sigma = (sigma_uu + sigma_dd) + (sigma_ud + sigma_ud)
    ct = 4.0 * math.pi / (16.0 * (3.0 * math.pi**2) ** (1.0 / 3.0))
    kt = (ct * inv_third) * (inv_dens * inv_dens) * inv_sq
    t2 = sigma * kt
    w = weight_a * t2
    num = 1.0 + w
    den = num + w * w
    add = (BETA_C / GAMMA_C) * t2 * num
    both = den + add
    inv_both = 1.0 / (den * both)
    h = g3 * jnp.log(1.0 + add * (inv_both * both))
    h_t = ((BETA_C / GAMMA_C) * g3) * ((num + w) * inv_both)
    h_a = -((w * w) * w) * ((1.0 + num) * grow) * inv_both
    total = local + h
    ht_t2 = h_t * t2
    one_ha = 1.0 + h_a
    d_n = total - one_ha * ((1.0 / 3.0) * local_r) - (7.0 / 3.0) * ht_t2
    d_z = one_ha * local_z + phi_log_slope * (3.0 * (h - h_a * local) - (ht_t2 + ht_t2))
    d_sigma = 2.0 * (dens * h_t * kt)
    energy = 0.5 * (e_up + e_down) + dens * total
    return (
        energy,
        d_up + d_n + minus * d_z,
        d_down + d_n - plus * d_z,
        d_uu + d_sigma,
        d_sigma,
        d_dd + d_sigma,
    )


def slope_along_z(slope_z_ref, hi, lo):
    both = jnp.concatenate([hi, lo], axis=0)
    return dot1(slope_z_ref[0], both) + dot1(slope_z_ref[1], both)


def slope_along_x(slope_ref, hi, lo):
    return -dot3(hi, lo, slope_ref[0], slope_ref[1])


def xc_steps(in_ref, slope_ref, slope_z_ref, out_ref, total_ref, dens, gz, gy, gx):
    def gradients(part):
        rows = slice(part * 128, part * 128 + 128)
        for spin in range(2):
            field = get_rows(in_ref, spin * 4 + part * 2, OUT_ROWS)
            dens[spin, rows, :] = field
            gy[spin, rows, :] = get_rows(in_ref, 8 + spin * 4 + part * 2, OUT_ROWS)
            hi, lo = split(field)
            gz[spin, rows, :] = slope_along_z(slope_z_ref, hi, lo)
            gx[spin, rows, :] = slope_along_x(slope_ref, hi, lo)

    def points(i):
        rows = slice(i * XC_ROWS, (i + 1) * XC_ROWS)
        zu, zd = gz[0, rows, :], gz[1, rows, :]
        yu, yd = gy[0, rows, :], gy[1, rows, :]
        xu, xd = gx[0, rows, :], gx[1, rows, :]
        energy, d_up, d_down, d_uu, d_ud, d_dd = xc_point(
            dens[0, rows, :],
            dens[1, rows, :],
            zu * zu + yu * yu + xu * xu,
            zu * zd + yu * yd + xu * xd,
            zd * zd + yd * yd + xd * xd,
        )
        dens[0, rows, :] = d_up
        dens[1, rows, :] = d_down
        for ref, gu, gd in ((gz, zu, zd), (gy, yu, yd), (gx, xu, xd)):
            ref[0, rows, :] = d_uu * gu + d_ud * gd
            ref[1, rows, :] = d_dd * gd + d_ud * gu
        folded = sum(energy[r : r + 8] for r in range(0, XC_ROWS, 8))
        total_ref[...] = folded if i == 0 else total_ref[...] + folded

    def divergence(part):
        rows = slice(part * 128, part * 128 + 128)
        for spin in range(2):
            div = slope_along_z(slope_z_ref, *split(gz[spin, rows, :]))
            div = div + slope_along_x(slope_ref, *split(gx[spin, rows, :]))
            put_back(out_ref, spin * 4 + part * 2, dens[spin, rows, :] - div)
            put_back(out_ref, 8 + spin * 4 + part * 2, gy[spin, rows, :])

    steps = []
    for part in range(2):
        steps.append(lambda part=part: gradients(part))
        for i in range(part * 128 // XC_ROWS, (part + 1) * 128 // XC_ROWS):
            steps.append(lambda i=i: points(i))
        steps.append(lambda part=part: divergence(part))
    return steps


def hartree_steps(
    in_ref, filt_ref, other_ref, weight_ref, wx_ref, wz_ref, wzi_ref, wxi_ref, out_ref, power_ref,
    xp, sums, back,
):
    def forward_x(slot, conjugate):
        parts = []
        for parity in range(2):
            base = HART + 4 * slot + parity
            real = in_ref[pl.ds(base, ND, stride=OUT_ROWS), :]
            imag = in_ref[pl.ds(base + 2, ND, stride=OUT_ROWS), :]
            both = jnp.concatenate([real, -imag if conjugate else imag], axis=1)
            parts.append(dot3(*split(both), wx_ref[parity, 0], wx_ref[parity, 1]))
        place = 2 if conjugate else slot
        for half, value in ((0, parts[0] + parts[1]), (1, parts[0] - parts[1])):
            cols = slice(half * 256, half * 256 + 256)
            hi, lo = split(value)
            xp[place, 0, 0:128, cols] = hi[:, 0:256]
            xp[place, 0, 128:256, cols] = hi[:, 256:512]
            xp[place, 1, 0:128, cols] = lo[:, 0:256]
            xp[place, 1, 128:256, cols] = lo[:, 256:512]

    def filtered(slot, c):
        rows = slice(c * 128, c * 128 + 128)
        spec = dot3(wz_ref[0, rows, :], wz_ref[1, rows, :], xp[slot, 0], xp[slot, 1])
        if slot == 0:
            mirror = dot3(wz_ref[0, rows, :], wz_ref[1, rows, :], xp[2, 0], xp[2, 1])
        planes = []
        for high in range(2):
            place = slice(high * NZ + c * Z_CHUNK, high * NZ + (c + 1) * Z_CHUNK)
            own = filt_ref[slot, place, :]
            if slot == 0:
                swap = (own - other_ref[place, :]) * weight_ref[2]
                planes.append((own - swap, swap))
            else:
                planes.append((own, None))
        acc = None
        first = slot == 0 and c == 0
        for kind in range(2):
            pair = []
            for high in range(2):
                at = slice(kind * 64 + high * 32, kind * 64 + high * 32 + 32)
                value = spec[at] * planes[high][0]
                if slot == 0:
                    value = value + mirror[at] * planes[high][1]
                power = spec[at] * value
                power = power[0:8] + power[8:16] + (power[16:24] + power[24:32])
                acc = power if acc is None else acc + power
                pair.append(value)
            dest = slice(kind * NZ + c * Z_CHUNK, kind * NZ + (c + 1) * Z_CHUNK)
            for parity, value in ((0, pair[0] + pair[1]), (1, pair[0] - pair[1])):
                hi, lo = split(value)
                sums[slot, parity, 0, dest, :] = hi
                sums[slot, parity, 1, dest, :] = lo
        acc = weight_ref[slot] * acc
        power_ref[...] = acc if first else power_ref[...] + acc

    def back_z(slot, parity):
        src = sums.at[slot, parity]
        grid = dot3(wzi_ref[parity, 0], wzi_ref[parity, 1], src[0], src[1])
        for sign in range(2):
            a, b = grid[:, 0:256], grid[:, 256:512]
            hi, lo = split(a + b if sign == 0 else a - b)
            for part, value in ((0, hi), (1, lo)):
                rows = slice(parity * 64, parity * 64 + 64)
                back[slot, sign, part, rows, 0:256] = value[0:64]
                back[slot, sign, part, rows, 256:512] = value[64:128]

    def back_x(slot, sign):
        src = back.at[slot, sign]
        value = dot3(src[0], src[1], wxi_ref[sign, 0], wxi_ref[sign, 1])
        for parity in range(2):
            for kind in range(2):
                put_rows(
                    out_ref,
                    parity * BACK_ROWS + HART + slot * 4 + kind * 2 + sign,
                    2 * BACK_ROWS,
                    value[parity * 64 : parity * 64 + 64, kind * 128 : kind * 128 + 128],
                    count=64,
                )

    kinds = {
        "x": lambda slot, i: forward_x(slot, i == 1),
        "z": filtered,
        "b": back_z,
        "o": back_x,
    }
    return [
        (name, lambda name=name: kinds[name[0]](int(name[1]), int(name[2])))
        for name in HART_ORDER
    ]


def middle_kernel(
    first_ref, weight_ref, in_ref, other_ref, slope_ref, slope_z_ref, filt_hbm, wx_hbm, wz_hbm, wzi_hbm,
    wxi_hbm, out_ref, filt_ref, wx_ref, wz_ref, wzi_ref, wxi_ref, dens, gz, gy, gx, xp, sums, back,
    total_ref, power_ref, sems,
):
    moves = [(wx_hbm, wx_ref), (wz_hbm, wz_ref)]
    moves += [
        (filt_hbm.at[:, first_ref[0] + slot, :], filt_ref.at[slot]) for slot in range(2)
    ]
    moves += [(wzi_hbm, wzi_ref), (wxi_hbm, wxi_ref)]
    copies = [
        pltpu.make_async_copy(source, target, sems.at[i]) for i, (source, target) in enumerate(moves)
    ]
    for copy in copies:
        copy.start()
    xc = xc_steps(in_ref, slope_ref, slope_z_ref, out_ref, total_ref, dens, gz, gy, gx)
    hartree = hartree_steps(
        in_ref, filt_ref, other_ref, weight_ref, wx_ref, wz_ref, wzi_ref, wxi_ref, out_ref,
        power_ref, xp, sums, back,
    )
    for step in xc[:XC_AHEAD]:
        step()
    xc = xc[XC_AHEAD:]
    done = 0
    waits = {"x00": (0,), "z00": (1, 2), "z10": (3,), "b00": (4,), "o00": (5,)}
    for i, (name, step) in enumerate(hartree):
        for copy in waits.get(name, ()):
            copies[copy].wait()
        step()
        upto = min(len(xc), -(-(i + 1) * len(xc) // XC_SPREAD))
        for other in xc[done:upto]:
            other()
        done = max(done, upto)
    for other in xc[done:]:
        other()
    energies = jnp.where(
        iota((ND, 128), 1) < 64, jnp.sum(total_ref[...]), jnp.sum(power_ref[...])
    )
    put_rows(out_ref, BACK_ROWS - 1, BACK_ROWS, energies)


def homeward_kernel(in_ref, yb_ref, slope_ref, out_ref, energy_ref):
    field = jnp.concatenate(
        [get_back(in_ref, HART + 2 * s) for s in range(4)], axis=0
    )
    grid = dot3(yb_ref[0], yb_ref[1], *split(field))
    hi, lo = split(grid)
    parity = parity_matrix(True)
    hartree = dot1(hi, parity) + dot1(lo, parity)
    for spin in range(2):
        flux, rest = (
            jnp.concatenate(
                [get_back(in_ref, base + spin * 4 + part * 2) for part in range(2)],
                axis=0,
            )
            for base in (8, 0)
        )
        rows = slice(spin * NY, (spin + 1) * NY)
        out_ref[rows, :] = rest + hartree - dot3(slope_ref[0], slope_ref[1], *split(flux))
    row = jnp.sum(in_ref[pl.ds(BACK_ROWS - 1, ND, stride=BACK_ROWS), :], axis=0, keepdims=True)
    first = iota((1, 128), 1) < 64
    energy_ref[0] = jnp.sum(jnp.where(first, row, 0.0)) * (1.0 / (64.0 * CELLS))
    energy_ref[1] = jnp.sum(jnp.where(first, 0.0, row)) * (0.5 * NORM / (64.0 * CELLS))


def call(kernel, outs, in_specs, flops, scratch=(), smem_out=(), limit=40, flags=None):
    specs = [SMEM if i in smem_out else VMEM for i in range(len(outs))]
    return pl.pallas_call(
        kernel,
        out_shape=list(outs),
        in_specs=in_specs,
        out_specs=specs,
        scratch_shapes=list(scratch),
        cost_estimate=pl.CostEstimate(flops=flops, bytes_accessed=4 << 20, transcendentals=0),
        compiler_params=pltpu.CompilerParams(vmem_limit_bytes=limit << 20, flags=flags),
        name=kernel.__name__,
    )


def in_hbm(value):
    return pltpu.with_memory_space_constraint(value, pltpu.HBM)


def arr(*shape, dtype=F32):
    return jax.ShapeDtypeStruct(shape, dtype)


def exchange(value, rows, group, order):
    shaped = value.reshape(ND * rows // group, group, 128)
    out = lax.all_to_all(shaped, order, split_axis=0, concat_axis=0, tiled=True)
    return out.reshape(ND * rows, 128)


def per_device(density, kernel_hat):
    q = lax.axis_index(GZ)
    (outward,) = call(
        outward_kernel,
        [arr(ND * OUT_ROWS, 128)],
        [HBM, HBM],
        400_000_000,
        scratch=[
            pltpu.VMEM((2 * NY, NX), F32),
            pltpu.VMEM((2, 4 * ND, NY), BF16),
            pltpu.SemaphoreType.DMA((2,)),
        ],
    )(in_hbm(density.reshape(2 * NY, NX)), in_hbm(jnp.asarray(y_forward())))
    outward, kernel_hat = lax.optimization_barrier((outward, in_hbm(kernel_hat)))
    kernel_hat = in_hbm(kernel_hat)
    arrived = exchange(outward, OUT_ROWS, 8, BLOCKS)
    (plane,) = call(
        plane_kernel, [arr(MZ, MX)], [HBM], 1_000_000, scratch=[pltpu.SemaphoreType.DMA(())]
    )(kernel_hat)
    other = lax.ppermute(plane, GZ, [(0, PAIR)])
    shapes = [(2, 2, NX, MX), (2, 2 * MZ, 2 * NZ), (2, 2, NZ, 2 * NZ), (2, 2, MX, NX)]
    wx, wz, wzi, wxi, yb, slope, slope_z = call(
        tables_kernel,
        [arr(*shape, dtype=BF16) for shape in shapes]
        + [
            arr(2, NY, 4 * ND, dtype=BF16),
            arr(2, NY, NY, dtype=BF16),
            arr(2, NZ, 2 * NZ, dtype=BF16),
        ],
        [],
        2_000_000_000,
    )()
    start = jnp.where(q < ND // 2, 1, 0).astype(jnp.int32).reshape(1)
    weights = jnp.stack(
        [jnp.where(q == PAIR, 1.0, 2.0), jnp.full((), 2.0), jnp.where(q == PAIR, 0.5, 0.0)]
    ).astype(F32)
    field = pltpu.VMEM((2, 256, NX), F32)
    (back,) = call(
        middle_kernel,
        [arr(ND * BACK_ROWS, 128)],
        [SMEM, SMEM] + [VMEM] * 4 + [HBM] * 5,
        8_000_000_000,
        scratch=[pltpu.VMEM((2, MZ, MX), F32)]
        + [pltpu.VMEM(shape, BF16) for shape in shapes]
        + [field] * 4
        + [
            pltpu.VMEM((3, 2, 256, 512), BF16),
            pltpu.VMEM((2, 2, 2, 256, 512), BF16),
            pltpu.VMEM((2, 2, 2, 128, 512), BF16),
            pltpu.VMEM((8, NX), F32),
            pltpu.VMEM((8, MX), F32),
            pltpu.SemaphoreType.DMA((6,)),
        ],
    )(start, weights, arrived, other, slope, slope_z, kernel_hat, *map(in_hbm, (wx, wz, wzi, wxi)))
    returned = exchange(back, BACK_ROWS, 1, GZ)
    potential, energies = call(
        homeward_kernel,
        [arr(2 * NY, NX), arr(2)],
        [VMEM] * 3,
        1_000_000_000,
        smem_out=(1,),
    )(returned, yb, slope)
    return potential.reshape(2, 1, NY, NX), energies


def solution(mesh):
    torus = Mesh(mesh.devices.reshape(4, 4, 4, 2), GZ)
    placed = (P(None, GZ, None, None), P(None, GZ, None))
    return jax.shard_map(
        per_device,
        mesh=torus,
        in_specs=placed,
        out_specs=(P(None, GZ, None, None), P()),
        check_vma=False,
    )
```

```python
import math

import jax
import jax.numpy as jnp
import numpy as np
from jax import lax
from jax.experimental import pallas as pl
from jax.experimental.pallas import tpu as pltpu
from jax.sharding import Mesh
from jax.sharding import PartitionSpec as P


GZ = ("gz_0", "gz_1", "gz_2", "gz_3")
BLOCKS = ("gz_3", "gz_0", "gz_1", "gz_2")
HGRID = 0.35
STENCIL = (0.8, -0.2, 4.0 / 105.0, -1.0 / 280.0)
KAPPA = 0.804
MU_X = 0.2195149727645171
BETA_C = 0.06672455060314922
GAMMA_C = 0.031090690869654894
FZ_CURV = 1.709921
PARAMS_UNPOL = (0.031091, 0.2137, 7.5957, 3.5876, 1.6382, 0.49294)
PARAMS_POL = (0.015545, 0.20548, 14.1189, 6.1977, 3.3662, 0.62517)
PARAMS_STIFF = (0.016887, 0.11125, 10.357, 3.6231, 0.88026, 0.49671)

F32 = jnp.float32
BF16 = jnp.bfloat16
NZ, NY, NX = 128, 256, 256
MZ, MY, MX = 256, 512, 512
ND = 128
HART = 16
OUT_ROWS = 24
BACK_ROWS = 25
PAIR = ND // 2
CELLS = NZ * NY * NX
Z_CHUNK = 32
XC_ROWS = 8
XC_AHEAD = 12
XC_SPREAD = 19
HART_ORDER = (
    "x00", "x01", "x10", "z00", "z01", "z02", "z03", "z10",
    "b00", "z11", "b01", "z12", "o00", "z13", "o01", "b10",
    "b11", "o10", "o11",
)
NORM = 1.0 / (MX * MY * MZ)
VMEM = pl.BlockSpec(memory_space=pltpu.VMEM)
SMEM = pl.BlockSpec(memory_space=pltpu.SMEM)
HBM = pl.BlockSpec(memory_space=pltpu.HBM)


def halves(m):
    m = np.asarray(m, np.float32)
    hi = m.astype(BF16)
    lo = (m - hi.astype(np.float32)).astype(BF16)
    return np.stack([hi, lo])


def device_of(block):
    return (block & (ND // 2 - 1)) * 2 + (block >> 6)


def y_forward():
    y, q = np.arange(NY), device_of(np.arange(ND))
    first = np.where(q < ND // 2, 4 * q + 1, 4 * q)
    rows = []
    for ky in (first, first + 1):
        angle = 2.0 * np.pi * (np.outer(ky, y) % MY) / MY
        paired = (ky == MY // 2)[:, None]
        rows += [np.cos(angle), np.where(paired, 1.0, -np.sin(angle))]
    return halves(np.concatenate(rows, 0))


def split(value):
    hi = value.astype(BF16)
    lo = (value - hi.astype(F32)).astype(BF16)
    return hi, lo


def dot1(a, b):
    return jnp.dot(a, b, preferred_element_type=F32)


def dot3(a_hi, a_lo, b_hi, b_lo):
    return dot1(a_hi, b_hi) + (dot1(a_lo, b_hi) + dot1(a_hi, b_lo))


def put_rows(ref, row, rows, value, count=ND):
    for half in range(value.shape[1] // 128):
        ref[pl.ds(row + half, count, stride=rows), :] = value[
            :, half * 128 : half * 128 + 128
        ]


def get_rows(ref, row, rows):
    return jnp.concatenate(
        [ref[pl.ds(row + half, ND, stride=rows), :] for half in range(2)], axis=1
    )


def iota(shape, dim):
    return lax.broadcasted_iota(jnp.int32, shape, dim)


def slope_parts(n, place=lambda i: i):
    offset = place(iota((n, n), 1)) - place(iota((n, n), 0))
    parts = []
    coefs = halves([c / HGRID for c in STENCIL]).astype(np.float32)
    for part in range(2):
        value = jnp.zeros((n, n), F32)
        for k in range(1, 5):
            c = float(coefs[part, k - 1])
            value = jnp.where(offset == k, c, jnp.where(offset == -k, -c, value))
        parts.append(value.astype(BF16))
    return parts


def parity_matrix(transposed):
    x, place = iota((NX, NX), int(transposed)), iota((NX, NX), 1 - int(transposed))
    return jnp.where(place == (x & 1) * (NX // 2) + (x >> 1), 1.0, 0.0).astype(BF16)


def cos_sin(product):
    turn = product.astype(jnp.int32) & 511
    quarter = (turn + 64) >> 7
    angle = (turn - 128 * quarter).astype(F32) * (2.0 * math.pi / 512.0)
    sq = angle * angle
    s = angle * (
        1.0 + sq * (-1.0 / 6.0 + sq * (1.0 / 120.0 + sq * (-1.0 / 5040.0 + sq * (1.0 / 362880.0))))
    )
    c = 1.0 + sq * (-0.5 + sq * (1.0 / 24.0 + sq * (-1.0 / 720.0 + sq * (1.0 / 40320.0))))
    odd = (quarter & 1) == 1
    c, s = jnp.where(odd, s, c), jnp.where(odd, c, s)
    return (
        jnp.where(((quarter + 1) & 2) == 2, -c, c),
        jnp.where((quarter & 2) == 2, -s, s),
    )


def put_parts(ref, index, rows, cols, value):
    hi, lo = split(value)
    ref[(*index, 0, rows, cols)] = hi
    ref[(*index, 1, rows, cols)] = lo


def put_rotation(ref, index, row, c, s, transposed):
    n, m = c.shape
    top, low = slice(row, row + n), slice(row + n, row + 2 * n)
    put_parts(ref, index, top, slice(0, m), c)
    put_parts(ref, index, low, slice(m, 2 * m), c)
    put_parts(ref, index, top, slice(m, 2 * m), -s if transposed else s)
    put_parts(ref, index, low, slice(0, m), s if transposed else -s)


def float_iota(shape, dim):
    return iota(shape, dim).astype(F32)


def tables_kernel(wx_ref, wz_ref, wzi_ref, wxi_ref, yb_ref, slope_ref, slope_z_ref):
    for parity in range(2):
        shape = (NX // 2, MX // 2)
        x = 2.0 * float_iota(shape, 0) + parity
        put_rotation(wx_ref, (parity,), 0, *cos_sin(x * float_iota(shape, 1)), True)
        shape = (MX // 2, NX // 2)
        x = 2.0 * float_iota(shape, 1) + parity
        put_rotation(wxi_ref, (parity,), 0, *cos_sin(x * float_iota(shape, 0)), False)
        shape = (NZ // 2, NZ)
        z = 4.0 * float_iota(shape, 0) + 2.0 * parity
        put_rotation(wzi_ref, (parity,), 0, *cos_sin(z * float_iota(shape, 1)), True)
    for chunk in range(NZ // Z_CHUNK):
        shape = (2 * Z_CHUNK, NZ)
        row = iota(shape, 0)
        kz = chunk * Z_CHUNK + jnp.where(row < Z_CHUNK, row, row + NZ - Z_CHUNK)
        angle = 2.0 * kz.astype(F32) * device_of(iota(shape, 1)).astype(F32)
        put_rotation(wz_ref, (), chunk * 4 * Z_CHUNK, *cos_sin(angle), False)
    for slot in range(2):
        shape = (NY, ND)
        q = device_of(iota(shape, 1))
        ky = 4 * q + slot + jnp.where(q < ND // 2, 1, 0)
        c, s = cos_sin(ky.astype(F32) * float_iota(shape, 0))
        weight = jnp.where(ky == MY // 2, NORM, 2.0 * NORM)
        s = jnp.where(ky == MY // 2, -1.0, s)
        put_parts(yb_ref, (), slice(0, NY), slice(256 * slot, 256 * slot + 128), c * weight)
        put_parts(yb_ref, (), slice(0, NY), slice(256 * slot + 128, 256 * slot + 256), -s * weight)
    for part, value in enumerate(slope_parts(NY)):
        slope_ref[part] = value
    for part, value in enumerate(slope_parts(NZ, device_of)):
        slope_z_ref[part, :, 0:NZ] = value
        slope_z_ref[part, :, NZ : 2 * NZ] = value


def outward_kernel(dens_hbm, table_hbm, filt_hbm, out_ref, plane_ref, dens_ref, table_ref, sems):
    dens_copy = pltpu.make_async_copy(dens_hbm, dens_ref, sems.at[0])
    table_copy = pltpu.make_async_copy(table_hbm, table_ref, sems.at[1])
    plane_copy = pltpu.make_async_copy(filt_hbm.at[:, 0, :], plane_ref, sems.at[2])
    dens_copy.start()
    table_copy.start()
    plane_copy.start()
    slope = slope_parts(NY)
    parity = parity_matrix(False)
    dens_copy.wait()
    for spin in range(2):
        field = dens_ref[spin * NY : (spin + 1) * NY, :]
        grad = dot3(*slope, *split(field))
        for part in range(2):
            rows = slice(part * 128, part * 128 + 128)
            put_rows(out_ref, spin * 4 + part * 2, OUT_ROWS, field[rows])
            put_rows(out_ref, 8 + spin * 4 + part * 2, OUT_ROWS, grad[rows])
    hi, lo = split(dens_ref[0:NY, :] + dens_ref[NY : 2 * NY, :])
    hi, lo = dot1(hi, parity), dot1(lo, parity)
    hi, lo = hi.astype(BF16), lo.astype(BF16)
    table_copy.wait()
    for s in range(4):
        rows = slice(s * ND, (s + 1) * ND)
        value = dot3(table_ref[0, rows, :], table_ref[1, rows, :], hi, lo)
        put_rows(out_ref, HART + s * 2, OUT_ROWS, value)
    plane_copy.wait()


LN2 = math.log(2.0)


def pw_piece(powers, params):
    root, radius, cube, square = powers
    scale = 2.0 * params[0]
    t1, t2 = (scale * params[2]) * root, (scale * params[3]) * radius
    t3, t4 = (scale * params[4]) * cube, (scale * params[5]) * square
    series = (t1 + t2) + (t3 + t4)
    slope = (series + t4) + 0.5 * (t3 - t1)
    more = series + 1.0
    inv = 1.0 / (series * more)
    logarithm = jnp.log(1.0 + inv * more)
    tilt = (-scale * params[1]) * radius
    front = tilt - scale
    return front * logarithm, tilt * logarithm - (front * slope) * inv


def exchange_piece(twice, inv_root, sigma):
    inv2 = inv_root * inv_root
    inv4 = inv2 * inv2
    root = twice * inv2
    front = -0.75 * (3.0 / math.pi) ** (1.0 / 3.0)
    unit = 1.0 / (3.0 * math.pi**2) ** (2.0 / 3.0)
    damp = 1.0 / (1.0 + (MU_X / KAPPA * unit) * sigma * (inv4 * inv4))
    gain = KAPPA - KAPPA * damp
    scaled = front * root
    energy = twice * scaled * (1.0 + gain)
    d_dens = scaled * (4.0 / 3.0 + gain * (4.0 / 3.0 - (8.0 / 3.0) * damp))
    d_sigma = (front * MU_X * unit) * (damp * damp) * inv4
    return energy, d_dens, d_sigma, root


def xc_point(up, down, sigma_uu, sigma_ud, sigma_dd):
    twice_up, twice_down = up + up, down + down
    inv_up = jnp.exp2(jnp.log(twice_up) * (-1.0 / (3.0 * LN2)))
    inv_down = jnp.exp2(jnp.log(twice_down) * (-1.0 / (3.0 * LN2)))
    e_up, d_up, d_uu, root_up = exchange_piece(twice_up, inv_up, sigma_uu)
    e_down, d_down, d_dd, root_down = exchange_piece(twice_down, inv_down, sigma_dd)
    dens = up + down
    sixth = jnp.exp2(jnp.log(dens) * (-1.0 / (6.0 * LN2)))
    inv_third = sixth * sixth
    inv_two = inv_third * inv_third
    third = dens * inv_two
    inv_dens = inv_two * inv_third
    plus = twice_up * inv_dens
    minus = twice_down * inv_dens
    zeta = 0.5 * (plus - minus)
    plus_cube = root_up * inv_third
    minus_cube = root_down * inv_third
    f_scale = 1.0 / (2.0 ** (4.0 / 3.0) - 2.0)
    f = (plus * plus_cube + minus * minus_cube) * f_scale - 2.0 * f_scale
    f_slope = (plus_cube - minus_cube) * (4.0 / 3.0 * f_scale)
    root = (3.0 / (4.0 * math.pi)) ** (1.0 / 6.0) * sixth
    radius = root * root
    powers = (root, radius, radius * root, radius * radius)
    e0, e0_d = pw_piece(powers, PARAMS_UNPOL)
    e1, e1_d = pw_piece(powers, PARAMS_POL)
    ac, ac_d = pw_piece(powers, PARAMS_STIFF)
    z2 = zeta * zeta
    z4 = z2 * z2
    one_z4 = z4 * (1.0 / FZ_CURV) - 1.0 / FZ_CURV
    f_z4 = f * z4
    f_one = f * one_z4
    diff = e1 - e0
    local = e0 + ac * f_one + diff * f_z4
    local_r = e0_d + ac_d * f_one + (e1_d - e0_d) * f_z4
    local_z = (ac * one_z4 + diff * z4) * f_slope + (ac * (1.0 / FZ_CURV) + diff) * (
        4.0 * f * z2 * zeta
    )
    phi2 = plus_cube * plus_cube + minus_cube * minus_cube
    inv_phi2 = 1.0 / phi2
    inv_sq = inv_phi2 * inv_phi2
    phi_log_slope = (third * (inv_up - inv_down)) * ((2.0 / 3.0) * inv_phi2)
    g3 = (GAMMA_C / 8.0) * (phi2 * phi2) * phi2
    grow = jnp.exp2(local * (inv_sq * inv_phi2) * (-8.0 / (GAMMA_C * LN2)))
    weight_a = (BETA_C / GAMMA_C) / (grow - 1.0)
    sigma = (sigma_uu + sigma_dd) + (sigma_ud + sigma_ud)
    ct = 4.0 * math.pi / (16.0 * (3.0 * math.pi**2) ** (1.0 / 3.0))
    kt = (ct * inv_third) * (inv_dens * inv_dens) * inv_sq
    t2 = sigma * kt
    w = weight_a * t2
    num = 1.0 + w
    den = num + w * w
    add = (BETA_C / GAMMA_C) * t2 * num
    both = den + add
    inv_both = 1.0 / (den * both)
    h = g3 * jnp.log(1.0 + add * (inv_both * both))
    h_t = ((BETA_C / GAMMA_C) * g3) * ((num + w) * inv_both)
    h_a = -((w * w) * w) * ((1.0 + num) * grow) * inv_both
    total = local + h
    ht_t2 = h_t * t2
    one_ha = 1.0 + h_a
    d_n = total - one_ha * ((1.0 / 3.0) * local_r) - (7.0 / 3.0) * ht_t2
    d_z = one_ha * local_z + phi_log_slope * (3.0 * (h - h_a * local) - (ht_t2 + ht_t2))
    d_sigma = 2.0 * (dens * h_t * kt)
    energy = 0.5 * (e_up + e_down) + dens * total
    return (
        energy,
        d_up + d_n + minus * d_z,
        d_down + d_n - plus * d_z,
        d_uu + d_sigma,
        d_sigma,
        d_dd + d_sigma,
    )


def slope_along_z(slope_z_ref, hi, lo):
    both = jnp.concatenate([hi, lo], axis=0)
    return dot1(slope_z_ref[0], both) + dot1(slope_z_ref[1], both)


def slope_along_x(slope_ref, hi, lo):
    return -dot3(hi, lo, slope_ref[0], slope_ref[1])


def xc_steps(in_ref, slope_ref, slope_z_ref, out_ref, total_ref, dens, gz, gy, gx):
    def gradients(part):
        rows = slice(part * 128, part * 128 + 128)
        for spin in range(2):
            field = get_rows(in_ref, spin * 4 + part * 2, OUT_ROWS)
            dens[spin, rows, :] = field
            gy[spin, rows, :] = get_rows(in_ref, 8 + spin * 4 + part * 2, OUT_ROWS)
            hi, lo = split(field)
            gz[spin, rows, :] = slope_along_z(slope_z_ref, hi, lo)
            gx[spin, rows, :] = slope_along_x(slope_ref, hi, lo)

    def points(i):
        rows = slice(i * XC_ROWS, (i + 1) * XC_ROWS)
        zu, zd = gz[0, rows, :], gz[1, rows, :]
        yu, yd = gy[0, rows, :], gy[1, rows, :]
        xu, xd = gx[0, rows, :], gx[1, rows, :]
        energy, d_up, d_down, d_uu, d_ud, d_dd = xc_point(
            dens[0, rows, :],
            dens[1, rows, :],
            zu * zu + yu * yu + xu * xu,
            zu * zd + yu * yd + xu * xd,
            zd * zd + yd * yd + xd * xd,
        )
        dens[0, rows, :] = d_up
        dens[1, rows, :] = d_down
        for ref, gu, gd in ((gz, zu, zd), (gy, yu, yd), (gx, xu, xd)):
            ref[0, rows, :] = d_uu * gu + d_ud * gd
            ref[1, rows, :] = d_dd * gd + d_ud * gu
        folded = sum(energy[r : r + 8] for r in range(0, XC_ROWS, 8))
        total_ref[...] = folded if i == 0 else total_ref[...] + folded

    def divergence(part):
        rows = slice(part * 128, part * 128 + 128)
        for spin in range(2):
            div = slope_along_z(slope_z_ref, *split(gz[spin, rows, :]))
            div = div + slope_along_x(slope_ref, *split(gx[spin, rows, :]))
            put_rows(out_ref, spin * 4 + part * 2, BACK_ROWS, dens[spin, rows, :] - div)
            put_rows(out_ref, 8 + spin * 4 + part * 2, BACK_ROWS, gy[spin, rows, :])

    steps = []
    for part in range(2):
        steps.append(lambda part=part: gradients(part))
        for i in range(part * 128 // XC_ROWS, (part + 1) * 128 // XC_ROWS):
            steps.append(lambda i=i: points(i))
        steps.append(lambda part=part: divergence(part))
    return steps


def hartree_steps(
    in_ref, filt_ref, other_ref, weight_ref, wx_ref, wz_ref, wzi_ref, wxi_ref, out_ref, power_ref,
    xp, sums, back,
):
    def forward_x(slot, conjugate):
        parts = []
        for parity in range(2):
            base = HART + 4 * slot + parity
            real = in_ref[pl.ds(base, ND, stride=OUT_ROWS), :]
            imag = in_ref[pl.ds(base + 2, ND, stride=OUT_ROWS), :]
            both = jnp.concatenate([real, -imag if conjugate else imag], axis=1)
            parts.append(dot3(*split(both), wx_ref[parity, 0], wx_ref[parity, 1]))
        place = 2 if conjugate else slot
        for half, value in ((0, parts[0] + parts[1]), (1, parts[0] - parts[1])):
            cols = slice(half * 256, half * 256 + 256)
            hi, lo = split(value)
            xp[place, 0, 0:128, cols] = hi[:, 0:256]
            xp[place, 0, 128:256, cols] = hi[:, 256:512]
            xp[place, 1, 0:128, cols] = lo[:, 0:256]
            xp[place, 1, 128:256, cols] = lo[:, 256:512]

    def filtered(slot, c):
        rows = slice(c * 128, c * 128 + 128)
        spec = dot3(wz_ref[0, rows, :], wz_ref[1, rows, :], xp[slot, 0], xp[slot, 1])
        if slot == 0:
            mirror = dot3(wz_ref[0, rows, :], wz_ref[1, rows, :], xp[2, 0], xp[2, 1])
        planes = []
        for high in range(2):
            place = slice(high * NZ + c * Z_CHUNK, high * NZ + (c + 1) * Z_CHUNK)
            own = filt_ref[slot, place, :]
            if slot == 0:
                swap = (own - other_ref[place, :]) * weight_ref[2]
                planes.append((own - swap, swap))
            else:
                planes.append((own, None))
        acc = None
        first = slot == 0 and c == 0
        for kind in range(2):
            pair = []
            for high in range(2):
                at = slice(kind * 64 + high * 32, kind * 64 + high * 32 + 32)
                value = spec[at] * planes[high][0]
                if slot == 0:
                    value = value + mirror[at] * planes[high][1]
                power = spec[at] * value
                power = power[0:8] + power[8:16] + (power[16:24] + power[24:32])
                acc = power if acc is None else acc + power
                pair.append(value)
            dest = slice(kind * NZ + c * Z_CHUNK, kind * NZ + (c + 1) * Z_CHUNK)
            for parity, value in ((0, pair[0] + pair[1]), (1, pair[0] - pair[1])):
                hi, lo = split(value)
                sums[slot, parity, 0, dest, :] = hi
                sums[slot, parity, 1, dest, :] = lo
        acc = weight_ref[slot] * acc
        power_ref[...] = acc if first else power_ref[...] + acc

    def back_z(slot, parity):
        src = sums.at[slot, parity]
        grid = dot3(wzi_ref[parity, 0], wzi_ref[parity, 1], src[0], src[1])
        for sign in range(2):
            a, b = grid[:, 0:256], grid[:, 256:512]
            hi, lo = split(a + b if sign == 0 else a - b)
            for part, value in ((0, hi), (1, lo)):
                rows = slice(parity * 64, parity * 64 + 64)
                back[slot, sign, part, rows, 0:256] = value[0:64]
                back[slot, sign, part, rows, 256:512] = value[64:128]

    def back_x(slot, sign):
        src = back.at[slot, sign]
        value = dot3(src[0], src[1], wxi_ref[sign, 0], wxi_ref[sign, 1])
        for parity in range(2):
            for kind in range(2):
                put_rows(
                    out_ref,
                    parity * 64 * BACK_ROWS + HART + slot * 4 + kind * 2 + sign,
                    BACK_ROWS,
                    value[parity * 64 : parity * 64 + 64, kind * 128 : kind * 128 + 128],
                    count=64,
                )

    kinds = {
        "x": lambda slot, i: forward_x(slot, i == 1),
        "z": filtered,
        "b": back_z,
        "o": back_x,
    }
    return [
        (name, lambda name=name: kinds[name[0]](int(name[1]), int(name[2])))
        for name in HART_ORDER
    ]


def middle_kernel(
    first_ref, weight_ref, in_ref, other_ref, slope_ref, slope_z_ref, filt_hbm, wx_hbm, wz_hbm, wzi_hbm,
    wxi_hbm, out_ref, filt_ref, wx_ref, wz_ref, wzi_ref, wxi_ref, dens, gz, gy, gx, xp, sums, back,
    total_ref, power_ref, sems,
):
    moves = [(wx_hbm, wx_ref), (wz_hbm, wz_ref)]
    moves += [
        (filt_hbm.at[:, first_ref[0] + slot, :], filt_ref.at[slot]) for slot in range(2)
    ]
    moves += [(wzi_hbm, wzi_ref), (wxi_hbm, wxi_ref)]
    copies = [
        pltpu.make_async_copy(source, target, sems.at[i]) for i, (source, target) in enumerate(moves)
    ]
    for copy in copies:
        copy.start()
    xc = xc_steps(in_ref, slope_ref, slope_z_ref, out_ref, total_ref, dens, gz, gy, gx)
    hartree = hartree_steps(
        in_ref, filt_ref, other_ref, weight_ref, wx_ref, wz_ref, wzi_ref, wxi_ref, out_ref,
        power_ref, xp, sums, back,
    )
    for step in xc[:XC_AHEAD]:
        step()
    xc = xc[XC_AHEAD:]
    done = 0
    waits = {"x00": (0,), "z00": (1, 2), "z10": (3,), "b00": (4,), "o00": (5,)}
    for i, (name, step) in enumerate(hartree):
        for copy in waits.get(name, ()):
            copies[copy].wait()
        step()
        upto = min(len(xc), -(-(i + 1) * len(xc) // XC_SPREAD))
        for other in xc[done:upto]:
            other()
        done = max(done, upto)
    for other in xc[done:]:
        other()
    energies = jnp.where(
        iota((ND, 128), 1) < 64, jnp.sum(total_ref[...]), jnp.sum(power_ref[...])
    )
    put_rows(out_ref, BACK_ROWS - 1, BACK_ROWS, energies)


def homeward_kernel(in_ref, yb_ref, slope_ref, out_ref, energy_ref):
    field = jnp.concatenate(
        [get_rows(in_ref, HART + 2 * s, BACK_ROWS) for s in range(4)], axis=0
    )
    grid = dot3(yb_ref[0], yb_ref[1], *split(field))
    hi, lo = split(grid)
    parity = parity_matrix(True)
    hartree = dot1(hi, parity) + dot1(lo, parity)
    for spin in range(2):
        flux, rest = (
            jnp.concatenate(
                [get_rows(in_ref, base + spin * 4 + part * 2, BACK_ROWS) for part in range(2)],
                axis=0,
            )
            for base in (8, 0)
        )
        rows = slice(spin * NY, (spin + 1) * NY)
        out_ref[rows, :] = rest + hartree - dot3(slope_ref[0], slope_ref[1], *split(flux))
    row = jnp.sum(in_ref[pl.ds(BACK_ROWS - 1, ND, stride=BACK_ROWS), :], axis=0, keepdims=True)
    first = iota((1, 128), 1) < 64
    energy_ref[0] = jnp.sum(jnp.where(first, row, 0.0)) * (1.0 / (64.0 * CELLS))
    energy_ref[1] = jnp.sum(jnp.where(first, 0.0, row)) * (0.5 * NORM / (64.0 * CELLS))


def call(kernel, outs, in_specs, flops, scratch=(), smem_out=(), limit=40):
    specs = [SMEM if i in smem_out else VMEM for i in range(len(outs))]
    return pl.pallas_call(
        kernel,
        out_shape=list(outs),
        in_specs=in_specs,
        out_specs=specs,
        scratch_shapes=list(scratch),
        cost_estimate=pl.CostEstimate(flops=flops, bytes_accessed=4 << 20, transcendentals=0),
        compiler_params=pltpu.CompilerParams(vmem_limit_bytes=limit << 20),
    )


def in_hbm(value):
    return pltpu.with_memory_space_constraint(value, pltpu.HBM)


def arr(*shape, dtype=F32):
    return jax.ShapeDtypeStruct(shape, dtype)


def exchange(value, rows, group):
    shaped = value.reshape(ND * rows // group, group, 128)
    out = lax.all_to_all(shaped, BLOCKS, split_axis=0, concat_axis=0, tiled=True)
    return out.reshape(ND * rows, 128)


def per_device(density, kernel_hat):
    q = lax.axis_index(GZ)
    kernel_hat = in_hbm(kernel_hat)
    outward, plane = call(
        outward_kernel,
        [arr(ND * OUT_ROWS, 128), arr(MZ, MX)],
        [HBM, HBM, HBM],
        400_000_000,
        scratch=[
            pltpu.VMEM((2 * NY, NX), F32),
            pltpu.VMEM((2, 4 * ND, NY), BF16),
            pltpu.SemaphoreType.DMA((3,)),
        ],
    )(in_hbm(density.reshape(2 * NY, NX)), in_hbm(jnp.asarray(y_forward())), kernel_hat)
    other = lax.ppermute(plane, GZ, [(0, PAIR)])
    arrived = exchange(outward, OUT_ROWS, 8)
    shapes = [(2, 2, NX, MX), (2, 2 * MZ, 2 * NZ), (2, 2, NZ, 2 * NZ), (2, 2, MX, NX)]
    wx, wz, wzi, wxi, yb, slope, slope_z = call(
        tables_kernel,
        [arr(*shape, dtype=BF16) for shape in shapes]
        + [
            arr(2, NY, 4 * ND, dtype=BF16),
            arr(2, NY, NY, dtype=BF16),
            arr(2, NZ, 2 * NZ, dtype=BF16),
        ],
        [],
        2_000_000_000,
    )()
    start = jnp.where(q < ND // 2, 1, 0).astype(jnp.int32).reshape(1)
    weights = jnp.stack(
        [jnp.where(q == PAIR, 1.0, 2.0), jnp.full((), 2.0), jnp.where(q == PAIR, 0.5, 0.0)]
    ).astype(F32)
    field = pltpu.VMEM((2, 256, NX), F32)
    (back,) = call(
        middle_kernel,
        [arr(ND * BACK_ROWS, 128)],
        [SMEM, SMEM] + [VMEM] * 4 + [HBM] * 5,
        8_000_000_000,
        scratch=[pltpu.VMEM((2, MZ, MX), F32)]
        + [pltpu.VMEM(shape, BF16) for shape in shapes]
        + [field] * 4
        + [
            pltpu.VMEM((3, 2, 256, 512), BF16),
            pltpu.VMEM((2, 2, 2, 256, 512), BF16),
            pltpu.VMEM((2, 2, 2, 128, 512), BF16),
            pltpu.VMEM((8, NX), F32),
            pltpu.VMEM((8, MX), F32),
            pltpu.SemaphoreType.DMA((6,)),
        ],
    )(start, weights, arrived, other, slope, slope_z, kernel_hat, *map(in_hbm, (wx, wz, wzi, wxi)))
    returned = exchange(back, BACK_ROWS, 1)
    potential, energies = call(
        homeward_kernel,
        [arr(2 * NY, NX), arr(2)],
        [VMEM] * 3,
        1_000_000_000,
        smem_out=(1,),
    )(returned, yb, slope)
    return potential.reshape(2, 1, NY, NX), energies


def solution(mesh):
    torus = Mesh(mesh.devices.reshape(4, 4, 4, 2), GZ)
    placed = (P(None, GZ, None, None), P(None, GZ, None))
    return jax.shard_map(
        per_device,
        mesh=torus,
        in_specs=placed,
        out_specs=(P(None, GZ, None, None), P()),
        check_vma=False,
    )
```

```python
import math

import jax
import jax.numpy as jnp
import numpy as np
from jax import lax
from jax.experimental import pallas as pl
from jax.experimental.pallas import tpu as pltpu
from jax.sharding import Mesh
from jax.sharding import PartitionSpec as P


GZ = ("gz_0", "gz_1", "gz_2", "gz_3")
BLOCKS = ("gz_3", "gz_0", "gz_1", "gz_2")
HGRID = 0.35
STENCIL = (0.8, -0.2, 4.0 / 105.0, -1.0 / 280.0)
KAPPA = 0.804
MU_X = 0.2195149727645171
BETA_C = 0.06672455060314922
GAMMA_C = 0.031090690869654894
FZ_CURV = 1.709921
PARAMS_UNPOL = (0.031091, 0.2137, 7.5957, 3.5876, 1.6382, 0.49294)
PARAMS_POL = (0.015545, 0.20548, 14.1189, 6.1977, 3.3662, 0.62517)
PARAMS_STIFF = (0.016887, 0.11125, 10.357, 3.6231, 0.88026, 0.49671)

F32 = jnp.float32
BF16 = jnp.bfloat16
NZ, NY, NX = 128, 256, 256
MZ, MY, MX = 256, 512, 512
ND = 128
HART = 16
OUT_ROWS = 24
BACK_ROWS = 25
PAIR = ND // 2
CELLS = NZ * NY * NX
Z_CHUNK = 64
XC_ROWS = 8
XC_AHEAD = 12
XC_SPREAD = 16
HART_ORDER = (
    "x00", "x01", "z00", "z01", "z10", "b00", "b01", "z11", "o00", "o01", "b10", "b11", "o10", "o11",
)
NORM = 1.0 / (MX * MY * MZ)
VMEM = pl.BlockSpec(memory_space=pltpu.VMEM)
SMEM = pl.BlockSpec(memory_space=pltpu.SMEM)
HBM = pl.BlockSpec(memory_space=pltpu.HBM)


def halves(m):
    m = np.asarray(m, np.float32)
    hi = m.astype(BF16)
    lo = (m - hi.astype(np.float32)).astype(BF16)
    return np.stack([hi, lo])


def device_of(block):
    return (block & (ND // 2 - 1)) * 2 + (block >> 6)


def y_forward():
    y, q = np.arange(NY), device_of(np.arange(ND))
    first = np.where(q < ND // 2, 4 * q + 1, 4 * q)
    rows = []
    for ky in (first, first + 1):
        angle = 2.0 * np.pi * (np.outer(ky, y) % MY) / MY
        paired = (ky == MY // 2)[:, None]
        rows += [np.cos(angle), np.where(paired, 1.0, -np.sin(angle))]
    return halves(np.concatenate(rows, 0))


def split(value):
    hi = value.astype(BF16)
    lo = (value - hi.astype(F32)).astype(BF16)
    return hi, lo


def dot1(a, b):
    return jnp.dot(a, b, preferred_element_type=F32)


def dot3(a_hi, a_lo, b_hi, b_lo):
    return dot1(a_hi, b_hi) + (dot1(a_lo, b_hi) + dot1(a_hi, b_lo))


def put_rows(ref, row, rows, value, count=ND):
    for half in range(value.shape[1] // 128):
        ref[pl.ds(row + half, count, stride=rows), :] = value[
            :, half * 128 : half * 128 + 128
        ]


def get_rows(ref, row, rows):
    return jnp.concatenate(
        [ref[pl.ds(row + half, ND, stride=rows), :] for half in range(2)], axis=1
    )


def iota(shape, dim):
    return lax.broadcasted_iota(jnp.int32, shape, dim)


def slope_parts(n, place=lambda i: i):
    offset = place(iota((n, n), 1)) - place(iota((n, n), 0))
    parts = []
    coefs = halves([c / HGRID for c in STENCIL]).astype(np.float32)
    for part in range(2):
        value = jnp.zeros((n, n), F32)
        for k in range(1, 5):
            c = float(coefs[part, k - 1])
            value = jnp.where(offset == k, c, jnp.where(offset == -k, -c, value))
        parts.append(value.astype(BF16))
    return parts


def parity_matrix(transposed):
    x, place = iota((NX, NX), int(transposed)), iota((NX, NX), 1 - int(transposed))
    return jnp.where(place == (x & 1) * (NX // 2) + (x >> 1), 1.0, 0.0).astype(BF16)


def cos_sin(product):
    turn = product.astype(jnp.int32) & 511
    quarter = (turn + 64) >> 7
    angle = (turn - 128 * quarter).astype(F32) * (2.0 * math.pi / 512.0)
    sq = angle * angle
    s = angle * (
        1.0 + sq * (-1.0 / 6.0 + sq * (1.0 / 120.0 + sq * (-1.0 / 5040.0 + sq * (1.0 / 362880.0))))
    )
    c = 1.0 + sq * (-0.5 + sq * (1.0 / 24.0 + sq * (-1.0 / 720.0 + sq * (1.0 / 40320.0))))
    odd = (quarter & 1) == 1
    c, s = jnp.where(odd, s, c), jnp.where(odd, c, s)
    return (
        jnp.where(((quarter + 1) & 2) == 2, -c, c),
        jnp.where((quarter & 2) == 2, -s, s),
    )


def put_parts(ref, index, rows, cols, value):
    hi, lo = split(value)
    ref[(*index, 0, rows, cols)] = hi
    ref[(*index, 1, rows, cols)] = lo


def put_rotation(ref, index, row, c, s, transposed):
    n, m = c.shape
    top, low = slice(row, row + n), slice(row + n, row + 2 * n)
    put_parts(ref, index, top, slice(0, m), c)
    put_parts(ref, index, low, slice(m, 2 * m), c)
    put_parts(ref, index, top, slice(m, 2 * m), -s if transposed else s)
    put_parts(ref, index, low, slice(0, m), s if transposed else -s)


def float_iota(shape, dim):
    return iota(shape, dim).astype(F32)


def tables_kernel(wx_ref, wz_ref, wzi_ref, wxi_ref, yb_ref, slope_ref, slope_z_ref):
    for parity in range(2):
        shape = (NX // 2, MX // 2)
        x = 2.0 * float_iota(shape, 0) + parity
        put_rotation(wx_ref, (parity,), 0, *cos_sin(x * float_iota(shape, 1)), True)
        shape = (MX // 2, NX // 2)
        x = 2.0 * float_iota(shape, 1) + parity
        put_rotation(wxi_ref, (parity,), 0, *cos_sin(x * float_iota(shape, 0)), False)
        shape = (NZ // 2, NZ)
        z = 4.0 * float_iota(shape, 0) + 2.0 * parity
        put_rotation(wzi_ref, (parity,), 0, *cos_sin(z * float_iota(shape, 1)), True)
    for chunk in range(NZ // Z_CHUNK):
        shape = (2 * Z_CHUNK, NZ)
        row = iota(shape, 0)
        kz = chunk * Z_CHUNK + jnp.where(row < Z_CHUNK, row, row + NZ - Z_CHUNK)
        angle = 2.0 * kz.astype(F32) * device_of(iota(shape, 1)).astype(F32)
        put_rotation(wz_ref, (), chunk * 4 * Z_CHUNK, *cos_sin(angle), False)
    for slot in range(2):
        shape = (NY, ND)
        q = device_of(iota(shape, 1))
        ky = 4 * q + slot + jnp.where(q < ND // 2, 1, 0)
        c, s = cos_sin(ky.astype(F32) * float_iota(shape, 0))
        weight = jnp.where(ky == MY // 2, NORM, 2.0 * NORM)
        s = jnp.where(ky == MY // 2, -1.0, s)
        put_parts(yb_ref, (), slice(0, NY), slice(256 * slot, 256 * slot + 128), c * weight)
        put_parts(yb_ref, (), slice(0, NY), slice(256 * slot + 128, 256 * slot + 256), -s * weight)
    for part, value in enumerate(slope_parts(NY)):
        slope_ref[part] = value
    for part, value in enumerate(slope_parts(NZ, device_of)):
        slope_z_ref[part, :, 0:NZ] = value
        slope_z_ref[part, :, NZ : 2 * NZ] = value


def outward_kernel(dens_hbm, table_hbm, filt_hbm, out_ref, plane_ref, dens_ref, table_ref, sems):
    dens_copy = pltpu.make_async_copy(dens_hbm, dens_ref, sems.at[0])
    table_copy = pltpu.make_async_copy(table_hbm, table_ref, sems.at[1])
    plane_copy = pltpu.make_async_copy(filt_hbm.at[:, 0, :], plane_ref, sems.at[2])
    dens_copy.start()
    table_copy.start()
    plane_copy.start()
    slope = slope_parts(NY)
    parity = parity_matrix(False)
    dens_copy.wait()
    for spin in range(2):
        field = dens_ref[spin * NY : (spin + 1) * NY, :]
        grad = dot3(*slope, *split(field))
        for part in range(2):
            rows = slice(part * 128, part * 128 + 128)
            put_rows(out_ref, spin * 4 + part * 2, OUT_ROWS, field[rows])
            put_rows(out_ref, 8 + spin * 4 + part * 2, OUT_ROWS, grad[rows])
    hi, lo = split(dens_ref[0:NY, :] + dens_ref[NY : 2 * NY, :])
    hi, lo = dot1(hi, parity), dot1(lo, parity)
    hi, lo = hi.astype(BF16), lo.astype(BF16)
    table_copy.wait()
    for s in range(4):
        rows = slice(s * ND, (s + 1) * ND)
        value = dot3(table_ref[0, rows, :], table_ref[1, rows, :], hi, lo)
        put_rows(out_ref, HART + s * 2, OUT_ROWS, value)
    plane_copy.wait()


LN2 = math.log(2.0)


def pw_piece(powers, params):
    root, radius, cube, square = powers
    scale = 2.0 * params[0]
    t1, t2 = (scale * params[2]) * root, (scale * params[3]) * radius
    t3, t4 = (scale * params[4]) * cube, (scale * params[5]) * square
    series = (t1 + t2) + (t3 + t4)
    slope = (series + t4) + 0.5 * (t3 - t1)
    more = series + 1.0
    inv = 1.0 / (series * more)
    logarithm = jnp.log(1.0 + inv * more)
    tilt = (-scale * params[1]) * radius
    front = tilt - scale
    return front * logarithm, tilt * logarithm - (front * slope) * inv


def exchange_piece(twice, inv_root, sigma):
    inv2 = inv_root * inv_root
    inv4 = inv2 * inv2
    root = twice * inv2
    front = -0.75 * (3.0 / math.pi) ** (1.0 / 3.0)
    unit = 1.0 / (3.0 * math.pi**2) ** (2.0 / 3.0)
    damp = 1.0 / (1.0 + (MU_X / KAPPA * unit) * sigma * (inv4 * inv4))
    gain = KAPPA - KAPPA * damp
    scaled = front * root
    energy = twice * scaled * (1.0 + gain)
    d_dens = scaled * (4.0 / 3.0 + gain * (4.0 / 3.0 - (8.0 / 3.0) * damp))
    d_sigma = (front * MU_X * unit) * (damp * damp) * inv4
    return energy, d_dens, d_sigma, root


def xc_point(up, down, sigma_uu, sigma_ud, sigma_dd):
    twice_up, twice_down = up + up, down + down
    inv_up = jnp.exp2(jnp.log(twice_up) * (-1.0 / (3.0 * LN2)))
    inv_down = jnp.exp2(jnp.log(twice_down) * (-1.0 / (3.0 * LN2)))
    e_up, d_up, d_uu, root_up = exchange_piece(twice_up, inv_up, sigma_uu)
    e_down, d_down, d_dd, root_down = exchange_piece(twice_down, inv_down, sigma_dd)
    dens = up + down
    sixth = jnp.exp2(jnp.log(dens) * (-1.0 / (6.0 * LN2)))
    inv_third = sixth * sixth
    inv_two = inv_third * inv_third
    third = dens * inv_two
    inv_dens = inv_two * inv_third
    plus = twice_up * inv_dens
    minus = twice_down * inv_dens
    zeta = 0.5 * (plus - minus)
    plus_cube = root_up * inv_third
    minus_cube = root_down * inv_third
    f_scale = 1.0 / (2.0 ** (4.0 / 3.0) - 2.0)
    f = (plus * plus_cube + minus * minus_cube) * f_scale - 2.0 * f_scale
    f_slope = (plus_cube - minus_cube) * (4.0 / 3.0 * f_scale)
    root = (3.0 / (4.0 * math.pi)) ** (1.0 / 6.0) * sixth
    radius = root * root
    powers = (root, radius, radius * root, radius * radius)
    e0, e0_d = pw_piece(powers, PARAMS_UNPOL)
    e1, e1_d = pw_piece(powers, PARAMS_POL)
    ac, ac_d = pw_piece(powers, PARAMS_STIFF)
    z2 = zeta * zeta
    z4 = z2 * z2
    one_z4 = z4 * (1.0 / FZ_CURV) - 1.0 / FZ_CURV
    f_z4 = f * z4
    f_one = f * one_z4
    diff = e1 - e0
    local = e0 + ac * f_one + diff * f_z4
    local_r = e0_d + ac_d * f_one + (e1_d - e0_d) * f_z4
    local_z = (ac * one_z4 + diff * z4) * f_slope + (ac * (1.0 / FZ_CURV) + diff) * (
        4.0 * f * z2 * zeta
    )
    phi2 = plus_cube * plus_cube + minus_cube * minus_cube
    inv_phi2 = 1.0 / phi2
    inv_sq = inv_phi2 * inv_phi2
    phi_log_slope = (third * (inv_up - inv_down)) * ((2.0 / 3.0) * inv_phi2)
    g3 = (GAMMA_C / 8.0) * (phi2 * phi2) * phi2
    grow = jnp.exp2(local * (inv_sq * inv_phi2) * (-8.0 / (GAMMA_C * LN2)))
    weight_a = (BETA_C / GAMMA_C) / (grow - 1.0)
    sigma = (sigma_uu + sigma_dd) + (sigma_ud + sigma_ud)
    ct = 4.0 * math.pi / (16.0 * (3.0 * math.pi**2) ** (1.0 / 3.0))
    kt = (ct * inv_third) * (inv_dens * inv_dens) * inv_sq
    t2 = sigma * kt
    w = weight_a * t2
    num = 1.0 + w
    den = num + w * w
    add = (BETA_C / GAMMA_C) * t2 * num
    both = den + add
    inv_both = 1.0 / (den * both)
    h = g3 * jnp.log(1.0 + add * (inv_both * both))
    h_t = ((BETA_C / GAMMA_C) * g3) * ((num + w) * inv_both)
    h_a = -((w * w) * w) * ((1.0 + num) * grow) * inv_both
    total = local + h
    ht_t2 = h_t * t2
    one_ha = 1.0 + h_a
    d_n = total - one_ha * ((1.0 / 3.0) * local_r) - (7.0 / 3.0) * ht_t2
    d_z = one_ha * local_z + phi_log_slope * (3.0 * (h - h_a * local) - (ht_t2 + ht_t2))
    d_sigma = 2.0 * (dens * h_t * kt)
    energy = 0.5 * (e_up + e_down) + dens * total
    return (
        energy,
        d_up + d_n + minus * d_z,
        d_down + d_n - plus * d_z,
        d_uu + d_sigma,
        d_sigma,
        d_dd + d_sigma,
    )


def slope_along_z(slope_z_ref, hi, lo):
    both = jnp.concatenate([hi, lo], axis=0)
    return dot1(slope_z_ref[0], both) + dot1(slope_z_ref[1], both)


def slope_along_x(slope_ref, hi, lo):
    return -dot3(hi, lo, slope_ref[0], slope_ref[1])


def xc_steps(in_ref, slope_ref, slope_z_ref, out_ref, total_ref, dens, gz, gy, gx):
    def gradients(part):
        rows = slice(part * 128, part * 128 + 128)
        for spin in range(2):
            field = get_rows(in_ref, spin * 4 + part * 2, OUT_ROWS)
            dens[spin, rows, :] = field
            gy[spin, rows, :] = get_rows(in_ref, 8 + spin * 4 + part * 2, OUT_ROWS)
            hi, lo = split(field)
            gz[spin, rows, :] = slope_along_z(slope_z_ref, hi, lo)
            gx[spin, rows, :] = slope_along_x(slope_ref, hi, lo)

    def points(i):
        rows = slice(i * XC_ROWS, (i + 1) * XC_ROWS)
        zu, zd = gz[0, rows, :], gz[1, rows, :]
        yu, yd = gy[0, rows, :], gy[1, rows, :]
        xu, xd = gx[0, rows, :], gx[1, rows, :]
        energy, d_up, d_down, d_uu, d_ud, d_dd = xc_point(
            dens[0, rows, :],
            dens[1, rows, :],
            zu * zu + yu * yu + xu * xu,
            zu * zd + yu * yd + xu * xd,
            zd * zd + yd * yd + xd * xd,
        )
        dens[0, rows, :] = d_up
        dens[1, rows, :] = d_down
        for ref, gu, gd in ((gz, zu, zd), (gy, yu, yd), (gx, xu, xd)):
            ref[0, rows, :] = d_uu * gu + d_ud * gd
            ref[1, rows, :] = d_dd * gd + d_ud * gu
        folded = sum(energy[r : r + 8] for r in range(0, XC_ROWS, 8))
        total_ref[...] = folded if i == 0 else total_ref[...] + folded

    def divergence(part):
        rows = slice(part * 128, part * 128 + 128)
        for spin in range(2):
            div = slope_along_z(slope_z_ref, *split(gz[spin, rows, :]))
            div = div + slope_along_x(slope_ref, *split(gx[spin, rows, :]))
            put_rows(out_ref, spin * 4 + part * 2, BACK_ROWS, dens[spin, rows, :] - div)
            put_rows(out_ref, 8 + spin * 4 + part * 2, BACK_ROWS, gy[spin, rows, :])

    steps = []
    for part in range(2):
        steps.append(lambda part=part: gradients(part))
        for i in range(part * 128 // XC_ROWS, (part + 1) * 128 // XC_ROWS):
            steps.append(lambda i=i: points(i))
        steps.append(lambda part=part: divergence(part))
    return steps


def hartree_steps(
    in_ref, filt_ref, other_ref, weight_ref, wx_ref, wz_ref, wzi_ref, wxi_ref, out_ref, power_ref,
    half_ref, xp, sums, back,
):
    def forward_x(_slot, parity):
        stack = []
        for slot, sign in ((0, 1), (1, 1), (0, -1)):
            base = HART + 4 * slot + parity
            real = in_ref[pl.ds(base, ND, stride=OUT_ROWS), :]
            imag = in_ref[pl.ds(base + 2, ND, stride=OUT_ROWS), :]
            stack.append(jnp.concatenate([real, imag if sign > 0 else -imag], axis=1))
        both = jnp.concatenate(stack, axis=0)
        value = dot3(*split(both), wx_ref[parity, 0], wx_ref[parity, 1])
        if parity == 0:
            half_ref[...] = value
            return
        for half in range(2):
            cols = slice(half * 256, half * 256 + 256)
            whole = half_ref[...] + value if half == 0 else half_ref[...] - value
            hi, lo = split(whole)
            for place in range(3):
                rows = slice(place * 128, place * 128 + 128)
                xp[place, 0, 0:128, cols] = hi[rows, 0:256]
                xp[place, 0, 128:256, cols] = hi[rows, 256:512]
                xp[place, 1, 0:128, cols] = lo[rows, 0:256]
                xp[place, 1, 128:256, cols] = lo[rows, 256:512]

    def filtered(slot, c):
        rows = slice(c * 4 * Z_CHUNK, (c + 1) * 4 * Z_CHUNK)
        spec = dot3(wz_ref[0, rows, :], wz_ref[1, rows, :], xp[slot, 0], xp[slot, 1])
        if slot == 0:
            mirror = dot3(wz_ref[0, rows, :], wz_ref[1, rows, :], xp[2, 0], xp[2, 1])
        planes = []
        for high in range(2):
            place = slice(high * NZ + c * Z_CHUNK, high * NZ + (c + 1) * Z_CHUNK)
            own = filt_ref[slot, place, :]
            if slot == 0:
                swap = (own - other_ref[place, :]) * weight_ref[2]
                planes.append((own - swap, swap))
            else:
                planes.append((own, None))
        acc = None
        first = slot == 0 and c == 0
        for kind in range(2):
            pair = []
            for high in range(2):
                start = (2 * kind + high) * Z_CHUNK
                at = slice(start, start + Z_CHUNK)
                value = spec[at] * planes[high][0]
                if slot == 0:
                    value = value + mirror[at] * planes[high][1]
                power = spec[at] * value
                power = sum(power[r : r + 8] for r in range(0, Z_CHUNK, 8))
                acc = power if acc is None else acc + power
                pair.append(value)
            dest = slice(kind * NZ + c * Z_CHUNK, kind * NZ + (c + 1) * Z_CHUNK)
            for parity, value in ((0, pair[0] + pair[1]), (1, pair[0] - pair[1])):
                hi, lo = split(value)
                sums[slot, parity, 0, dest, :] = hi
                sums[slot, parity, 1, dest, :] = lo
        acc = weight_ref[slot] * acc
        power_ref[...] = acc if first else power_ref[...] + acc

    def back_z(slot, parity):
        src = sums.at[slot, parity]
        grid = dot3(wzi_ref[parity, 0], wzi_ref[parity, 1], src[0], src[1])
        for sign in range(2):
            a, b = grid[:, 0:256], grid[:, 256:512]
            hi, lo = split(a + b if sign == 0 else a - b)
            for part, value in ((0, hi), (1, lo)):
                rows = slice(parity * 64, parity * 64 + 64)
                back[slot, sign, part, rows, 0:256] = value[0:64]
                back[slot, sign, part, rows, 256:512] = value[64:128]

    def back_x(slot, sign):
        src = back.at[slot, sign]
        value = dot3(src[0], src[1], wxi_ref[sign, 0], wxi_ref[sign, 1])
        for parity in range(2):
            for kind in range(2):
                put_rows(
                    out_ref,
                    parity * 64 * BACK_ROWS + HART + slot * 4 + kind * 2 + sign,
                    BACK_ROWS,
                    value[parity * 64 : parity * 64 + 64, kind * 128 : kind * 128 + 128],
                    count=64,
                )

    kinds = {
        "x": forward_x,
        "z": filtered,
        "b": back_z,
        "o": back_x,
    }
    return [
        (name, lambda name=name: kinds[name[0]](int(name[1]), int(name[2])))
        for name in HART_ORDER
    ]


def middle_kernel(
    first_ref, weight_ref, in_ref, other_ref, slope_ref, slope_z_ref, filt_hbm, wx_hbm, wz_hbm, wzi_hbm,
    wxi_hbm, out_ref, filt_ref, wx_ref, wz_ref, wzi_ref, wxi_ref, dens, gz, gy, gx, xp, sums, back,
    total_ref, power_ref, half_ref, sems,
):
    moves = [(wx_hbm, wx_ref), (wz_hbm, wz_ref)]
    moves += [
        (filt_hbm.at[:, first_ref[0] + slot, :], filt_ref.at[slot]) for slot in range(2)
    ]
    moves += [(wzi_hbm, wzi_ref), (wxi_hbm, wxi_ref)]
    copies = [
        pltpu.make_async_copy(source, target, sems.at[i]) for i, (source, target) in enumerate(moves)
    ]
    for copy in copies:
        copy.start()
    xc = xc_steps(in_ref, slope_ref, slope_z_ref, out_ref, total_ref, dens, gz, gy, gx)
    hartree = hartree_steps(
        in_ref, filt_ref, other_ref, weight_ref, wx_ref, wz_ref, wzi_ref, wxi_ref, out_ref,
        power_ref, half_ref, xp, sums, back,
    )
    for step in xc[:XC_AHEAD]:
        step()
    xc = xc[XC_AHEAD:]
    done = 0
    waits = {"x00": (0,), "z00": (1, 2), "z10": (3,), "b00": (4,), "o00": (5,)}
    for i, (name, step) in enumerate(hartree):
        for copy in waits.get(name, ()):
            copies[copy].wait()
        step()
        upto = min(len(xc), -(-(i + 1) * len(xc) // XC_SPREAD))
        for other in xc[done:upto]:
            other()
        done = max(done, upto)
    for other in xc[done:]:
        other()
    energies = jnp.where(
        iota((ND, 128), 1) < 64, jnp.sum(total_ref[...]), jnp.sum(power_ref[...])
    )
    put_rows(out_ref, BACK_ROWS - 1, BACK_ROWS, energies)


def homeward_kernel(in_ref, yb_ref, slope_ref, out_ref, energy_ref):
    field = jnp.concatenate(
        [get_rows(in_ref, HART + 2 * s, BACK_ROWS) for s in range(4)], axis=0
    )
    grid = dot3(yb_ref[0], yb_ref[1], *split(field))
    hi, lo = split(grid)
    parity = parity_matrix(True)
    hartree = dot1(hi, parity) + dot1(lo, parity)
    for spin in range(2):
        flux, rest = (
            jnp.concatenate(
                [get_rows(in_ref, base + spin * 4 + part * 2, BACK_ROWS) for part in range(2)],
                axis=0,
            )
            for base in (8, 0)
        )
        rows = slice(spin * NY, (spin + 1) * NY)
        out_ref[rows, :] = rest + hartree - dot3(slope_ref[0], slope_ref[1], *split(flux))
    row = jnp.sum(in_ref[pl.ds(BACK_ROWS - 1, ND, stride=BACK_ROWS), :], axis=0, keepdims=True)
    first = iota((1, 128), 1) < 64
    energy_ref[0] = jnp.sum(jnp.where(first, row, 0.0)) * (1.0 / (64.0 * CELLS))
    energy_ref[1] = jnp.sum(jnp.where(first, 0.0, row)) * (0.5 * NORM / (64.0 * CELLS))


def call(kernel, outs, in_specs, flops, scratch=(), smem_out=(), limit=40):
    specs = [SMEM if i in smem_out else VMEM for i in range(len(outs))]
    return pl.pallas_call(
        kernel,
        out_shape=list(outs),
        in_specs=in_specs,
        out_specs=specs,
        scratch_shapes=list(scratch),
        cost_estimate=pl.CostEstimate(flops=flops, bytes_accessed=4 << 20, transcendentals=0),
        compiler_params=pltpu.CompilerParams(vmem_limit_bytes=limit << 20),
    )


def in_hbm(value):
    return pltpu.with_memory_space_constraint(value, pltpu.HBM)


def arr(*shape, dtype=F32):
    return jax.ShapeDtypeStruct(shape, dtype)


def exchange(value, rows, group):
    shaped = value.reshape(ND * rows // group, group, 128)
    out = lax.all_to_all(shaped, BLOCKS, split_axis=0, concat_axis=0, tiled=True)
    return out.reshape(ND * rows, 128)


def per_device(density, kernel_hat):
    q = lax.axis_index(GZ)
    kernel_hat = in_hbm(kernel_hat)
    outward, plane = call(
        outward_kernel,
        [arr(ND * OUT_ROWS, 128), arr(MZ, MX)],
        [HBM, HBM, HBM],
        400_000_000,
        scratch=[
            pltpu.VMEM((2 * NY, NX), F32),
            pltpu.VMEM((2, 4 * ND, NY), BF16),
            pltpu.SemaphoreType.DMA((3,)),
        ],
    )(in_hbm(density.reshape(2 * NY, NX)), in_hbm(jnp.asarray(y_forward())), kernel_hat)
    other = lax.ppermute(plane, GZ, [(0, PAIR)])
    arrived = exchange(outward, OUT_ROWS, 8)
    shapes = [(2, 2, NX, MX), (2, 2 * MZ, 2 * NZ), (2, 2, NZ, 2 * NZ), (2, 2, MX, NX)]
    wx, wz, wzi, wxi, yb, slope, slope_z = call(
        tables_kernel,
        [arr(*shape, dtype=BF16) for shape in shapes]
        + [
            arr(2, NY, 4 * ND, dtype=BF16),
            arr(2, NY, NY, dtype=BF16),
            arr(2, NZ, 2 * NZ, dtype=BF16),
        ],
        [],
        2_000_000_000,
    )()
    start = jnp.where(q < ND // 2, 1, 0).astype(jnp.int32).reshape(1)
    weights = jnp.stack(
        [jnp.where(q == PAIR, 1.0, 2.0), jnp.full((), 2.0), jnp.where(q == PAIR, 0.5, 0.0)]
    ).astype(F32)
    field = pltpu.VMEM((2, 256, NX), F32)
    (back,) = call(
        middle_kernel,
        [arr(ND * BACK_ROWS, 128)],
        [SMEM, SMEM] + [VMEM] * 4 + [HBM] * 5,
        8_000_000_000,
        scratch=[pltpu.VMEM((2, MZ, MX), F32)]
        + [pltpu.VMEM(shape, BF16) for shape in shapes]
        + [field] * 4
        + [
            pltpu.VMEM((3, 2, 256, 512), BF16),
            pltpu.VMEM((2, 2, 2, 256, 512), BF16),
            pltpu.VMEM((2, 2, 2, 128, 512), BF16),
            pltpu.VMEM((8, NX), F32),
            pltpu.VMEM((8, MX), F32),
            pltpu.VMEM((3 * ND, MX), F32),
            pltpu.SemaphoreType.DMA((6,)),
        ],
    )(start, weights, arrived, other, slope, slope_z, kernel_hat, *map(in_hbm, (wx, wz, wzi, wxi)))
    returned = exchange(back, BACK_ROWS, 1)
    potential, energies = call(
        homeward_kernel,
        [arr(2 * NY, NX), arr(2)],
        [VMEM] * 3,
        1_000_000_000,
        smem_out=(1,),
    )(returned, yb, slope)
    return potential.reshape(2, 1, NY, NX), energies


def solution(mesh):
    torus = Mesh(mesh.devices.reshape(4, 4, 4, 2), GZ)
    placed = (P(None, GZ, None, None), P(None, GZ, None))
    return jax.shard_map(
        per_device,
        mesh=torus,
        in_specs=placed,
        out_specs=(P(None, GZ, None, None), P()),
        check_vma=False,
    )
```
